16 devices in a mesh: dp: 4 (over z, y), sp: 4 (over x, core).
Axes of the slice: x: 2, y: 2, z: 2, core: 2. Of those that a mesh axis runs over, the one named last changes fastest.
Arguments:
- x_steps: bfloat16 [4, 256, 4096], P(None, 'dp'), parts along dimension 1
- k_cache: bfloat16 [256, 512, 8, 128], P('dp', 'sp'), parts along dimension 0
- v_cache: bfloat16 [256, 512, 8, 128], P('dp', 'sp'), parts along dimension 0
- seq_lens: int32 [256], P('dp'), parts along dimension 0
- norm_gain: bfloat16 [4096], replicated
- w_q: bfloat16 [4096, 4096], replicated
- w_k: bfloat16 [4096, 1024], replicated
- w_v: bfloat16 [4096, 1024], replicated
- w_o: bfloat16 [4096, 4096], replicated
- q_gain: bfloat16 [128], replicated
- k_gain: bfloat16 [128], replicated
Outputs:
- output 1: bfloat16 [4, 256, 4096], P(None, 'dp'), parts along dimension 1
- output 2: bfloat16 [256, 512, 8, 128], P('dp', 'sp'), parts along dimension 0
- output 3: bfloat16 [256, 512, 8, 128], P('dp', 'sp'), parts along dimension 0
There are 4 independent parts. The reference program is written for one: setup_inputs(seed, part) draws one part's arguments, and reference() takes and returns one part's arrays. A program takes and returns all parts, laid end to end along the dimension named above; an argument that names none is the same for every part.
All inputs are finite; a program needn't handle non-finite values.
Results may differ from the reference program's by a relative error of at most 0.0105101.
Values sent between devices are 32-bit elements.
A program may use at most 1 GiB of HBM per device.

```python
import math
import jax
import jax.numpy as jnp
from jax import lax

STEPS = 4
BATCH = 64
SEQ_LEN = 512
HIDDEN = 4096
NUM_Q_HEADS = 32
NUM_KV_HEADS = 8
HEAD_DIM = 128
ROPE_BASE = 1000000
NORM_EPS = 1e-6


def draw_lengths(key):
    keys = jax.random.split(key, 3)
    lengths = jax.random.randint(keys[0], (BATCH,), 0, SEQ_LEN - STEPS + 1, dtype=jnp.int32)
    order = jax.random.permutation(keys[1], BATCH)
    short_count = max(1, BATCH // 4)
    lengths = lengths.at[order[0]].set(SEQ_LEN - STEPS)
    short_lens = jax.random.randint(keys[2], (short_count,), 0, 16, dtype=jnp.int32)
    return lengths.at[order[1:1 + short_count]].set(short_lens)


def setup_inputs(seed: int = 0, part: int = 0) -> dict:
    shared = jax.random.split(jax.random.key(seed), 7)
    own_keys = jax.random.split(jax.random.fold_in(jax.random.key(seed + 1), part), 4)
    q_dim = NUM_Q_HEADS * HEAD_DIM
    kv_dim = NUM_KV_HEADS * HEAD_DIM
    score_scale = math.sqrt(math.log(SEQ_LEN / 16))
    cache_shape = (BATCH, SEQ_LEN, NUM_KV_HEADS, HEAD_DIM)

    def normal(key, shape):
        return jax.random.normal(key, shape, jnp.float32)

    return {
        'x_steps': (0.5 * normal(own_keys[0], (STEPS, BATCH, HIDDEN))).astype(jnp.bfloat16),
        'k_cache': normal(own_keys[1], cache_shape).astype(jnp.bfloat16),
        'v_cache': normal(own_keys[2], cache_shape).astype(jnp.bfloat16),
        'seq_lens': draw_lengths(own_keys[3]),
        'norm_gain': (1.0 + 0.3 * normal(shared[0], (HIDDEN,))).astype(jnp.bfloat16),
        'w_q': (normal(shared[1], (HIDDEN, q_dim)) * HIDDEN ** -0.5).astype(jnp.bfloat16),
        'w_k': (normal(shared[2], (HIDDEN, kv_dim)) * HIDDEN ** -0.5).astype(jnp.bfloat16),
        'w_v': (normal(shared[3], (HIDDEN, kv_dim)) * HIDDEN ** -0.5).astype(jnp.bfloat16),
        'w_o': (normal(shared[4], (q_dim, HIDDEN)) * q_dim ** -0.5).astype(jnp.bfloat16),
        'q_gain': (score_scale * (1.0 + 0.2 * normal(shared[5], (HEAD_DIM,)))).astype(jnp.bfloat16),
        'k_gain': (1.0 + 0.2 * normal(shared[6], (HEAD_DIM,))).astype(jnp.bfloat16),
    }


def rms_scale(values, gain):
    inv_rms = lax.rsqrt(jnp.mean(values * values, axis=-1, keepdims=True) + NORM_EPS)
    return values * inv_rms * gain.astype(jnp.float32)


def rope_rotate(values, positions):
    half_dim = HEAD_DIM // 2
    inv_freq = jnp.exp(jnp.arange(half_dim, dtype=jnp.float32) * (-2.0 * math.log(ROPE_BASE) / HEAD_DIM))
    angles = positions.astype(jnp.float32)[..., None, None] * inv_freq
    cosine = jnp.cos(angles)
    sine = jnp.sin(angles)
    lower_half = values[..., :half_dim]
    upper_half = values[..., half_dim:]
    return jnp.concatenate([lower_half * cosine - upper_half * sine, upper_half * cosine + lower_half * sine], axis=-1)


def reference(x_steps, k_cache, v_cache, seq_lens, norm_gain, w_q, w_k, w_v, w_o, q_gain, k_gain):
    group = NUM_Q_HEADS // NUM_KV_HEADS
    slot_ids = jnp.arange(SEQ_LEN)
    rows = jnp.arange(BATCH)

    def attend_one(operands):
        query, keys, vals, position = operands
        grouped = query.reshape(NUM_KV_HEADS, group, HEAD_DIM).astype(jnp.float32)
        scores = jnp.einsum('kgd,skd->kgs', grouped, keys.astype(jnp.float32)) * HEAD_DIM ** -0.5
        scores = jnp.where((slot_ids <= position)[None, None, :], scores, -jnp.inf)
        weights = jax.nn.softmax(scores, axis=-1)
        mixed = jnp.einsum('kgs,skd->kgd', weights, vals.astype(jnp.float32))
        return mixed.reshape(NUM_Q_HEADS, HEAD_DIM)

    def decode_step(caches, step_in):
        k_now, v_now = caches
        x_now, step = step_in
        positions = seq_lens + step
        x_f32 = x_now.astype(jnp.float32)
        normed = rms_scale(x_f32, norm_gain).astype(jnp.bfloat16)
        queries = jnp.dot(normed, w_q, preferred_element_type=jnp.float32).astype(jnp.bfloat16)
        keys_new = jnp.dot(normed, w_k, preferred_element_type=jnp.float32).astype(jnp.bfloat16)
        vals_new = jnp.dot(normed, w_v, preferred_element_type=jnp.float32).astype(jnp.bfloat16)
        queries = queries.reshape(BATCH, NUM_Q_HEADS, HEAD_DIM)
        keys_new = keys_new.reshape(BATCH, NUM_KV_HEADS, HEAD_DIM)
        vals_new = vals_new.reshape(BATCH, NUM_KV_HEADS, HEAD_DIM)
        queries = rope_rotate(rms_scale(queries.astype(jnp.float32), q_gain), positions).astype(jnp.bfloat16)
        keys_new = rope_rotate(rms_scale(keys_new.astype(jnp.float32), k_gain), positions).astype(jnp.bfloat16)
        k_now = k_now.at[rows, positions].set(keys_new)
        v_now = v_now.at[rows, positions].set(vals_new)
        attended = lax.map(attend_one, (queries, k_now, v_now, positions)).astype(jnp.bfloat16)
        out_proj = jnp.dot(attended.reshape(BATCH, -1), w_o, preferred_element_type=jnp.float32)
        y_now = (x_f32 + out_proj).astype(jnp.bfloat16)
        return (k_now, v_now), y_now

    (k_out, v_out), y_steps = lax.scan(decode_step, (k_cache, v_cache), (x_steps, jnp.arange(STEPS)))
    return (y_steps, k_out, v_out)
```

```python
import functools
import math

import jax
import jax.numpy as jnp
from jax import lax
from jax.experimental import pallas as pl
from jax.experimental.pallas import tpu as pltpu
from jax.sharding import PartitionSpec as P

NORM_EPS = 1e-6
ROPE_BASE = 1000000.0
MASKED_MAX = -1e30
HEAD_DIM = 128
F32 = jnp.float32
BF16 = jnp.bfloat16
MIB = 1024 * 1024
VMEM = pltpu.VMEM


def rope_tables(seq_lens, steps):
    half = HEAD_DIM // 2
    positions = (seq_lens[:, None] + jnp.arange(steps, dtype=jnp.int32)[None, :]).reshape(-1)
    inv_freq = jnp.exp(jnp.arange(half, dtype=F32) * (-2.0 * math.log(ROPE_BASE) / HEAD_DIM))
    angles = positions.astype(F32)[:, None] * inv_freq
    cosine = jnp.cos(angles)
    sine = jnp.sin(angles)
    return jnp.concatenate([cosine, cosine], axis=-1), jnp.concatenate([-sine, sine], axis=-1)


def project_kernel(width, heads, kv_heads, x_ref, gain_ref, cos_ref, sin_ref, q_gain_ref, k_gain_ref, wq_ref, wk_ref, wv_ref, q_ref, k_ref, v_ref, rows_f32, rows_bf16, acc, wbuf, sems):
    steps, batch, hidden = x_ref.shape
    rows = steps * batch
    depth = wbuf.shape[0]
    per_block = width // HEAD_DIM
    q_blocks = heads // per_block
    kv_blocks = kv_heads // per_block
    total = q_blocks + 2 * kv_blocks

    def fetch(index, slot):
        def start(w_ref, block):
            cols = pl.ds(pl.multiple_of(block * width, width), width)
            pltpu.make_async_copy(w_ref.at[:, cols], wbuf.at[slot], sems.at[slot]).start()

        @pl.when(index < kv_blocks)
        def _():
            start(wk_ref, index)

        @pl.when((index >= kv_blocks) & (index < 2 * kv_blocks))
        def _():
            start(wv_ref, index - kv_blocks)

        @pl.when(index >= 2 * kv_blocks)
        def _():
            start(wq_ref, index - 2 * kv_blocks)

    for slot in range(depth - 1):
        fetch(jnp.int32(slot), slot)

    for step in range(steps):
        values = x_ref[step].astype(F32)
        inv_rms = lax.rsqrt(jnp.mean(values * values, axis=-1, keepdims=True) + NORM_EPS)
        normed = values * inv_rms * gain_ref[...].astype(F32)
        for n in range(hidden // 128):
            rows_f32[n, pl.ds(step, batch, stride=steps), :] = normed[:, n * 128:(n + 1) * 128]
    for n in range(hidden // 128):
        rows_bf16[:, n * 128:(n + 1) * 128] = rows_f32[n].astype(BF16)

    def normed_rotated(values, gain):
        inv_rms = lax.rsqrt(jnp.mean(values * values, axis=-1, keepdims=True) + NORM_EPS)
        scaled = values * inv_rms * gain
        return scaled * cos_ref[...] + pltpu.roll(scaled, HEAD_DIM // 2, 1) * sin_ref[...]

    def block_step(index, carry):
        slot = lax.rem(index, depth)
        ahead = index + depth - 1

        @pl.when(ahead < total)
        def _():
            fetch(ahead, lax.rem(ahead, depth))

        pltpu.make_async_copy(wq_ref.at[:, pl.ds(0, width)], wbuf.at[slot], sems.at[slot]).wait()
        acc[...] = jnp.dot(rows_bf16[...], wbuf[slot], preferred_element_type=F32)

        def head_values(j):
            return acc[:, j * HEAD_DIM:(j + 1) * HEAD_DIM].astype(BF16).astype(F32)

        @pl.when(index < kv_blocks)
        def _():
            for j in range(per_block):
                out = normed_rotated(head_values(j), k_gain_ref[...].astype(F32)).astype(BF16).astype(F32)
                k_ref[pl.ds(index * per_block + j, rows, stride=kv_heads), :] = out

        @pl.when((index >= kv_blocks) & (index < 2 * kv_blocks))
        def _():
            for j in range(per_block):
                v_ref[pl.ds((index - kv_blocks) * per_block + j, rows, stride=kv_heads), :] = head_values(j)

        @pl.when(index >= 2 * kv_blocks)
        def _():
            for j in range(per_block):
                out = normed_rotated(head_values(j), q_gain_ref[...].astype(F32)).astype(BF16).astype(F32)
                q_ref[pl.ds((index - 2 * kv_blocks) * per_block + j, rows, stride=heads), :] = out

        return carry

    lax.fori_loop(0, total, block_step, 0)


def project(x_steps, norm_gain, cosine, sine, q_gain, k_gain, w_q, w_k, w_v):
    steps, batch, hidden = x_steps.shape
    rows = steps * batch
    heads = w_q.shape[1] // HEAD_DIM
    kv_heads = w_k.shape[1] // HEAD_DIM
    width = 512
    depth = 4
    vmem = pl.BlockSpec(memory_space=VMEM)
    hbm = pl.BlockSpec(memory_space=pl.ANY)
    return pl.pallas_call(
        functools.partial(project_kernel, width, heads, kv_heads),
        name='project',
        out_shape=(
            jax.ShapeDtypeStruct((rows * heads, HEAD_DIM), F32),
            jax.ShapeDtypeStruct((rows * kv_heads, HEAD_DIM), F32),
            jax.ShapeDtypeStruct((rows * kv_heads, HEAD_DIM), F32),
        ),
        in_specs=[vmem] * 6 + [hbm] * 3,
        out_specs=(vmem, vmem, vmem),
        scratch_shapes=[
            VMEM((hidden // 128, rows, 128), F32),
            VMEM((rows, hidden), BF16),
            VMEM((rows, width), F32),
            VMEM((depth, hidden, width), BF16),
            pltpu.SemaphoreType.DMA((depth,)),
        ],
        compiler_params=pltpu.CompilerParams(vmem_limit_bytes=48 * MIB),
    )(x_steps, norm_gain.reshape(1, -1), cosine, sine, q_gain.reshape(1, -1), k_gain.reshape(1, -1), w_q, w_k, w_v)


def attend_kernel(steps, heads, kv_heads, lens_ref, k_ref, v_ref, q_ref, kn_ref, vn_ref, dist_ref, k_out, v_out, num_ref, stat_ref):
    block, key_rows, _ = k_ref.shape
    slots = key_rows // kv_heads
    batch = lens_ref.shape[0]
    rows = steps * heads
    first_slot = lax.axis_index('sp') * slots
    lane = lax.broadcasted_iota(jnp.int32, (rows, 128), 1)
    upper = lax.broadcasted_iota(jnp.int32, (2 * kv_heads, HEAD_DIM), 0) >= kv_heads
    scale = HEAD_DIM ** -0.5 * math.log2(math.e)

    @pl.when(pl.program_id(0) == 0)
    def _():
        stat_ref[...] = jnp.where(lane < batch, MASKED_MAX, 0.0)

    def one(s, carry):
        b = pl.program_id(0) * block + s
        rel = lens_ref[b] - first_slot
        k_out[s] = k_ref[s]
        v_out[s] = v_ref[s]
        for t in range(steps):
            slot = rel + t

            @pl.when((slot >= 0) & (slot < slots))
            def _():
                base = pl.multiple_of((slot >> 1) * (2 * kv_heads), 2 * kv_heads)
                mine = upper == ((slot & 1) == 1)
                new_rows = pl.ds(pl.multiple_of((s * steps + t) * kv_heads, kv_heads), kv_heads)
                for out, new in ((k_out, kn_ref), (v_out, vn_ref)):
                    fresh = new[new_rows, :]
                    fresh = jnp.concatenate([fresh, fresh], axis=0)
                    old = out[s, pl.ds(base, 2 * kv_heads), :].astype(F32)
                    out[s, pl.ds(base, 2 * kv_heads), :] = jnp.where(mine, fresh, old).astype(BF16)

        out_rows = pl.ds(pl.multiple_of(s * rows, rows), rows)
        visible = rel + steps - 1 >= 0

        @pl.when(visible)
        def _():
            query = q_ref[out_rows, :].astype(BF16)
            scores = lax.dot_general(query, k_out[s], (((1,), (1,)), ((), ())), preferred_element_type=F32)
            scores = jnp.where(dist_ref[...] <= rel, scores, -jnp.inf)
            row_max = jnp.maximum(jnp.max(scores, axis=1, keepdims=True), MASKED_MAX)
            weights = jnp.exp2((scores - row_max) * scale)
            row_sum = jnp.sum(weights, axis=1, keepdims=True)
            num_ref[out_rows, :] = jnp.dot(weights.astype(BF16), v_out[s], preferred_element_type=F32)
            stats = stat_ref[...]
            stats = jnp.where(lane == b, row_max, stats)
            stat_ref[...] = jnp.where(lane == b + batch, row_sum, stats)

        @pl.when(jnp.logical_not(visible))
        def _():
            num_ref[out_rows, :] = jnp.zeros((rows, HEAD_DIM), F32)

        return carry

    lax.fori_loop(0, block, one, 0)


def attend(seq_lens, k_cache, v_cache, queries, k_new, v_new, steps, heads):
    batch, slots, kv_heads, head_dim = k_cache.shape
    rows = steps * heads
    key_rows = slots * kv_heads
    row = jnp.arange(rows, dtype=jnp.int32)
    col = jnp.arange(key_rows, dtype=jnp.int32)
    same_head = ((row % heads) // (heads // kv_heads))[:, None] == (col % kv_heads)[None, :]
    distance = jnp.where(same_head, (col // kv_heads)[None, :] - (row // heads)[:, None], jnp.int32(1 << 24))
    block = 4
    grid_spec = pltpu.PrefetchScalarGridSpec(
        num_scalar_prefetch=1,
        grid=(batch // block,),
        in_specs=[
            pl.BlockSpec((block, key_rows, head_dim), lambda i, _: (i, 0, 0)),
            pl.BlockSpec((block, key_rows, head_dim), lambda i, _: (i, 0, 0)),
            pl.BlockSpec((block * rows, head_dim), lambda i, _: (i, 0)),
            pl.BlockSpec((block * steps * kv_heads, head_dim), lambda i, _: (i, 0)),
            pl.BlockSpec((block * steps * kv_heads, head_dim), lambda i, _: (i, 0)),
            pl.BlockSpec((rows, key_rows), lambda i, _: (0, 0)),
        ],
        out_specs=[
            pl.BlockSpec((block, key_rows, head_dim), lambda i, _: (i, 0, 0)),
            pl.BlockSpec((block, key_rows, head_dim), lambda i, _: (i, 0, 0)),
            pl.BlockSpec((block * rows, head_dim), lambda i, _: (i, 0)),
            pl.BlockSpec((rows, 128), lambda i, _: (0, 0)),
        ],
    )
    k_out, v_out, numer, stats = pl.pallas_call(
        functools.partial(attend_kernel, steps, heads, kv_heads),
        name='attend',
        grid_spec=grid_spec,
        out_shape=[
            jax.ShapeDtypeStruct((batch, key_rows, head_dim), BF16),
            jax.ShapeDtypeStruct((batch, key_rows, head_dim), BF16),
            jax.ShapeDtypeStruct((batch * rows, head_dim), F32),
            jax.ShapeDtypeStruct((rows, 128), F32),
        ],
        compiler_params=pltpu.CompilerParams(vmem_limit_bytes=32 * MIB),
    )(seq_lens, k_cache.reshape(batch, key_rows, head_dim), v_cache.reshape(batch, key_rows, head_dim), queries, k_new, v_new, distance)
    return k_out.reshape(k_cache.shape), v_out.reshape(v_cache.shape), numer, stats


def merge_kernel(chunks, steps, heads, numer, stats, x_ref, wo_hbm, y_ref, wo, stat_d, stat_send, stat_x, recv_d, send_x, recv_x, scaled, attended, projected, y_own, y_other, sems_w, sem_stat, sems_d, sems_x, sems_y):
    _, batch, hidden = y_ref.shape
    q_dim = heads * HEAD_DIM
    rows = steps * heads
    me = lax.axis_index('sp')
    core = lax.rem(me, 2)
    other_core = me + 1 - 2 * core
    other_chip = lax.rem(me + 2, 4)
    half = batch // 2
    own_row = pl.multiple_of(core * (half * rows), half * rows)
    other_row = pl.multiple_of((1 - core) * (half * rows), half * rows)
    own_seq = pl.multiple_of(core * half, half)
    other_seq = pl.multiple_of((1 - core) * half, half)
    seqs = half // chunks
    chunk_rows = seqs * rows

    barrier = pltpu.get_barrier_semaphore()
    for peer in (other_core, other_chip):
        pl.semaphore_signal(barrier, inc=1, device_id={'sp': peer}, device_id_type=pl.DeviceIdType.MESH)
    pl.semaphore_wait(barrier, 2)

    def remote(src, dst, sem, peer):
        return pltpu.make_async_remote_copy(src_ref=src, dst_ref=dst, send_sem=sem.at[0], recv_sem=sem.at[1], device_id={'sp': peer}, device_id_type=pl.DeviceIdType.MESH)

    stat_copy = remote(stats, stat_d, sem_stat.at[0], other_core)
    stat_copy.start()
    core_copies = []
    for c in range(chunks):
        copy = remote(numer.at[pl.ds(other_row + c * chunk_rows, chunk_rows), :], recv_d.at[pl.ds(c * chunk_rows, chunk_rows), :], sems_d.at[c], other_core)
        copy.start()
        core_copies.append(copy)
    w_pieces = sems_w.shape[0]
    w_rows = q_dim // w_pieces
    w_copies = []
    for p in range(w_pieces):
        copy = pltpu.make_async_copy(wo_hbm.at[pl.ds(p * w_rows, w_rows), :], wo.at[pl.ds(p * w_rows, w_rows), :], sems_w.at[p])
        copy.start()
        w_copies.append(copy)
    for t in range(steps):
        y_own[t] = x_ref[t, pl.ds(own_seq, half), :].astype(F32)

    lane = lax.broadcasted_iota(jnp.int32, (rows, 128), 1)

    def mine(values):
        return jnp.where(core == 1, pltpu.roll(values, 128 - half, 1), values)

    stat_copy.wait()
    max_a, max_b = stats[...], stat_d[...]
    sum_a, sum_b = pltpu.roll(max_a, 128 - batch, 1), pltpu.roll(max_b, 128 - batch, 1)
    chip_max = jnp.maximum(max_a, max_b)
    scale = HEAD_DIM ** -0.5
    fac_a, fac_b = jnp.exp((max_a - chip_max) * scale), jnp.exp((max_b - chip_max) * scale)
    chip_sum = sum_a * fac_a + sum_b * fac_b
    stat_send[...] = jnp.where(lane < batch, chip_max, pltpu.roll(chip_sum, batch, 1))
    chip_stat_copy = remote(stat_send, stat_x, sem_stat.at[1], other_chip)
    chip_stat_copy.start()
    scaled[0] = mine(fac_a)
    scaled[1] = mine(fac_b)

    chip_copies = []
    for c in range(chunks):
        core_copies[c].wait()
        for s in range(seqs):
            index = c * seqs + s
            here = pl.ds(index * rows, rows)
            send_x[here, :] = numer[pl.ds(own_row + index * rows, rows), :] * scaled[0, :, index:index + 1] + recv_d[here, :] * scaled[1, :, index:index + 1]
        here = pl.ds(c * chunk_rows, chunk_rows)
        copy = remote(send_x.at[here, :], recv_x.at[here, :], sems_x.at[c], other_chip)
        copy.start()
        chip_copies.append(copy)

    chip_stat_copy.wait()
    max_a, max_b = stat_send[...], stat_x[...]
    sum_a, sum_b = pltpu.roll(max_a, 128 - batch, 1), pltpu.roll(max_b, 128 - batch, 1)
    full_max = jnp.maximum(max_a, max_b)
    fac_a, fac_b = jnp.exp((max_a - full_max) * scale), jnp.exp((max_b - full_max) * scale)
    full_sum = sum_a * fac_a + sum_b * fac_b
    scaled[0] = mine(fac_a / full_sum)
    scaled[1] = mine(fac_b / full_sum)

    width = 512
    y_copies = []
    for c in range(chunks):
        chip_copies[c].wait()
        for s in range(seqs):
            index = c * seqs + s
            here = pl.ds(index * rows, rows)
            recv_x[here, :] = send_x[here, :] * scaled[0, :, index:index + 1] + recv_x[here, :] * scaled[1, :, index:index + 1]
        for h in range(heads):
            values = recv_x[pl.ds(c * chunk_rows + h, seqs * steps, stride=heads), :]
            attended[:, h * HEAD_DIM:(h + 1) * HEAD_DIM] = values.astype(BF16)
        if c == 0:
            for copy in w_copies:
                copy.wait()

        @pl.loop(0, hidden // width)
        def _(j):
            cols = pl.ds(pl.multiple_of(j * width, width), width)
            out = jnp.dot(attended[...], wo[:, cols], preferred_element_type=F32)
            for i in range(width // 128):
                projected[i] = out[:, i * 128:(i + 1) * 128]
            for i in range(width // 128):
                piece = pl.ds(pl.multiple_of(j * width + i * 128, 128), 128)
                for t in range(steps):
                    y_own[t, c * seqs:(c + 1) * seqs, piece] += projected[i, pl.ds(t, seqs, stride=steps), :]

        there = pl.ds(c * seqs, seqs)
        copy = remote(y_own.at[:, there, :], y_other.at[:, there, :], sems_y.at[c], other_core)
        copy.start()
        y_copies.append(copy)

    for t in range(steps):
        y_ref[t, pl.ds(own_seq, half), :] = y_own[t].astype(BF16)
    for copy in y_copies:
        copy.wait()
    for t in range(steps):
        y_ref[t, pl.ds(other_seq, half), :] = y_other[t].astype(BF16)


def merge(numer, stats, x_steps, w_o):
    steps, batch, hidden = x_steps.shape
    heads = w_o.shape[0] // HEAD_DIM
    rows = steps * heads
    chunks = 4
    seqs = batch // 2 // chunks
    vmem = pl.BlockSpec(memory_space=VMEM)
    half_rows = batch // 2 * rows
    return pl.pallas_call(
        functools.partial(merge_kernel, chunks, steps, heads),
        name='merge',
        out_shape=jax.ShapeDtypeStruct(x_steps.shape, BF16),
        in_specs=[vmem, vmem, vmem, pl.BlockSpec(memory_space=pl.ANY)],
        out_specs=vmem,
        scratch_shapes=[
            VMEM(w_o.shape, BF16),
            VMEM((rows, 128), F32),
            VMEM((rows, 128), F32),
            VMEM((rows, 128), F32),
            VMEM((half_rows, HEAD_DIM), F32),
            VMEM((half_rows, HEAD_DIM), F32),
            VMEM((half_rows, HEAD_DIM), F32),
            VMEM((2, rows, 128), F32),
            VMEM((seqs * steps, heads * HEAD_DIM), BF16),
            VMEM((4, seqs * steps, 128), F32),
            VMEM((steps, batch // 2, hidden), F32),
            VMEM((steps, batch // 2, hidden), F32),
            pltpu.SemaphoreType.DMA((8,)),
            pltpu.SemaphoreType.DMA((2, 2)),
            pltpu.SemaphoreType.DMA((chunks, 2)),
            pltpu.SemaphoreType.DMA((chunks, 2)),
            pltpu.SemaphoreType.DMA((chunks, 2)),
        ],
        compiler_params=pltpu.CompilerParams(collective_id=0, has_side_effects=True, vmem_limit_bytes=62 * MIB),
    )(numer, stats, x_steps, w_o)


def solution(mesh):
    def per_device(x_steps, k_local, v_local, seq_lens, norm_gain, w_q, w_k, w_v, w_o, q_gain, k_gain):
        steps = x_steps.shape[0]
        heads = w_q.shape[1] // HEAD_DIM
        cosine, sine = rope_tables(seq_lens, steps)
        queries, keys_new, vals_new = project(x_steps, norm_gain, cosine, sine, q_gain, k_gain, w_q, w_k, w_v)
        k_out, v_out, numer, stats = attend(seq_lens, k_local, v_local, queries, keys_new, vals_new, steps, heads)
        y_steps = merge(numer, stats, x_steps, w_o)
        return y_steps, k_out, v_out

    cache_spec = P('dp', 'sp', None, None)
    step_spec = P(None, 'dp', None)
    return jax.shard_map(per_device, mesh=mesh, in_specs=(step_spec, cache_spec, cache_spec, P('dp'), P(), P(), P(), P(), P(), P(), P()), out_specs=(step_spec, cache_spec, cache_spec), check_vma=False)
```

```python
import functools
import math

import jax
import jax.numpy as jnp
from jax import lax
from jax.experimental import pallas as pl
from jax.experimental.pallas import tpu as pltpu
from jax.sharding import PartitionSpec as P

NORM_EPS = 1e-6
ROPE_BASE = 1000000.0
MASKED_MAX = -1e30
HEAD_DIM = 128
F32 = jnp.float32
BF16 = jnp.bfloat16
MIB = 1024 * 1024
VMEM = pltpu.VMEM
DMA = pltpu.SemaphoreType.DMA
IN_VMEM = pl.BlockSpec(memory_space=VMEM)
IN_PLACE = pl.BlockSpec(memory_space=pl.ANY)


def small_tables(seq_lens, steps, norm_gain, q_gain, k_gain):
    half = HEAD_DIM // 2
    positions = (seq_lens[None, :] + jnp.arange(steps, dtype=jnp.int32)[:, None]).reshape(-1)
    inv_freq = jnp.exp(jnp.arange(half, dtype=F32) * (-2.0 * math.log(ROPE_BASE) / HEAD_DIM))
    angles = positions.astype(F32)[:, None] * inv_freq
    cosine = jnp.cos(angles)
    sine = jnp.sin(angles)
    rope = jnp.concatenate([jnp.concatenate([cosine, cosine], axis=-1), jnp.concatenate([-sine, sine], axis=-1)], axis=0)
    gains = jnp.concatenate([norm_gain, q_gain, k_gain]).astype(F32).reshape(-1, HEAD_DIM)
    return rope, gains


def remote(src, dst, sems, peer):
    return pltpu.make_async_remote_copy(src_ref=src, dst_ref=dst, send_sem=sems.at[0], recv_sem=sems.at[1], device_id={'sp': peer}, device_id_type=pl.DeviceIdType.MESH)


def meet(*peers):
    barrier = pltpu.get_barrier_semaphore()
    for peer in peers:
        pl.semaphore_signal(barrier, inc=1, device_id={'sp': peer}, device_id_type=pl.DeviceIdType.MESH)
    pl.semaphore_wait(barrier, len(peers))


def project_kernel(width, heads, kv_heads, x_hbm, rope_ref, gain_ref, wq_hbm, wk_hbm, wv_hbm, q_ref, k_ref, v_ref, x_rows, normed, acc, wbuf, sem_x, sems_w, sems_q, sems_k, sems_v):
    rows, hidden = x_rows.shape
    per_block = width // HEAD_DIM
    core = lax.rem(lax.axis_index('sp'), 2)
    other_core = lax.axis_index('sp') + 1 - 2 * core

    x_copy = pltpu.make_async_copy(x_hbm, x_rows, sem_x)
    x_copy.start()
    blocks = [(wk_hbm, k_ref, sems_k, kv_heads, 0)]
    blocks += [(wq_hbm, q_ref, sems_q, heads, i) for i in range(heads // 2 // per_block)]
    blocks += [(wv_hbm, v_ref, sems_v, kv_heads, 0)]
    w_copies = []
    for n, (w_hbm, _, _, total, i) in enumerate(blocks):
        cols = pl.ds(pl.multiple_of(core * (total // 2 * HEAD_DIM) + i * width, width), width)
        copy = pltpu.make_async_copy(w_hbm.at[:, cols], wbuf.at[n], sems_w.at[n])
        copy.start()
        w_copies.append(copy)

    meet(other_core)
    x_copy.wait()

    @pl.loop(0, rows // 16)
    def _(i):
        here = pl.ds(pl.multiple_of(i * 16, 16), 16)
        values = x_rows[here, :].astype(F32)
        inv_rms = lax.rsqrt(jnp.mean(values * values, axis=-1, keepdims=True) + NORM_EPS)
        for n in range(hidden // HEAD_DIM):
            lanes = slice(n * HEAD_DIM, (n + 1) * HEAD_DIM)
            normed[here, lanes] = (x_rows[here, lanes].astype(F32) * inv_rms * gain_ref[n:n + 1, :]).astype(BF16)

    def finish(n):
        w_hbm, out_ref, sems, total, i = blocks[n]
        first = core * (total // 2) + i * per_block
        for j in range(per_block):
            values = acc[n % 2, :, j * HEAD_DIM:(j + 1) * HEAD_DIM].astype(BF16).astype(F32)
            if out_ref is not v_ref:
                row = hidden // HEAD_DIM + (1 if out_ref is k_ref else 0)
                inv_rms = lax.rsqrt(jnp.mean(values * values, axis=-1, keepdims=True) + NORM_EPS)
                scaled = values * inv_rms * gain_ref[row:row + 1, :]
                values = scaled * rope_ref[:rows, :] + pltpu.roll(scaled, HEAD_DIM // 2, 1) * rope_ref[rows:, :]
                values = values.astype(BF16).astype(F32)
            out_ref[:, first + j, :, :] = values.reshape(rows // 8, 8, HEAD_DIM)

    def send(n):
        _, out_ref, sems, total, i = blocks[n]
        there = pl.ds(core * (total // 2) + i * per_block, per_block)
        copy = remote(out_ref.at[:, there], out_ref.at[:, there], sems.at[i], other_core)
        copy.start()
        return copy

    sends = []
    for n in range(len(blocks)):
        w_copies[n].wait()
        acc[n % 2] = jnp.dot(normed[...], wbuf[n], preferred_element_type=F32)
        if n > 0:
            finish(n - 1)
            sends.append(send(n - 1))
    finish(len(blocks) - 1)
    sends.append(send(len(blocks) - 1))
    for copy in sends:
        copy.wait()


def project(x_steps, rope, gains, w_q, w_k, w_v):
    steps, batch, hidden = x_steps.shape
    rows = steps * batch
    heads = w_q.shape[1] // HEAD_DIM
    kv_heads = w_k.shape[1] // HEAD_DIM
    width = kv_heads // 2 * HEAD_DIM
    q_blocks = heads // kv_heads
    return pl.pallas_call(
        functools.partial(project_kernel, width, heads, kv_heads),
        name='project',
        out_shape=tuple(jax.ShapeDtypeStruct((rows // 8, n, 8, HEAD_DIM), F32) for n in (heads, kv_heads, kv_heads)),
        in_specs=[IN_PLACE, IN_VMEM, IN_VMEM] + [IN_PLACE] * 3,
        out_specs=(IN_VMEM,) * 3,
        scratch_shapes=[
            VMEM((rows, hidden), BF16),
            VMEM((rows, hidden), BF16),
            VMEM((2, rows, width), F32),
            VMEM((q_blocks + 2, hidden, width), BF16),
            DMA,
            DMA((q_blocks + 2,)),
            DMA((q_blocks, 2)),
            DMA((1, 2)),
            DMA((1, 2)),
        ],
        compiler_params=pltpu.CompilerParams(collective_id=1, has_side_effects=True, vmem_limit_bytes=40 * MIB),
    )(x_steps.reshape(rows, hidden), rope, gains, w_q, w_k, w_v)


def attend_kernel(steps, group, depth, lens_ref, k_hbm, v_hbm, q_ref, kn_ref, vn_ref, ko_hbm, vo_hbm, num_ref, stat_ref, k_buf, v_buf, dist, sems_in, sems_out):
    slots_held, _, key_rows, _ = k_buf.shape
    batch = lens_ref.shape[0]
    heads, kv_heads = q_ref.shape[0] // (steps * batch), kn_ref.shape[0] // (steps * batch)
    slots = key_rows // kv_heads
    rows = steps * heads
    half = heads // 2
    first_slot = lax.axis_index('sp') * slots
    lane = lax.broadcasted_iota(jnp.int32, (rows, 128), 1)
    upper = lax.broadcasted_iota(jnp.int32, (2 * kv_heads, HEAD_DIM), 0) >= kv_heads
    scale = HEAD_DIM ** -0.5 * math.log2(math.e)
    groups = batch // group

    def copies_in(g, slot):
        here = pl.ds(g * group, group)
        return (pltpu.make_async_copy(k_hbm.at[here], k_buf.at[slot], sems_in.at[slot, 0]),
                pltpu.make_async_copy(v_hbm.at[here], v_buf.at[slot], sems_in.at[slot, 1]))

    def copies_out(g, slot):
        here = pl.ds(g * group, group)
        return (pltpu.make_async_copy(k_buf.at[slot], ko_hbm.at[here], sems_out.at[slot, 0]),
                pltpu.make_async_copy(v_buf.at[slot], vo_hbm.at[here], sems_out.at[slot, 1]))

    for g in range(depth):
        for copy in copies_in(g, g):
            copy.start()

    stat_ref[...] = jnp.where(lane < batch, MASKED_MAX, 0.0)
    row = lax.broadcasted_iota(jnp.int32, (rows, key_rows), 0)
    col = lax.broadcasted_iota(jnp.int32, (rows, key_rows), 1)
    row_half, in_half = row // (steps * half), lax.rem(row, steps * half)
    row_kv = (row_half * half + lax.rem(in_half, half)) // (heads // kv_heads)
    dist[...] = jnp.where(row_kv == lax.rem(col, kv_heads), col // kv_heads - in_half // half, 1 << 24)

    def one_group(g, carry):
        slot = lax.rem(g, slots_held)
        for copy in copies_in(g, slot):
            copy.wait()

        for s in range(group):
            b = g * group + s
            rel = lens_ref[b] - first_slot
            for t in range(steps):
                at = rel + t

                @pl.when((at >= 0) & (at < slots))
                def _():
                    base = pl.multiple_of((at >> 1) * (2 * kv_heads), 2 * kv_heads)
                    mine = upper == ((at & 1) == 1)
                    r = t * batch + b
                    new_rows = pl.ds((r >> 3) * (8 * kv_heads) + (r & 7), kv_heads, stride=8)
                    for buf, new in ((k_buf, kn_ref), (v_buf, vn_ref)):
                        fresh = new[new_rows, :]
                        fresh = jnp.concatenate([fresh, fresh], axis=0)
                        old = buf[slot, s, pl.ds(base, 2 * kv_heads), :].astype(F32)
                        buf[slot, s, pl.ds(base, 2 * kv_heads), :] = jnp.where(mine, fresh, old).astype(BF16)

        rels = [lens_ref[g * group + s] - first_slot for s in range(group)]
        longest = functools.reduce(jnp.maximum, rels)
        visible = longest + steps - 1 >= 0

        @pl.when(visible)
        def _():
            stats = stat_ref[...]
            for s in range(group):
                b = g * group + s
                pieces = []
                for h in range(2):
                    for t in range(steps):
                        r = t * batch + b
                        start = (r >> 3) * (8 * heads) + (r & 7) + h * (8 * half)
                        pieces.append(q_ref[pl.ds(start, half, stride=8), :].astype(BF16))
                query = jnp.concatenate(pieces, axis=0)
                scores = lax.dot_general(query, k_buf[slot, s], (((1,), (1,)), ((), ())), preferred_element_type=F32)
                scores = jnp.where(dist[...] <= rels[s], scores, -jnp.inf)
                row_max = jnp.maximum(jnp.max(scores, axis=1, keepdims=True), MASKED_MAX)
                weights = jnp.exp2((scores - row_max) * scale)
                row_sum = jnp.sum(weights, axis=1, keepdims=True)
                num_ref[b] = jnp.dot(weights.astype(BF16), v_buf[slot, s], preferred_element_type=F32)
                stats = jnp.where(lane == b, row_max, stats)
                stats = jnp.where(lane == b + batch, row_sum, stats)
            stat_ref[...] = stats

        @pl.when(jnp.logical_not(visible))
        def _():
            for s in range(group):
                num_ref[g * group + s] = jnp.zeros((rows, HEAD_DIM), F32)

        for copy in copies_out(g, slot):
            copy.start()
        ahead = g + depth
        next_slot = lax.rem(ahead, slots_held)

        @pl.when(ahead < groups)
        def _():
            @pl.when(ahead >= slots_held)
            def _():
                for copy in copies_out(ahead - slots_held, next_slot):
                    copy.wait()

            for copy in copies_in(ahead, next_slot):
                copy.start()

        return carry

    lax.fori_loop(0, groups, one_group, 0)
    for g in range(groups - slots_held, groups):
        for copy in copies_out(g, g % slots_held):
            copy.wait()


def attend(seq_lens, k_cache, v_cache, queries, k_new, v_new, steps):
    batch, slots, kv_heads, head_dim = k_cache.shape
    heads = queries.shape[1]
    rows = steps * heads
    key_rows = slots * kv_heads
    group, depth, held = 2, 5, 8
    cache = jax.ShapeDtypeStruct((batch, key_rows, head_dim), BF16)
    k_out, v_out, numer, stats = pl.pallas_call(
        functools.partial(attend_kernel, steps, group, depth),
        name='attend',
        in_specs=[pl.BlockSpec(memory_space=pltpu.SMEM), IN_PLACE, IN_PLACE, IN_VMEM, IN_VMEM, IN_VMEM],
        out_specs=(IN_PLACE, IN_PLACE, IN_VMEM, IN_VMEM),
        out_shape=(cache, cache, jax.ShapeDtypeStruct((batch, rows, head_dim), F32), jax.ShapeDtypeStruct((rows, 128), F32)),
        scratch_shapes=[
            VMEM((held, group, key_rows, head_dim), BF16),
            VMEM((held, group, key_rows, head_dim), BF16),
            VMEM((rows, key_rows), jnp.int32),
            DMA((held, 2)),
            DMA((held, 2)),
        ],
        compiler_params=pltpu.CompilerParams(vmem_limit_bytes=32 * MIB),
    )(seq_lens, k_cache.reshape(batch, key_rows, head_dim), v_cache.reshape(batch, key_rows, head_dim), queries.reshape(-1, head_dim), k_new.reshape(-1, head_dim), v_new.reshape(-1, head_dim))
    return k_out.reshape(k_cache.shape), v_out.reshape(v_cache.shape), numer, stats


def merge_kernel(chunks, steps, numer, stats, wo_hbm, y_own, y_other, wo, stat_d, stat_send, stat_x, recv_d, send_x, recv_x, scaled, att_f32, attended, sems_w, sem_stat, sems_d, sems_x, sems_y):
    _, batch, hidden = y_own.shape
    rows = numer.shape[1] // 2
    half = rows // steps
    me = lax.axis_index('sp')
    core = lax.rem(me, 2)
    other_core = me + 1 - 2 * core
    other_chip = lax.rem(me + 2, 4)
    own = pl.ds(pl.multiple_of(core * rows, rows), rows)
    other = pl.ds(pl.multiple_of((1 - core) * rows, rows), rows)
    firsts = [sum(chunks[:c]) for c in range(len(chunks))]

    w_pieces = sems_w.shape[0]
    w_rows = half * HEAD_DIM // w_pieces
    w_first = core * (half * HEAD_DIM)
    meet(other_core, other_chip)

    stat_copy = remote(stats.at[other], stat_d, sem_stat.at[0], other_core)
    stat_copy.start()
    core_copies = []
    for c, (first, seqs) in enumerate(zip(firsts, chunks)):
        here = pl.ds(first, seqs)
        copy = remote(numer.at[here, other], recv_d.at[here], sems_d.at[c], other_core)
        copy.start()
        core_copies.append(copy)
    w_copies = []
    for p in range(w_pieces):
        src = wo_hbm.at[pl.ds(pl.multiple_of(w_first + p * w_rows, w_rows), w_rows), :]
        copy = pltpu.make_async_copy(src, wo.at[pl.ds(p * w_rows, w_rows), :], sems_w.at[p])
        copy.start()
        w_copies.append(copy)

    lane = lax.broadcasted_iota(jnp.int32, (rows, 128), 1)
    scale = HEAD_DIM ** -0.5

    def combine(mine, theirs):
        top = jnp.maximum(mine, theirs)
        fac_a, fac_b = jnp.exp((mine - top) * scale), jnp.exp((theirs - top) * scale)
        total = pltpu.roll(mine, 128 - batch, 1) * fac_a + pltpu.roll(theirs, 128 - batch, 1) * fac_b
        return top, fac_a, fac_b, total

    stat_copy.wait()
    top, fac_a, fac_b, total = combine(stats[own, :], stat_d[...])
    stat_send[...] = jnp.where(lane < batch, top, pltpu.roll(total, batch, 1))
    scaled[0] = fac_a
    scaled[1] = fac_b
    chip_stat_copy = remote(stat_send, stat_x, sem_stat.at[1], other_chip)
    chip_stat_copy.start()

    chip_copies = []
    for c, (first, seqs) in enumerate(zip(firsts, chunks)):
        core_copies[c].wait()
        for b in range(first, first + seqs):
            send_x[b] = numer[b, own, :] * scaled[0, :, b:b + 1] + recv_d[b] * scaled[1, :, b:b + 1]
        here = pl.ds(first, seqs)
        copy = remote(send_x.at[here], recv_x.at[here], sems_x.at[c], other_chip)
        copy.start()
        chip_copies.append(copy)

    chip_stat_copy.wait()
    _, fac_a, fac_b, total = combine(stat_send[...], stat_x[...])
    scaled[0] = fac_a / total
    scaled[1] = fac_b / total

    width = 512
    y_copies = []
    for c, (first, seqs) in enumerate(zip(firsts, chunks)):
        chip_copies[c].wait()
        for b in range(first, first + seqs):
            merged = send_x[b] * scaled[0, :, b:b + 1] + recv_x[b] * scaled[1, :, b:b + 1]
            att_f32[pl.ds((b - first) * rows, rows), :] = merged
        for t in range(steps):
            for h in range(half):
                values = att_f32[pl.ds(t * half + h, seqs, stride=rows), :]
                attended[t * seqs:(t + 1) * seqs, h * HEAD_DIM:(h + 1) * HEAD_DIM] = values
        if c == 0:
            for copy in w_copies:
                copy.wait()

        @pl.loop(0, hidden // width)
        def _(j):
            cols = pl.ds(pl.multiple_of(j * width, width), width)
            out = jnp.dot(attended[:steps * seqs, :].astype(BF16), wo[:, cols], preferred_element_type=F32)
            for t in range(steps):
                y_own[t, first:first + seqs, cols] = out[t * seqs:(t + 1) * seqs, :]

        here = pl.ds(first, seqs)
        copy = remote(y_own.at[:, here, :], y_other.at[:, here, :], sems_y.at[c], other_core)
        copy.start()
        y_copies.append(copy)
    for copy in y_copies:
        copy.wait()


def merge(numer, stats, w_o, steps):
    batch, rows, _ = numer.shape
    hidden = w_o.shape[1]
    chunks = (16, 16, 16, 8, 8)
    largest = max(chunks)
    part = jax.ShapeDtypeStruct((steps, batch, hidden), F32)
    stat = VMEM((rows // 2, 128), F32)
    return pl.pallas_call(
        functools.partial(merge_kernel, chunks, steps),
        name='merge',
        out_shape=(part, part),
        in_specs=[IN_VMEM, IN_VMEM, IN_PLACE],
        out_specs=(IN_VMEM, IN_VMEM),
        scratch_shapes=[
            VMEM((w_o.shape[0] // 2, hidden), BF16),
            stat,
            stat,
            stat,
            VMEM((batch, rows // 2, HEAD_DIM), F32),
            VMEM((batch, rows // 2, HEAD_DIM), F32),
            VMEM((batch, rows // 2, HEAD_DIM), F32),
            VMEM((2, rows // 2, 128), F32),
            VMEM((largest * rows // 2, HEAD_DIM), F32),
            VMEM((steps * largest, w_o.shape[0] // 2), F32),
            DMA((8,)),
            DMA((2, 2)),
            DMA((len(chunks), 2)),
            DMA((len(chunks), 2)),
            DMA((len(chunks), 2)),
        ],
        compiler_params=pltpu.CompilerParams(collective_id=0, has_side_effects=True, vmem_limit_bytes=40 * MIB),
    )(numer, stats, w_o)


def solution(mesh):
    def per_device(x_steps, k_local, v_local, seq_lens, norm_gain, w_q, w_k, w_v, w_o, q_gain, k_gain):
        steps = x_steps.shape[0]
        rope, gains = small_tables(seq_lens, steps, norm_gain, q_gain, k_gain)
        queries, keys_new, vals_new = project(x_steps, rope, gains, w_q, w_k, w_v)
        k_out, v_out, numer, stats = attend(seq_lens, k_local, v_local, queries, keys_new, vals_new, steps)
        own, other = merge(numer, stats, w_o, steps)
        y_steps = (x_steps.astype(F32) + (own + other)).astype(BF16)
        return y_steps, k_out, v_out

    cache_spec = P('dp', 'sp', None, None)
    step_spec = P(None, 'dp', None)
    return jax.shard_map(per_device, mesh=mesh, in_specs=(step_spec, cache_spec, cache_spec, P('dp'), P(), P(), P(), P(), P(), P(), P()), out_specs=(step_spec, cache_spec, cache_spec), check_vma=False)
```

```python
import functools
import math

import jax
import jax.numpy as jnp
from jax import lax
from jax.experimental import pallas as pl
from jax.experimental.pallas import tpu as pltpu
from jax.sharding import PartitionSpec as P

NORM_EPS = 1e-6
ROPE_BASE = 1000000.0
MASKED_MAX = -1e30
HEAD_DIM = 128
F32 = jnp.float32
BF16 = jnp.bfloat16
MIB = 1024 * 1024
VMEM = pltpu.VMEM
DMA = pltpu.SemaphoreType.DMA
IN_VMEM = pl.BlockSpec(memory_space=VMEM)
IN_PLACE = pl.BlockSpec(memory_space=pl.ANY)


def small_tables(seq_lens, steps, norm_gain, q_gain, k_gain):
    half = HEAD_DIM // 2
    positions = (seq_lens[None, :] + jnp.arange(steps, dtype=jnp.int32)[:, None]).reshape(-1)
    inv_freq = jnp.exp(jnp.arange(half, dtype=F32) * (-2.0 * math.log(ROPE_BASE) / HEAD_DIM))
    angles = positions.astype(F32)[:, None] * inv_freq
    cosine = jnp.cos(angles)
    sine = jnp.sin(angles)
    rope = jnp.concatenate([jnp.concatenate([cosine, cosine], axis=-1), jnp.concatenate([-sine, sine], axis=-1)], axis=0)
    gains = jnp.concatenate([norm_gain, q_gain, k_gain]).astype(F32).reshape(-1, HEAD_DIM)
    return rope, gains


def remote(src, dst, sems, peer):
    return pltpu.make_async_remote_copy(src_ref=src, dst_ref=dst, send_sem=sems.at[0], recv_sem=sems.at[1], device_id={'sp': peer}, device_id_type=pl.DeviceIdType.MESH)


def meet(*peers):
    barrier = pltpu.get_barrier_semaphore()
    for peer in peers:
        pl.semaphore_signal(barrier, inc=1, device_id={'sp': peer}, device_id_type=pl.DeviceIdType.MESH)
    pl.semaphore_wait(barrier, len(peers))


def project_kernel(width, heads, kv_heads, x_hbm, rope_ref, gain_ref, wq_hbm, wk_hbm, wv_hbm, q_ref, k_ref, v_ref, x_rows, normed, acc, wbuf, sem_x, sems_w, sems_q, sems_k, sems_v):
    rows, hidden = x_rows.shape
    per_block = width // HEAD_DIM
    core = lax.rem(lax.axis_index('sp'), 2)
    other_core = lax.axis_index('sp') + 1 - 2 * core

    x_copy = pltpu.make_async_copy(x_hbm, x_rows, sem_x)
    x_copy.start()
    blocks = [(wk_hbm, k_ref, sems_k, kv_heads, 0)]
    blocks += [(wq_hbm, q_ref, sems_q, heads, i) for i in range(heads // 2 // per_block)]
    blocks += [(wv_hbm, v_ref, sems_v, kv_heads, 0)]
    w_copies = []
    for n, (w_hbm, _, _, total, i) in enumerate(blocks):
        cols = pl.ds(pl.multiple_of(core * (total // 2 * HEAD_DIM) + i * width, width), width)
        copy = pltpu.make_async_copy(w_hbm.at[:, cols], wbuf.at[n], sems_w.at[n])
        copy.start()
        w_copies.append(copy)

    meet(other_core)
    x_copy.wait()

    @pl.loop(0, rows // 16)
    def _(i):
        here = pl.ds(pl.multiple_of(i * 16, 16), 16)
        values = x_rows[here, :].astype(F32)
        inv_rms = lax.rsqrt(jnp.mean(values * values, axis=-1, keepdims=True) + NORM_EPS)
        for n in range(hidden // HEAD_DIM):
            lanes = slice(n * HEAD_DIM, (n + 1) * HEAD_DIM)
            normed[here, lanes] = (x_rows[here, lanes].astype(F32) * inv_rms * gain_ref[n:n + 1, :]).astype(BF16)

    def finish(n):
        w_hbm, out_ref, sems, total, i = blocks[n]
        first = core * (total // 2) + i * per_block
        for j in range(per_block):
            values = acc[n % 2, :, j * HEAD_DIM:(j + 1) * HEAD_DIM].astype(BF16).astype(F32)
            if out_ref is not v_ref:
                row = hidden // HEAD_DIM + (1 if out_ref is k_ref else 0)
                inv_rms = lax.rsqrt(jnp.mean(values * values, axis=-1, keepdims=True) + NORM_EPS)
                scaled = values * inv_rms * gain_ref[row:row + 1, :]
                values = scaled * rope_ref[:rows, :] + pltpu.roll(scaled, HEAD_DIM // 2, 1) * rope_ref[rows:, :]
                values = values.astype(BF16).astype(F32)
            out_ref[:, first + j, :, :] = values.reshape(rows // 8, 8, HEAD_DIM)

    def send(n):
        _, out_ref, sems, total, i = blocks[n]
        there = pl.ds(core * (total // 2) + i * per_block, per_block)
        copy = remote(out_ref.at[:, there], out_ref.at[:, there], sems.at[i], other_core)
        copy.start()
        return copy

    sends = []
    for n in range(len(blocks)):
        w_copies[n].wait()
        acc[n % 2] = jnp.dot(normed[...], wbuf[n], preferred_element_type=F32)
        if n > 0:
            finish(n - 1)
            sends.append(send(n - 1))
    finish(len(blocks) - 1)
    sends.append(send(len(blocks) - 1))
    for copy in sends:
        copy.wait()


def project(x_steps, rope, gains, w_q, w_k, w_v):
    steps, batch, hidden = x_steps.shape
    rows = steps * batch
    heads = w_q.shape[1] // HEAD_DIM
    kv_heads = w_k.shape[1] // HEAD_DIM
    width = kv_heads // 2 * HEAD_DIM
    q_blocks = heads // kv_heads
    return pl.pallas_call(
        functools.partial(project_kernel, width, heads, kv_heads),
        name='project',
        out_shape=tuple(jax.ShapeDtypeStruct((rows // 8, n, 8, HEAD_DIM), F32) for n in (heads, kv_heads, kv_heads)),
        in_specs=[pl.BlockSpec(memory_space=pltpu.HBM), IN_VMEM, IN_VMEM] + [IN_PLACE] * 3,
        out_specs=(IN_VMEM,) * 3,
        scratch_shapes=[
            VMEM((rows, hidden), BF16),
            VMEM((rows, hidden), BF16),
            VMEM((2, rows, width), F32),
            VMEM((q_blocks + 2, hidden, width), BF16),
            DMA,
            DMA((q_blocks + 2,)),
            DMA((q_blocks, 2)),
            DMA((1, 2)),
            DMA((1, 2)),
        ],
        compiler_params=pltpu.CompilerParams(collective_id=1, has_side_effects=True, vmem_limit_bytes=40 * MIB),
    )(x_steps.reshape(rows, hidden), rope, gains, w_q, w_k, w_v)


def attend_kernel(steps, depth, lens_ref, k_hbm, v_hbm, q_ref, kn_ref, vn_ref, ko_hbm, vo_hbm, num_ref, stat_ref, k_buf, v_buf, dist, scores_0, scores_1, weights_0, weights_1, sems_in, sems_out):
    held, key_rows, _ = k_buf.shape
    batch = lens_ref.shape[0]
    heads, kv_heads = q_ref.shape[0] // (steps * batch), kn_ref.shape[0] // (steps * batch)
    slots = key_rows // kv_heads
    rows = steps * heads
    half = heads // 2
    first_slot = lax.axis_index('sp') * slots
    upper = lax.broadcasted_iota(jnp.int32, (2 * kv_heads, HEAD_DIM), 0) >= kv_heads
    scale = HEAD_DIM ** -0.5 * math.log2(math.e)
    scores_refs, weights_refs = (scores_0, scores_1), (weights_0, weights_1)

    def copies_in(b):
        slot = lax.rem(b, held)
        return (pltpu.make_async_copy(k_hbm.at[b], k_buf.at[slot], sems_in.at[slot, 0]),
                pltpu.make_async_copy(v_hbm.at[b], v_buf.at[slot], sems_in.at[slot, 1]))

    def copies_out(b):
        slot = lax.rem(b, held)
        return (pltpu.make_async_copy(k_buf.at[slot], ko_hbm.at[b], sems_out.at[slot, 0]),
                pltpu.make_async_copy(v_buf.at[slot], vo_hbm.at[b], sems_out.at[slot, 1]))

    for b in range(depth):
        for copy in copies_in(b):
            copy.start()

    lane = lax.broadcasted_iota(jnp.int32, (rows, 128), 1)
    stat_ref[...] = jnp.where(lane < batch, MASKED_MAX, 0.0)
    row = lax.broadcasted_iota(jnp.int32, (rows, key_rows), 0)
    col = lax.broadcasted_iota(jnp.int32, (rows, key_rows), 1)
    row_half, in_half = row // (steps * half), lax.rem(row, steps * half)
    row_kv = (row_half * half + lax.rem(in_half, half)) // (heads // kv_heads)
    dist[...] = jnp.where(row_kv == lax.rem(col, kv_heads), col // kv_heads - in_half // half, 1 << 24)

    def rel_of(b):
        return lens_ref[jnp.clip(b, 0, batch - 1)] - first_slot

    def receive(b):
        slot = lax.rem(b, held)
        for copy in copies_in(b):
            copy.wait()
        rel = rel_of(b)
        for t in range(steps):
            at = rel + t

            @pl.when((at >= 0) & (at < slots))
            def _():
                base = pl.multiple_of((at >> 1) * (2 * kv_heads), 2 * kv_heads)
                mine = upper == ((at & 1) == 1)
                r = t * batch + b
                new_rows = pl.ds((r >> 3) * (8 * kv_heads) + (r & 7), kv_heads, stride=8)
                for buf, new in ((k_buf, kn_ref), (v_buf, vn_ref)):
                    fresh = new[new_rows, :]
                    fresh = jnp.concatenate([fresh, fresh], axis=0)
                    old = buf[slot, pl.ds(base, 2 * kv_heads), :].astype(F32)
                    buf[slot, pl.ds(base, 2 * kv_heads), :] = jnp.where(mine, fresh, old).astype(BF16)

    def score(j, parity):
        b = jnp.clip(j, 0, batch - 1)
        pieces = []
        for h in range(2):
            for t in range(steps):
                r = t * batch + b
                start = (r >> 3) * (8 * heads) + (r & 7) + h * (8 * half)
                pieces.append(q_ref[pl.ds(start, half, stride=8), :].astype(BF16))
        query = jnp.concatenate(pieces, axis=0)
        scores_refs[parity][...] = lax.dot_general(query, k_buf[lax.rem(b, held)], (((1,), (1,)), ((), ())), preferred_element_type=F32)

    def soften(j, parity):
        rel = rel_of(j)
        known = (j >= 0) & (j < batch)
        max_lane = jnp.where(known, j, 1024)
        sum_lane = jnp.where(known, j + batch, 1024)
        size = 16
        block_lane = lax.broadcasted_iota(jnp.int32, (size, 128), 1)
        for first in range(0, rows, size):
            here = slice(first, first + size)
            scores = jnp.where(dist[here, :] <= rel, scores_refs[parity][here, :], -jnp.inf)
            row_max = jnp.maximum(jnp.max(scores, axis=1, keepdims=True), MASKED_MAX)
            weights = jnp.exp2((scores - row_max) * scale)
            row_sum = jnp.sum(weights, axis=1, keepdims=True)
            weights_refs[parity][here, :] = weights.astype(BF16)
            stats = jnp.where(block_lane == max_lane, row_max, stat_ref[here, :])
            stat_ref[here, :] = jnp.where(block_lane == sum_lane, row_sum, stats)

    def mix(j, parity):
        b = jnp.clip(j, 0, batch - 1)
        mixed = jnp.dot(weights_refs[parity][...], v_buf[lax.rem(b, held)], preferred_element_type=F32)
        num_ref[b] = jnp.where(rel_of(j) + steps - 1 >= 0, mixed, 0.0)

    def pair(k, carry):
        first = 2 * k

        @pl.when(first < batch)
        def _():
            receive(first)
            receive(first + 1)

        longest = functools.reduce(jnp.maximum, [rel_of(first + n) for n in range(-2, 2)])
        visible = longest + steps - 1 >= 0

        @pl.when(visible)
        def _():
            for parity in range(2):
                score(first + parity, parity)
                soften(first + parity - 1, 1 - parity)
                mix(first + parity - 2, parity)

        @pl.when(jnp.logical_not(visible))
        def _():
            for parity in range(2):
                num_ref[jnp.clip(first + parity - 2, 0, batch - 1)] = jnp.zeros((rows, HEAD_DIM), F32)

        @pl.when(first >= 2)
        def _():
            for n in range(2):
                for copy in copies_out(first - 2 + n):
                    copy.start()

        for n in range(2):
            ahead = first + depth + n

            @pl.when(ahead < batch)
            def _():
                @pl.when(ahead >= held)
                def _():
                    for copy in copies_out(ahead - held):
                        copy.wait()

                for copy in copies_in(ahead):
                    copy.start()

        return carry

    lax.fori_loop(0, batch // 2 + 1, pair, 0)
    for b in range(batch - held, batch):
        for copy in copies_out(b):
            copy.wait()


def attend(seq_lens, k_cache, v_cache, queries, k_new, v_new, steps):
    batch, slots, kv_heads, head_dim = k_cache.shape
    heads = queries.shape[1]
    rows = steps * heads
    key_rows = slots * kv_heads
    depth, held = 16, 32
    cache = jax.ShapeDtypeStruct((batch, key_rows, head_dim), BF16)
    k_out, v_out, numer, stats = pl.pallas_call(
        functools.partial(attend_kernel, steps, depth),
        name='attend',
        in_specs=[pl.BlockSpec(memory_space=pltpu.SMEM), IN_PLACE, IN_PLACE, IN_VMEM, IN_VMEM, IN_VMEM],
        out_specs=(IN_PLACE, IN_PLACE, IN_VMEM, IN_VMEM),
        out_shape=(cache, cache, jax.ShapeDtypeStruct((batch, rows, head_dim), F32), jax.ShapeDtypeStruct((rows, 128), F32)),
        scratch_shapes=[
            VMEM((held, key_rows, head_dim), BF16),
            VMEM((held, key_rows, head_dim), BF16),
            VMEM((rows, key_rows), jnp.int32),
            VMEM((rows, key_rows), F32),
            VMEM((rows, key_rows), F32),
            VMEM((rows, key_rows), BF16),
            VMEM((rows, key_rows), BF16),
            DMA((held, 2)),
            DMA((held, 2)),
        ],
        compiler_params=pltpu.CompilerParams(vmem_limit_bytes=32 * MIB),
    )(seq_lens, k_cache.reshape(batch, key_rows, head_dim), v_cache.reshape(batch, key_rows, head_dim), queries.reshape(-1, head_dim), k_new.reshape(-1, head_dim), v_new.reshape(-1, head_dim))
    return k_out.reshape(k_cache.shape), v_out.reshape(v_cache.shape), numer, stats


def merge_kernel(chunks, steps, numer, stats, wo_hbm, y_own, y_other, wo, stat_d, stat_send, stat_x, recv_d, send_x, recv_x, scaled, att_f32, attended, sems_w, sem_stat, sems_d, sems_x, sems_y):
    _, batch, hidden = y_own.shape
    rows = numer.shape[1] // 2
    half = rows // steps
    me = lax.axis_index('sp')
    core = lax.rem(me, 2)
    other_core = me + 1 - 2 * core
    other_chip = lax.rem(me + 2, 4)
    own = pl.ds(pl.multiple_of(core * rows, rows), rows)
    other = pl.ds(pl.multiple_of((1 - core) * rows, rows), rows)
    firsts = [sum(chunks[:c]) for c in range(len(chunks))]

    w_pieces = sems_w.shape[0]
    w_rows = half * HEAD_DIM // w_pieces
    w_first = core * (half * HEAD_DIM)
    meet(other_core, other_chip)

    stat_copy = remote(stats.at[other], stat_d, sem_stat.at[0], other_core)
    stat_copy.start()
    core_copies = []
    for c, (first, seqs) in enumerate(zip(firsts, chunks)):
        here = pl.ds(first, seqs)
        copy = remote(numer.at[here, other], recv_d.at[here], sems_d.at[c], other_core)
        copy.start()
        core_copies.append(copy)
    w_copies = []
    for p in range(w_pieces):
        src = wo_hbm.at[pl.ds(pl.multiple_of(w_first + p * w_rows, w_rows), w_rows), :]
        copy = pltpu.make_async_copy(src, wo.at[pl.ds(p * w_rows, w_rows), :], sems_w.at[p])
        copy.start()
        w_copies.append(copy)

    lane = lax.broadcasted_iota(jnp.int32, (rows, 128), 1)
    scale = HEAD_DIM ** -0.5

    def combine(mine, theirs):
        top = jnp.maximum(mine, theirs)
        fac_a, fac_b = jnp.exp((mine - top) * scale), jnp.exp((theirs - top) * scale)
        total = pltpu.roll(mine, 128 - batch, 1) * fac_a + pltpu.roll(theirs, 128 - batch, 1) * fac_b
        return top, fac_a, fac_b, total

    stat_copy.wait()
    top, fac_a, fac_b, total = combine(stats[own, :], stat_d[...])
    stat_send[...] = jnp.where(lane < batch, top, pltpu.roll(total, batch, 1))
    scaled[0] = fac_a
    scaled[1] = fac_b
    chip_stat_copy = remote(stat_send, stat_x, sem_stat.at[1], other_chip)
    chip_stat_copy.start()

    chip_copies = []
    for c, (first, seqs) in enumerate(zip(firsts, chunks)):
        core_copies[c].wait()
        for b in range(first, first + seqs):
            send_x[b] = numer[b, own, :] * scaled[0, :, b:b + 1] + recv_d[b] * scaled[1, :, b:b + 1]
        here = pl.ds(first, seqs)
        copy = remote(send_x.at[here], recv_x.at[here], sems_x.at[c], other_chip)
        copy.start()
        chip_copies.append(copy)

    chip_stat_copy.wait()
    _, fac_a, fac_b, total = combine(stat_send[...], stat_x[...])
    scaled[0] = fac_a / total
    scaled[1] = fac_b / total

    width = 512
    y_copies = []
    for c, (first, seqs) in enumerate(zip(firsts, chunks)):
        chip_copies[c].wait()
        for b in range(first, first + seqs):
            merged = send_x[b] * scaled[0, :, b:b + 1] + recv_x[b] * scaled[1, :, b:b + 1]
            att_f32[pl.ds((b - first) * rows, rows), :] = merged
        for t in range(steps):
            for h in range(half):
                values = att_f32[pl.ds(t * half + h, seqs, stride=rows), :]
                attended[t * seqs:(t + 1) * seqs, h * HEAD_DIM:(h + 1) * HEAD_DIM] = values
        if c == 0:
            for copy in w_copies:
                copy.wait()

        @pl.loop(0, hidden // width)
        def _(j):
            cols = pl.ds(pl.multiple_of(j * width, width), width)
            out = jnp.dot(attended[:steps * seqs, :].astype(BF16), wo[:, cols], preferred_element_type=F32)
            for t in range(steps):
                y_own[t, first:first + seqs, cols] = out[t * seqs:(t + 1) * seqs, :]

        here = pl.ds(first, seqs)
        copy = remote(y_own.at[:, here, :], y_other.at[:, here, :], sems_y.at[c], other_core)
        copy.start()
        y_copies.append(copy)
    for copy in y_copies:
        copy.wait()


def merge(numer, stats, w_o, steps):
    batch, rows, _ = numer.shape
    hidden = w_o.shape[1]
    chunks = (16, 16, 16, 8, 8)
    largest = max(chunks)
    part = jax.ShapeDtypeStruct((steps, batch, hidden), F32)
    stat = VMEM((rows // 2, 128), F32)
    return pl.pallas_call(
        functools.partial(merge_kernel, chunks, steps),
        name='merge',
        out_shape=(part, part),
        in_specs=[IN_VMEM, IN_VMEM, IN_PLACE],
        out_specs=(IN_VMEM, IN_VMEM),
        scratch_shapes=[
            VMEM((w_o.shape[0] // 2, hidden), BF16),
            stat,
            stat,
            stat,
            VMEM((batch, rows // 2, HEAD_DIM), F32),
            VMEM((batch, rows // 2, HEAD_DIM), F32),
            VMEM((batch, rows // 2, HEAD_DIM), F32),
            VMEM((2, rows // 2, 128), F32),
            VMEM((largest * rows // 2, HEAD_DIM), F32),
            VMEM((steps * largest, w_o.shape[0] // 2), F32),
            DMA((8,)),
            DMA((2, 2)),
            DMA((len(chunks), 2)),
            DMA((len(chunks), 2)),
            DMA((len(chunks), 2)),
        ],
        compiler_params=pltpu.CompilerParams(collective_id=0, has_side_effects=True, vmem_limit_bytes=40 * MIB),
    )(numer, stats, w_o)


def solution(mesh):
    def per_device(x_steps, k_local, v_local, seq_lens, norm_gain, w_q, w_k, w_v, w_o, q_gain, k_gain):
        steps = x_steps.shape[0]
        rope, gains = small_tables(seq_lens, steps, norm_gain, q_gain, k_gain)
        queries, keys_new, vals_new = project(x_steps, rope, gains, w_q, w_k, w_v)
        k_out, v_out, numer, stats = attend(seq_lens, k_local, v_local, queries, keys_new, vals_new, steps)
        own, other = merge(numer, stats, w_o, steps)
        y_steps = (x_steps.astype(F32) + (own + other)).astype(BF16)
        return y_steps, k_out, v_out

    cache_spec = P('dp', 'sp', None, None)
    step_spec = P(None, 'dp', None)
    return jax.shard_map(per_device, mesh=mesh, in_specs=(step_spec, cache_spec, cache_spec, P('dp'), P(), P(), P(), P(), P(), P(), P()), out_specs=(step_spec, cache_spec, cache_spec), check_vma=False)
```

```python
import functools
import math

import jax
import jax.numpy as jnp
from jax import lax
from jax.experimental import pallas as pl
from jax.experimental.pallas import tpu as pltpu
from jax.sharding import PartitionSpec as P

NORM_EPS = 1e-6
ROPE_BASE = 1000000.0
MASKED_MAX = -1e30
HEAD_DIM = 128
F32 = jnp.float32
BF16 = jnp.bfloat16
MIB = 1024 * 1024
VMEM = pltpu.VMEM
DMA = pltpu.SemaphoreType.DMA
IN_VMEM = pl.BlockSpec(memory_space=VMEM)
IN_PLACE = pl.BlockSpec(memory_space=pl.ANY)


def small_tables(seq_lens, steps, norm_gain, q_gain, k_gain):
    half = HEAD_DIM // 2
    positions = (seq_lens[None, :] + jnp.arange(steps, dtype=jnp.int32)[:, None]).reshape(-1)
    inv_freq = jnp.exp(jnp.arange(half, dtype=F32) * (-2.0 * math.log(ROPE_BASE) / HEAD_DIM))
    angles = positions.astype(F32)[:, None] * inv_freq
    cosine = jnp.cos(angles)
    sine = jnp.sin(angles)
    rope = jnp.concatenate([jnp.concatenate([cosine, cosine], axis=-1), jnp.concatenate([-sine, sine], axis=-1)], axis=0)
    gains = jnp.concatenate([norm_gain, q_gain, k_gain]).astype(F32).reshape(-1, HEAD_DIM)
    return rope, gains


def remote(src, dst, sems, peer):
    return pltpu.make_async_remote_copy(src_ref=src, dst_ref=dst, send_sem=sems.at[0], recv_sem=sems.at[1], device_id={'sp': peer}, device_id_type=pl.DeviceIdType.MESH)


def meet(*peers):
    barrier = pltpu.get_barrier_semaphore()
    for peer in peers:
        pl.semaphore_signal(barrier, inc=1, device_id={'sp': peer}, device_id_type=pl.DeviceIdType.MESH)
    pl.semaphore_wait(barrier, len(peers))


def project_kernel(width, heads, kv_heads, x_hbm, rope_ref, gain_ref, wq_hbm, wk_hbm, wv_hbm, q_ref, k_ref, v_ref, x_rows, normed, acc, wbuf, sem_x, sems_w, sems_q, sems_k, sems_v):
    rows, hidden = x_rows.shape
    per_block = width // HEAD_DIM
    core = lax.rem(lax.axis_index('sp'), 2)
    other_core = lax.axis_index('sp') + 1 - 2 * core

    x_copy = pltpu.make_async_copy(x_hbm, x_rows, sem_x)
    x_copy.start()
    blocks = [(wk_hbm, k_ref, sems_k, kv_heads, 0)]
    blocks += [(wq_hbm, q_ref, sems_q, heads, i) for i in range(heads // 2 // per_block)]
    blocks += [(wv_hbm, v_ref, sems_v, kv_heads, 0)]
    w_copies = []
    for n, (w_hbm, _, _, total, i) in enumerate(blocks):
        cols = pl.ds(pl.multiple_of(core * (total // 2 * HEAD_DIM) + i * width, width), width)
        copy = pltpu.make_async_copy(w_hbm.at[:, cols], wbuf.at[n], sems_w.at[n])
        copy.start()
        w_copies.append(copy)

    meet(other_core)
    x_copy.wait()

    @pl.loop(0, rows // 16)
    def _(i):
        here = pl.ds(pl.multiple_of(i * 16, 16), 16)
        values = x_rows[here, :].astype(F32)
        inv_rms = lax.rsqrt(jnp.mean(values * values, axis=-1, keepdims=True) + NORM_EPS)
        for n in range(hidden // HEAD_DIM):
            lanes = slice(n * HEAD_DIM, (n + 1) * HEAD_DIM)
            normed[here, lanes] = (x_rows[here, lanes].astype(F32) * inv_rms * gain_ref[n:n + 1, :]).astype(BF16)

    def finish(n):
        w_hbm, out_ref, sems, total, i = blocks[n]
        first = core * (total // 2) + i * per_block
        for j in range(per_block):
            values = acc[n % 2, :, j * HEAD_DIM:(j + 1) * HEAD_DIM].astype(BF16).astype(F32)
            if out_ref is not v_ref:
                row = hidden // HEAD_DIM + (1 if out_ref is k_ref else 0)
                inv_rms = lax.rsqrt(jnp.mean(values * values, axis=-1, keepdims=True) + NORM_EPS)
                scaled = values * inv_rms * gain_ref[row:row + 1, :]
                values = scaled * rope_ref[:rows, :] + pltpu.roll(scaled, HEAD_DIM // 2, 1) * rope_ref[rows:, :]
                values = values.astype(BF16).astype(F32)
            out_ref[:, first + j, :, :] = values.reshape(rows // 8, 8, HEAD_DIM)

    def send(n):
        _, out_ref, sems, total, i = blocks[n]
        there = pl.ds(core * (total // 2) + i * per_block, per_block)
        copy = remote(out_ref.at[:, there], out_ref.at[:, there], sems.at[i], other_core)
        copy.start()
        return copy

    sends = []
    for n in range(len(blocks)):
        w_copies[n].wait()
        acc[n % 2] = jnp.dot(normed[...], wbuf[n], preferred_element_type=F32)
        if n > 0:
            finish(n - 1)
            sends.append(send(n - 1))
    finish(len(blocks) - 1)
    sends.append(send(len(blocks) - 1))
    for copy in sends:
        copy.wait()


def project(x_steps, rope, gains, w_q, w_k, w_v):
    steps, batch, hidden = x_steps.shape
    rows = steps * batch
    heads = w_q.shape[1] // HEAD_DIM
    kv_heads = w_k.shape[1] // HEAD_DIM
    width = kv_heads // 2 * HEAD_DIM
    q_blocks = heads // kv_heads
    return pl.pallas_call(
        functools.partial(project_kernel, width, heads, kv_heads),
        name='project',
        out_shape=tuple(jax.ShapeDtypeStruct((rows // 8, n, 8, HEAD_DIM), F32) for n in (heads, kv_heads, kv_heads)),
        in_specs=[pl.BlockSpec(memory_space=pltpu.HBM), IN_VMEM, IN_VMEM] + [IN_PLACE] * 3,
        out_specs=(IN_VMEM,) * 3,
        scratch_shapes=[
            VMEM((rows, hidden), BF16),
            VMEM((rows, hidden), BF16),
            VMEM((2, rows, width), F32),
            VMEM((q_blocks + 2, hidden, width), BF16),
            DMA,
            DMA((q_blocks + 2,)),
            DMA((q_blocks, 2)),
            DMA((1, 2)),
            DMA((1, 2)),
        ],
        compiler_params=pltpu.CompilerParams(collective_id=1, has_side_effects=True, vmem_limit_bytes=40 * MIB),
    )(x_steps.reshape(rows, hidden), rope, gains, w_q, w_k, w_v)


def attend_kernel(steps, depth, start, lens_ref, k_hbm, v_hbm, q_ref, kn_ref, vn_ref, ko_hbm, vo_hbm, num_ref, stat_ref, k_buf, v_buf, dist, scores_0, scores_1, weights_0, weights_1, sems_in, sems_out):
    held, key_rows, _ = k_buf.shape
    batch = lens_ref.shape[0]
    count = num_ref.shape[0]
    heads, kv_heads = q_ref.shape[0] // (steps * batch), kn_ref.shape[0] // (steps * batch)
    slots = key_rows // kv_heads
    rows = steps * heads
    half = heads // 2
    first_slot = lax.axis_index('sp') * slots
    upper = lax.broadcasted_iota(jnp.int32, (2 * kv_heads, HEAD_DIM), 0) >= kv_heads
    scale = HEAD_DIM ** -0.5 * math.log2(math.e)
    scores_refs, weights_refs = (scores_0, scores_1), (weights_0, weights_1)

    def copies_in(b):
        slot = lax.rem(b, held)
        return (pltpu.make_async_copy(k_hbm.at[start + b], k_buf.at[slot], sems_in.at[slot, 0]),
                pltpu.make_async_copy(v_hbm.at[start + b], v_buf.at[slot], sems_in.at[slot, 1]))

    def copies_out(b):
        slot = lax.rem(b, held)
        return (pltpu.make_async_copy(k_buf.at[slot], ko_hbm.at[start + b], sems_out.at[slot, 0]),
                pltpu.make_async_copy(v_buf.at[slot], vo_hbm.at[start + b], sems_out.at[slot, 1]))

    for b in range(depth):
        for copy in copies_in(b):
            copy.start()

    lane = lax.broadcasted_iota(jnp.int32, (rows, 128), 1)
    stat_ref[...] = jnp.where(lane < batch, MASKED_MAX, 0.0)
    row = lax.broadcasted_iota(jnp.int32, (rows, key_rows), 0)
    col = lax.broadcasted_iota(jnp.int32, (rows, key_rows), 1)
    row_half, in_half = row // (steps * half), lax.rem(row, steps * half)
    row_kv = (row_half * half + lax.rem(in_half, half)) // (heads // kv_heads)
    dist[...] = jnp.where(row_kv == lax.rem(col, kv_heads), col // kv_heads - in_half // half, 1 << 24)

    def rel_of(b):
        return lens_ref[start + jnp.clip(b, 0, count - 1)] - first_slot

    def receive(b):
        slot = lax.rem(b, held)
        for copy in copies_in(b):
            copy.wait()
        rel = rel_of(b)
        for t in range(steps):
            at = rel + t

            @pl.when((at >= 0) & (at < slots))
            def _():
                base = pl.multiple_of((at >> 1) * (2 * kv_heads), 2 * kv_heads)
                mine = upper == ((at & 1) == 1)
                r = t * batch + start + b
                new_rows = pl.ds((r >> 3) * (8 * kv_heads) + (r & 7), kv_heads, stride=8)
                for buf, new in ((k_buf, kn_ref), (v_buf, vn_ref)):
                    fresh = new[new_rows, :]
                    fresh = jnp.concatenate([fresh, fresh], axis=0)
                    old = buf[slot, pl.ds(base, 2 * kv_heads), :].astype(F32)
                    buf[slot, pl.ds(base, 2 * kv_heads), :] = jnp.where(mine, fresh, old).astype(BF16)

    def score(j, parity):
        b = jnp.clip(j, 0, count - 1)
        pieces = []
        for h in range(2):
            for t in range(steps):
                r = t * batch + start + b
                at = (r >> 3) * (8 * heads) + (r & 7) + h * (8 * half)
                pieces.append(q_ref[pl.ds(at, half, stride=8), :].astype(BF16))
        query = jnp.concatenate(pieces, axis=0)
        scores_refs[parity][...] = lax.dot_general(query, k_buf[lax.rem(b, held)], (((1,), (1,)), ((), ())), preferred_element_type=F32)

    def soften(j, parity):
        rel = rel_of(j)
        known = (j >= 0) & (j < count)
        max_lane = jnp.where(known, start + j, 1024)
        sum_lane = jnp.where(known, start + j + batch, 1024)
        size = 16
        block_lane = lax.broadcasted_iota(jnp.int32, (size, 128), 1)
        for first in range(0, rows, size):
            here = slice(first, first + size)
            scores = jnp.where(dist[here, :] <= rel, scores_refs[parity][here, :], -jnp.inf)
            row_max = jnp.maximum(jnp.max(scores, axis=1, keepdims=True), MASKED_MAX)
            weights = jnp.exp2((scores - row_max) * scale)
            row_sum = jnp.sum(weights, axis=1, keepdims=True)
            weights_refs[parity][here, :] = weights.astype(BF16)
            stats = jnp.where(block_lane == max_lane, row_max, stat_ref[here, :])
            stat_ref[here, :] = jnp.where(block_lane == sum_lane, row_sum, stats)

    def mix(j, parity):
        b = jnp.clip(j, 0, count - 1)
        mixed = jnp.dot(weights_refs[parity][...], v_buf[lax.rem(b, held)], preferred_element_type=F32)
        num_ref[b] = jnp.where(rel_of(j) + steps - 1 >= 0, mixed, 0.0)

    def pair(k, carry):
        first = 2 * k

        @pl.when(first < count)
        def _():
            receive(first)
            receive(first + 1)

        longest = functools.reduce(jnp.maximum, [rel_of(first + n) for n in range(-2, 2)])
        visible = longest + steps - 1 >= 0

        @pl.when(visible)
        def _():
            for parity in range(2):
                score(first + parity, parity)
                soften(first + parity - 1, 1 - parity)
                mix(first + parity - 2, parity)

        @pl.when(jnp.logical_not(visible))
        def _():
            for parity in range(2):
                num_ref[jnp.clip(first + parity - 2, 0, count - 1)] = jnp.zeros((rows, HEAD_DIM), F32)

        @pl.when(first >= 2)
        def _():
            for n in range(2):
                for copy in copies_out(first - 2 + n):
                    copy.start()

        for n in range(2):
            ahead = first + depth + n

            @pl.when(ahead < count)
            def _():
                @pl.when(ahead >= held)
                def _():
                    for copy in copies_out(ahead - held):
                        copy.wait()

                for copy in copies_in(ahead):
                    copy.start()

        return carry

    lax.fori_loop(0, count // 2 + 1, pair, 0)
    for b in range(max(count - held, 0), count):
        for copy in copies_out(b):
            copy.wait()


def attend(seq_lens, k_cache, v_cache, queries, k_new, v_new, steps, start, count, partial=()):
    batch, key_rows, head_dim = k_cache.shape
    heads = queries.shape[1]
    rows = steps * heads
    depth, held = 16, 32
    cache = jax.ShapeDtypeStruct(k_cache.shape, BF16)
    flops = 4 * count * rows * key_rows * head_dim
    kernel = functools.partial(attend_kernel, steps, depth, start)

    def continued(*refs):
        kernel(*refs[:6], *refs[8:])

    return pl.pallas_call(
        continued if partial else kernel,
        name='attend',
        in_specs=[pl.BlockSpec(memory_space=pltpu.SMEM), IN_PLACE, IN_PLACE, IN_VMEM, IN_VMEM, IN_VMEM] + [IN_PLACE] * len(partial),
        out_specs=(IN_PLACE, IN_PLACE, IN_VMEM, IN_VMEM),
        out_shape=(cache, cache, jax.ShapeDtypeStruct((count, rows, head_dim), F32), jax.ShapeDtypeStruct((rows, 128), F32)),
        input_output_aliases={6: 0, 7: 1} if partial else {},
        scratch_shapes=[
            VMEM((held, key_rows, head_dim), BF16),
            VMEM((held, key_rows, head_dim), BF16),
            VMEM((rows, key_rows), jnp.int32),
            VMEM((rows, key_rows), F32),
            VMEM((rows, key_rows), F32),
            VMEM((rows, key_rows), BF16),
            VMEM((rows, key_rows), BF16),
            DMA((held, 2)),
            DMA((held, 2)),
        ],
        cost_estimate=pl.CostEstimate(flops=flops, bytes_accessed=4 * count * key_rows * head_dim * 2, transcendentals=0),
        compiler_params=pltpu.CompilerParams(vmem_limit_bytes=32 * MIB),
    )(seq_lens, k_cache, v_cache, queries.reshape(-1, head_dim), k_new.reshape(-1, head_dim), v_new.reshape(-1, head_dim), *partial)


def combine(mine, theirs, batch):
    scale = HEAD_DIM ** -0.5
    top = jnp.maximum(mine, theirs)
    fac_a, fac_b = jnp.exp((mine - top) * scale), jnp.exp((theirs - top) * scale)
    total = pltpu.roll(mine, 128 - batch, 1) * fac_a + pltpu.roll(theirs, 128 - batch, 1) * fac_b
    return top, fac_a, fac_b, total


def join_stats(top, total, batch):
    lane = lax.broadcasted_iota(jnp.int32, top.shape, 1)
    return jnp.where(lane < batch, top, pltpu.roll(total, batch, 1))


def places():
    me = lax.axis_index('sp')
    core = lax.rem(me, 2)
    return core, me + 1 - 2 * core, lax.rem(me + 2, 4)


def spans(chunks):
    return [(sum(chunks[:c]), seqs) for c, seqs in enumerate(chunks)]


def pair_kernel(chunks, batch, numer, stats, out, stat_d, recv_d, scaled, sem_stat, sems_d):
    rows = numer.shape[1] // 2
    core, other_core, _ = places()
    own = pl.ds(pl.multiple_of(core * rows, rows), rows)
    other = pl.ds(pl.multiple_of((1 - core) * rows, rows), rows)
    meet(other_core)
    stat_copy = remote(stats.at[other], stat_d, sem_stat, other_core)
    stat_copy.start()
    copies = []
    for c, (first, seqs) in enumerate(spans(chunks)):
        here = pl.ds(first, seqs)
        copy = remote(numer.at[here, other], recv_d.at[here], sems_d.at[c], other_core)
        copy.start()
        copies.append(copy)
    stat_copy.wait()
    top, fac_a, fac_b, total = combine(stats[own, :], stat_d[...], batch)
    out[numer.shape[0]] = join_stats(top, total, batch)
    scaled[0] = fac_a
    scaled[1] = fac_b
    for copy, (first, seqs) in zip(copies, spans(chunks)):
        copy.wait()
        for b in range(first, first + seqs):
            out[b] = numer[b, own, :] * scaled[0, :, b:b + 1] + recv_d[b] * scaled[1, :, b:b + 1]


def merge_pair(numer, stats, batch):
    count, rows, _ = numer.shape
    chunks = (8,) * (count // 8)
    return pl.pallas_call(
        functools.partial(pair_kernel, chunks, batch),
        name='merge_pair',
        out_shape=jax.ShapeDtypeStruct((count + 1, rows // 2, HEAD_DIM), F32),
        in_specs=[IN_VMEM, IN_VMEM],
        out_specs=IN_VMEM,
        scratch_shapes=[
            VMEM((rows // 2, 128), F32),
            VMEM((count, rows // 2, HEAD_DIM), F32),
            VMEM((2, rows // 2, 128), F32),
            DMA((2,)),
            DMA((len(chunks), 2)),
        ],
        compiler_params=pltpu.CompilerParams(collective_id=2, has_side_effects=True, vmem_limit_bytes=16 * MIB),
    )(numer, stats)


def merge_kernel(early_chunks, chunks, steps, numer, stats, early_own, early_theirs, wo_hbm, y_own, y_other, wo, stat_d, stat_send, stat_x, recv_d, send_x, recv_x, scaled, att_f32, attended, sems_w, sem_stat, sems_d, sems_x, sems_y):
    _, batch, hidden = y_own.shape
    rows = numer.shape[1] // 2
    half = rows // steps
    start = batch - numer.shape[0]
    core, other_core, other_chip = places()
    own = pl.ds(pl.multiple_of(core * rows, rows), rows)
    other = pl.ds(pl.multiple_of((1 - core) * rows, rows), rows)

    w_pieces = sems_w.shape[0]
    w_rows = half * HEAD_DIM // w_pieces
    w_first = core * (half * HEAD_DIM)
    meet(other_core, other_chip)

    stat_copy = remote(stats.at[other], stat_d, sem_stat.at[0], other_core)
    stat_copy.start()
    core_copies = []
    for c, (first, seqs) in enumerate(spans(chunks)):
        here = pl.ds(first, seqs)
        copy = remote(numer.at[here, other], recv_d.at[here], sems_d.at[c], other_core)
        copy.start()
        core_copies.append(copy)
    w_copies = []
    for p in range(w_pieces):
        src = wo_hbm.at[pl.ds(pl.multiple_of(w_first + p * w_rows, w_rows), w_rows), :]
        copy = pltpu.make_async_copy(src, wo.at[pl.ds(p * w_rows, w_rows), :], sems_w.at[p])
        copy.start()
        w_copies.append(copy)

    stat_copy.wait()
    top, fac_a, fac_b, total = combine(stats[own, :], stat_d[...], batch)
    stat_send[...] = join_stats(top, total, batch)
    scaled[0] = fac_a
    scaled[1] = fac_b
    chip_stat_copy = remote(stat_send, stat_x, sem_stat.at[1], other_chip)
    chip_stat_copy.start()

    chip_copies = []
    for c, (first, seqs) in enumerate(spans(chunks)):
        core_copies[c].wait()
        for i in range(first, first + seqs):
            b = start + i
            send_x[i] = numer[i, own, :] * scaled[0, :, b:b + 1] + recv_d[i] * scaled[1, :, b:b + 1]
        here = pl.ds(first, seqs)
        copy = remote(send_x.at[here], recv_x.at[here], sems_x.at[c], other_chip)
        copy.start()
        chip_copies.append(copy)

    width = 512
    y_copies = []

    def finish(mine, theirs, first, seqs, begin):
        for i in range(first, first + seqs):
            b = begin + i
            merged = mine[i] * scaled[0, :, b:b + 1] + theirs[i] * scaled[1, :, b:b + 1]
            att_f32[pl.ds((i - first) * rows, rows), :] = merged
        for t in range(steps):
            for h in range(half):
                values = att_f32[pl.ds(t * half + h, seqs, stride=rows), :]
                attended[t * seqs:(t + 1) * seqs, h * HEAD_DIM:(h + 1) * HEAD_DIM] = values
        if not y_copies:
            for copy in w_copies:
                copy.wait()
        at = begin + first

        @pl.loop(0, hidden // width)
        def _(j):
            cols = pl.ds(pl.multiple_of(j * width, width), width)
            out = jnp.dot(attended[:steps * seqs, :].astype(BF16), wo[:, cols], preferred_element_type=F32)
            for t in range(steps):
                y_own[t, at:at + seqs, cols] = out[t * seqs:(t + 1) * seqs, :]

        here = pl.ds(at, seqs)
        copy = remote(y_own.at[:, here, :], y_other.at[:, here, :], sems_y.at[len(y_copies)], other_core)
        copy.start()
        y_copies.append(copy)

    def set_factors(mine, theirs):
        _, fac_a, fac_b, total = combine(mine, theirs, batch)
        scaled[0] = fac_a / total
        scaled[1] = fac_b / total

    set_factors(early_own[start], early_theirs[start])
    for first, seqs in spans(early_chunks):
        finish(early_own, early_theirs, first, seqs, 0)
    chip_stat_copy.wait()
    set_factors(stat_send[...], stat_x[...])
    for c, (first, seqs) in enumerate(spans(chunks)):
        chip_copies[c].wait()
        finish(send_x, recv_x, first, seqs, start)
    for copy in y_copies:
        copy.wait()


def merge(numer, stats, early_own, early_theirs, w_o, steps, batch):
    count, rows, _ = numer.shape
    hidden = w_o.shape[1]
    early_chunks = (16, 8)
    chunks = (8, 16, 8, 8)
    largest = max(chunks + early_chunks)
    part = jax.ShapeDtypeStruct((steps, batch, hidden), F32)
    stat = VMEM((rows // 2, 128), F32)
    moved = VMEM((count, rows // 2, HEAD_DIM), F32)
    return pl.pallas_call(
        functools.partial(merge_kernel, early_chunks, chunks, steps),
        name='merge',
        out_shape=(part, part),
        in_specs=[IN_VMEM] * 4 + [IN_PLACE],
        out_specs=(IN_VMEM, IN_VMEM),
        scratch_shapes=[
            VMEM((w_o.shape[0] // 2, hidden), BF16),
            stat,
            stat,
            stat,
            moved,
            moved,
            moved,
            VMEM((2, rows // 2, 128), F32),
            VMEM((largest * rows // 2, HEAD_DIM), F32),
            VMEM((steps * largest, w_o.shape[0] // 2), F32),
            DMA((8,)),
            DMA((2, 2)),
            DMA((len(chunks), 2)),
            DMA((len(chunks), 2)),
            DMA((len(chunks) + len(early_chunks), 2)),
        ],
        compiler_params=pltpu.CompilerParams(collective_id=0, has_side_effects=True, vmem_limit_bytes=40 * MIB),
    )(numer, stats, early_own, early_theirs, w_o)


def solution(mesh):
    def per_device(x_steps, k_local, v_local, seq_lens, norm_gain, w_q, w_k, w_v, w_o, q_gain, k_gain):
        steps, batch, _ = x_steps.shape
        early = 24
        rope, gains = small_tables(seq_lens, steps, norm_gain, q_gain, k_gain)
        fresh = project(x_steps, rope, gains, w_q, w_k, w_v)
        flat = (batch, -1, HEAD_DIM)
        caches = (k_local.reshape(flat), v_local.reshape(flat))
        k_part, v_part, early_numer, early_stats = attend(seq_lens, *caches, *fresh, steps, 0, early)
        early_own = merge_pair(early_numer, early_stats, batch)
        early_theirs = lax.ppermute(early_own, 'sp', [(i, (i + 2) % 4) for i in range(4)])
        k_out, v_out, numer, stats = attend(seq_lens, *caches, *fresh, steps, early, batch - early, (k_part, v_part))
        own, other = merge(numer, stats, early_own, early_theirs, w_o, steps, batch)
        y_steps = (x_steps.astype(F32) + (own + other)).astype(BF16)
        return y_steps, k_out.reshape(k_local.shape), v_out.reshape(v_local.shape)

    cache_spec = P('dp', 'sp', None, None)
    step_spec = P(None, 'dp', None)
    return jax.shard_map(per_device, mesh=mesh, in_specs=(step_spec, cache_spec, cache_spec, P('dp'), P(), P(), P(), P(), P(), P(), P()), out_specs=(step_spec, cache_spec, cache_spec), check_vma=False)
```

```python
import functools
import math

import jax
import jax.numpy as jnp
from jax import lax
from jax.experimental import pallas as pl
from jax.experimental.pallas import tpu as pltpu
from jax.sharding import PartitionSpec as P

NORM_EPS = 1e-6
ROPE_BASE = 1000000.0
MASKED_MAX = -1e30
HEAD_DIM = 128
F32 = jnp.float32
BF16 = jnp.bfloat16
MIB = 1024 * 1024
VMEM = pltpu.VMEM
DMA = pltpu.SemaphoreType.DMA
IN_VMEM = pl.BlockSpec(memory_space=VMEM)
IN_PLACE = pl.BlockSpec(memory_space=pl.ANY)


def small_tables(seq_lens, steps, norm_gain, q_gain, k_gain):
    half = HEAD_DIM // 2
    positions = (seq_lens[None, :] + jnp.arange(steps, dtype=jnp.int32)[:, None]).reshape(-1)
    inv_freq = jnp.exp(jnp.arange(half, dtype=F32) * (-2.0 * math.log(ROPE_BASE) / HEAD_DIM))
    angles = positions.astype(F32)[:, None] * inv_freq
    cosine = jnp.cos(angles)
    sine = jnp.sin(angles)
    rope = jnp.concatenate([jnp.concatenate([cosine, cosine], axis=-1), jnp.concatenate([-sine, sine], axis=-1)], axis=0)
    gains = jnp.concatenate([norm_gain, q_gain, k_gain]).astype(F32).reshape(-1, HEAD_DIM)
    return rope, gains


def remote(src, dst, sems, peer):
    return pltpu.make_async_remote_copy(src_ref=src, dst_ref=dst, send_sem=sems.at[0], recv_sem=sems.at[1], device_id={'sp': peer}, device_id_type=pl.DeviceIdType.MESH)


def meet(*peers):
    barrier = pltpu.get_barrier_semaphore()
    for peer in peers:
        pl.semaphore_signal(barrier, inc=1, device_id={'sp': peer}, device_id_type=pl.DeviceIdType.MESH)
    pl.semaphore_wait(barrier, len(peers))


def project_kernel(width, heads, kv_heads, x_hbm, rope_ref, gain_ref, wq_hbm, wk_hbm, wv_hbm, q_ref, k_ref, v_ref, x_rows, normed, acc, wbuf, sem_x, sems_w, sems_q, sems_k, sems_v):
    rows, hidden = x_rows.shape
    per_block = width // HEAD_DIM
    core = lax.rem(lax.axis_index('sp'), 2)
    other_core = lax.axis_index('sp') + 1 - 2 * core

    x_copy = pltpu.make_async_copy(x_hbm, x_rows, sem_x)
    x_copy.start()
    blocks = [(wk_hbm, k_ref, sems_k, kv_heads, 0)]
    blocks += [(wq_hbm, q_ref, sems_q, heads, i) for i in range(heads // 2 // per_block)]
    blocks += [(wv_hbm, v_ref, sems_v, kv_heads, 0)]
    w_copies = []
    for n, (w_hbm, _, _, total, i) in enumerate(blocks):
        cols = pl.ds(pl.multiple_of(core * (total // 2 * HEAD_DIM) + i * width, width), width)
        copy = pltpu.make_async_copy(w_hbm.at[:, cols], wbuf.at[n], sems_w.at[n])
        copy.start()
        w_copies.append(copy)

    meet(other_core)
    x_copy.wait()

    @pl.loop(0, rows // 16)
    def _(i):
        here = pl.ds(pl.multiple_of(i * 16, 16), 16)
        values = x_rows[here, :].astype(F32)
        inv_rms = lax.rsqrt(jnp.mean(values * values, axis=-1, keepdims=True) + NORM_EPS)
        for n in range(hidden // HEAD_DIM):
            lanes = slice(n * HEAD_DIM, (n + 1) * HEAD_DIM)
            normed[here, lanes] = (x_rows[here, lanes].astype(F32) * inv_rms * gain_ref[n:n + 1, :]).astype(BF16)

    def finish(n):
        w_hbm, out_ref, sems, total, i = blocks[n]
        first = core * (total // 2) + i * per_block
        for j in range(per_block):
            values = acc[n % 2, :, j * HEAD_DIM:(j + 1) * HEAD_DIM].astype(BF16).astype(F32)
            if out_ref is not v_ref:
                row = hidden // HEAD_DIM + (1 if out_ref is k_ref else 0)
                inv_rms = lax.rsqrt(jnp.mean(values * values, axis=-1, keepdims=True) + NORM_EPS)
                scaled = values * inv_rms * gain_ref[row:row + 1, :]
                values = scaled * rope_ref[:rows, :] + pltpu.roll(scaled, HEAD_DIM // 2, 1) * rope_ref[rows:, :]
                values = values.astype(BF16).astype(F32)
            out_ref[:, first + j, :, :] = values.reshape(rows // 8, 8, HEAD_DIM)

    def send(n):
        _, out_ref, sems, total, i = blocks[n]
        there = pl.ds(core * (total // 2) + i * per_block, per_block)
        copy = remote(out_ref.at[:, there], out_ref.at[:, there], sems.at[i], other_core)
        copy.start()
        return copy

    sends = []
    for n in range(len(blocks)):
        w_copies[n].wait()
        acc[n % 2] = jnp.dot(normed[...], wbuf[n], preferred_element_type=F32)
        if n > 0:
            finish(n - 1)
            sends.append(send(n - 1))
    finish(len(blocks) - 1)
    sends.append(send(len(blocks) - 1))
    for copy in sends:
        copy.wait()


def project(x_steps, rope, gains, w_q, w_k, w_v):
    steps, batch, hidden = x_steps.shape
    rows = steps * batch
    heads = w_q.shape[1] // HEAD_DIM
    kv_heads = w_k.shape[1] // HEAD_DIM
    width = kv_heads // 2 * HEAD_DIM
    q_blocks = heads // kv_heads
    return pl.pallas_call(
        functools.partial(project_kernel, width, heads, kv_heads),
        name='project',
        out_shape=tuple(jax.ShapeDtypeStruct((rows // 8, n, 8, HEAD_DIM), F32) for n in (heads, kv_heads, kv_heads)),
        in_specs=[pl.BlockSpec(memory_space=pltpu.HBM), IN_VMEM, IN_VMEM] + [IN_PLACE] * 3,
        out_specs=(IN_VMEM,) * 3,
        scratch_shapes=[
            VMEM((rows, hidden), BF16),
            VMEM((rows, hidden), BF16),
            VMEM((2, rows, width), F32),
            VMEM((q_blocks + 2, hidden, width), BF16),
            DMA,
            DMA((q_blocks + 2,)),
            DMA((q_blocks, 2)),
            DMA((1, 2)),
            DMA((1, 2)),
        ],
        compiler_params=pltpu.CompilerParams(collective_id=1, has_side_effects=True, vmem_limit_bytes=40 * MIB),
    )(pltpu.with_memory_space_constraint(x_steps.reshape(rows, hidden), pltpu.HBM), rope, gains, w_q, w_k, w_v)


def attend_kernel(steps, depth, start, lens_ref, k_hbm, v_hbm, q_ref, kn_ref, vn_ref, ko_hbm, vo_hbm, num_ref, stat_ref, k_buf, v_buf, dist, scores_0, scores_1, weights_0, weights_1, sems_in, sems_out):
    held, key_rows, _ = k_buf.shape
    batch = lens_ref.shape[0]
    count = num_ref.shape[0]
    heads, kv_heads = q_ref.shape[0] // (steps * batch), kn_ref.shape[0] // (steps * batch)
    slots = key_rows // kv_heads
    rows = steps * heads
    half = heads // 2
    first_slot = lax.axis_index('sp') * slots
    upper = lax.broadcasted_iota(jnp.int32, (2 * kv_heads, HEAD_DIM), 0) >= kv_heads
    scale = HEAD_DIM ** -0.5 * math.log2(math.e)
    scores_refs, weights_refs = (scores_0, scores_1), (weights_0, weights_1)

    def copies_in(b):
        slot = lax.rem(b, held)
        return (pltpu.make_async_copy(k_hbm.at[start + b], k_buf.at[slot], sems_in.at[slot, 0]),
                pltpu.make_async_copy(v_hbm.at[start + b], v_buf.at[slot], sems_in.at[slot, 1]))

    def copies_out(b):
        slot = lax.rem(b, held)
        return (pltpu.make_async_copy(k_buf.at[slot], ko_hbm.at[start + b], sems_out.at[slot, 0]),
                pltpu.make_async_copy(v_buf.at[slot], vo_hbm.at[start + b], sems_out.at[slot, 1]))

    for b in range(depth):
        for copy in copies_in(b):
            copy.start()

    lane = lax.broadcasted_iota(jnp.int32, (rows, 128), 1)
    stat_ref[...] = jnp.where(lane < batch, MASKED_MAX, 0.0)
    row = lax.broadcasted_iota(jnp.int32, (rows, key_rows), 0)
    col = lax.broadcasted_iota(jnp.int32, (rows, key_rows), 1)
    row_half, in_half = row // (steps * half), lax.rem(row, steps * half)
    row_kv = (row_half * half + lax.rem(in_half, half)) // (heads // kv_heads)
    dist[...] = jnp.where(row_kv == lax.rem(col, kv_heads), col // kv_heads - in_half // half, 1 << 24)

    def rel_of(b):
        return lens_ref[start + jnp.clip(b, 0, count - 1)] - first_slot

    def receive(b):
        slot = lax.rem(b, held)
        for copy in copies_in(b):
            copy.wait()
        rel = rel_of(b)
        for t in range(steps):
            at = rel + t

            @pl.when((at >= 0) & (at < slots))
            def _():
                base = pl.multiple_of((at >> 1) * (2 * kv_heads), 2 * kv_heads)
                mine = upper == ((at & 1) == 1)
                r = t * batch + start + b
                new_rows = pl.ds((r >> 3) * (8 * kv_heads) + (r & 7), kv_heads, stride=8)
                for buf, new in ((k_buf, kn_ref), (v_buf, vn_ref)):
                    fresh = new[new_rows, :]
                    fresh = jnp.concatenate([fresh, fresh], axis=0)
                    old = buf[slot, pl.ds(base, 2 * kv_heads), :].astype(F32)
                    buf[slot, pl.ds(base, 2 * kv_heads), :] = jnp.where(mine, fresh, old).astype(BF16)

    def score(j, parity):
        b = jnp.clip(j, 0, count - 1)
        pieces = []
        for h in range(2):
            for t in range(steps):
                r = t * batch + start + b
                at = (r >> 3) * (8 * heads) + (r & 7) + h * (8 * half)
                pieces.append(q_ref[pl.ds(at, half, stride=8), :].astype(BF16))
        query = jnp.concatenate(pieces, axis=0)
        scores_refs[parity][...] = lax.dot_general(query, k_buf[lax.rem(b, held)], (((1,), (1,)), ((), ())), preferred_element_type=F32)

    def soften(j, parity):
        rel = rel_of(j)
        known = (j >= 0) & (j < count)
        max_lane = jnp.where(known, start + j, 1024)
        sum_lane = jnp.where(known, start + j + batch, 1024)
        size = 16
        block_lane = lax.broadcasted_iota(jnp.int32, (size, 128), 1)
        for first in range(0, rows, size):
            here = slice(first, first + size)
            scores = jnp.where(dist[here, :] <= rel, scores_refs[parity][here, :], -jnp.inf)
            row_max = jnp.maximum(jnp.max(scores, axis=1, keepdims=True), MASKED_MAX)
            weights = jnp.exp2((scores - row_max) * scale)
            row_sum = jnp.sum(weights, axis=1, keepdims=True)
            weights_refs[parity][here, :] = weights.astype(BF16)
            stats = jnp.where(block_lane == max_lane, row_max, stat_ref[here, :])
            stat_ref[here, :] = jnp.where(block_lane == sum_lane, row_sum, stats)

    def mix(j, parity):
        b = jnp.clip(j, 0, count - 1)
        mixed = jnp.dot(weights_refs[parity][...], v_buf[lax.rem(b, held)], preferred_element_type=F32)
        num_ref[b] = jnp.where(rel_of(j) + steps - 1 >= 0, mixed, 0.0)

    def pair(k, carry):
        first = 2 * k

        @pl.when(first < count)
        def _():
            receive(first)
            receive(first + 1)

        longest = functools.reduce(jnp.maximum, [rel_of(first + n) for n in range(-2, 2)])
        visible = longest + steps - 1 >= 0

        @pl.when(visible)
        def _():
            for parity in range(2):
                score(first + parity, parity)
                soften(first + parity - 1, 1 - parity)
                mix(first + parity - 2, parity)

        @pl.when(jnp.logical_not(visible))
        def _():
            for parity in range(2):
                num_ref[jnp.clip(first + parity - 2, 0, count - 1)] = jnp.zeros((rows, HEAD_DIM), F32)

        @pl.when(first >= 2)
        def _():
            for n in range(2):
                for copy in copies_out(first - 2 + n):
                    copy.start()

        for n in range(2):
            ahead = first + depth + n

            @pl.when(ahead < count)
            def _():
                @pl.when(ahead >= held)
                def _():
                    for copy in copies_out(ahead - held):
                        copy.wait()

                for copy in copies_in(ahead):
                    copy.start()

        return carry

    lax.fori_loop(0, count // 2 + 1, pair, 0)
    for b in range(max(count - held, 0), count):
        for copy in copies_out(b):
            copy.wait()


def attend(seq_lens, k_cache, v_cache, queries, k_new, v_new, steps, start, count, partial=()):
    batch, key_rows, head_dim = k_cache.shape
    heads = queries.shape[1]
    rows = steps * heads
    depth, held = 16, 32
    cache = jax.ShapeDtypeStruct(k_cache.shape, BF16)
    flops = 4 * count * rows * key_rows * head_dim
    kernel = functools.partial(attend_kernel, steps, depth, start)

    def continued(*refs):
        kernel(*refs[:6], *refs[8:])

    return pl.pallas_call(
        continued if partial else kernel,
        name='attend',
        in_specs=[pl.BlockSpec(memory_space=pltpu.SMEM), IN_PLACE, IN_PLACE, IN_VMEM, IN_VMEM, IN_VMEM] + [IN_PLACE] * len(partial),
        out_specs=(IN_PLACE, IN_PLACE, IN_VMEM, IN_VMEM),
        out_shape=(cache, cache, jax.ShapeDtypeStruct((count, rows, head_dim), F32), jax.ShapeDtypeStruct((rows, 128), F32)),
        input_output_aliases={6: 0, 7: 1} if partial else {},
        scratch_shapes=[
            VMEM((held, key_rows, head_dim), BF16),
            VMEM((held, key_rows, head_dim), BF16),
            VMEM((rows, key_rows), jnp.int32),
            VMEM((rows, key_rows), F32),
            VMEM((rows, key_rows), F32),
            VMEM((rows, key_rows), BF16),
            VMEM((rows, key_rows), BF16),
            DMA((held, 2)),
            DMA((held, 2)),
        ],
        cost_estimate=pl.CostEstimate(flops=flops, bytes_accessed=4 * count * key_rows * head_dim * 2, transcendentals=0),
        compiler_params=pltpu.CompilerParams(vmem_limit_bytes=32 * MIB),
    )(seq_lens, k_cache, v_cache, queries.reshape(-1, head_dim), k_new.reshape(-1, head_dim), v_new.reshape(-1, head_dim), *partial)


def combine(mine, theirs, batch):
    scale = HEAD_DIM ** -0.5
    top = jnp.maximum(mine, theirs)
    fac_a, fac_b = jnp.exp((mine - top) * scale), jnp.exp((theirs - top) * scale)
    total = pltpu.roll(mine, 128 - batch, 1) * fac_a + pltpu.roll(theirs, 128 - batch, 1) * fac_b
    return top, fac_a, fac_b, total


def join_stats(top, total, batch):
    lane = lax.broadcasted_iota(jnp.int32, top.shape, 1)
    return jnp.where(lane < batch, top, pltpu.roll(total, batch, 1))


def places():
    me = lax.axis_index('sp')
    core = lax.rem(me, 2)
    return core, me + 1 - 2 * core, lax.rem(me + 2, 4)


def spans(chunks):
    return [(sum(chunks[:c]), seqs) for c, seqs in enumerate(chunks)]


def pair_kernel(chunks, batch, numer, stats, out, stat_d, recv_d, scaled, sem_stat, sems_d):
    rows = numer.shape[1] // 2
    core, other_core, _ = places()
    own = pl.ds(pl.multiple_of(core * rows, rows), rows)
    other = pl.ds(pl.multiple_of((1 - core) * rows, rows), rows)
    meet(other_core)
    stat_copy = remote(stats.at[other], stat_d, sem_stat, other_core)
    stat_copy.start()
    copies = []
    for c, (first, seqs) in enumerate(spans(chunks)):
        here = pl.ds(first, seqs)
        copy = remote(numer.at[here, other], recv_d.at[here], sems_d.at[c], other_core)
        copy.start()
        copies.append(copy)
    stat_copy.wait()
    top, fac_a, fac_b, total = combine(stats[own, :], stat_d[...], batch)
    out[numer.shape[0]] = join_stats(top, total, batch)
    scaled[0] = fac_a
    scaled[1] = fac_b
    for copy, (first, seqs) in zip(copies, spans(chunks)):
        copy.wait()
        for b in range(first, first + seqs):
            out[b] = numer[b, own, :] * scaled[0, :, b:b + 1] + recv_d[b] * scaled[1, :, b:b + 1]


def merge_pair(numer, stats, batch):
    count, rows, _ = numer.shape
    chunks = (8,) * (count // 8)
    return pl.pallas_call(
        functools.partial(pair_kernel, chunks, batch),
        name='merge_pair',
        out_shape=jax.ShapeDtypeStruct((count + 1, rows // 2, HEAD_DIM), F32),
        in_specs=[IN_VMEM, IN_VMEM],
        out_specs=IN_VMEM,
        scratch_shapes=[
            VMEM((rows // 2, 128), F32),
            VMEM((count, rows // 2, HEAD_DIM), F32),
            VMEM((2, rows // 2, 128), F32),
            DMA((2,)),
            DMA((len(chunks), 2)),
        ],
        compiler_params=pltpu.CompilerParams(collective_id=2, has_side_effects=True, vmem_limit_bytes=16 * MIB),
    )(numer, stats)


def merge_kernel(early_chunks, chunks, steps, numer, stats, early_own, early_theirs, wo_hbm, y_own, y_other, wo, stat_d, stat_send, stat_x, recv_d, send_x, recv_x, scaled, att_f32, attended, sems_w, sem_stat, sems_d, sems_x, sems_y):
    _, batch, hidden = y_own.shape
    rows = numer.shape[1] // 2
    half = rows // steps
    start = batch - numer.shape[0]
    core, other_core, other_chip = places()
    own = pl.ds(pl.multiple_of(core * rows, rows), rows)
    other = pl.ds(pl.multiple_of((1 - core) * rows, rows), rows)

    w_pieces = sems_w.shape[0]
    w_rows = half * HEAD_DIM // w_pieces
    w_first = core * (half * HEAD_DIM)
    meet(other_core, other_chip)

    stat_copy = remote(stats.at[other], stat_d, sem_stat.at[0], other_core)
    stat_copy.start()
    core_copies = []
    for c, (first, seqs) in enumerate(spans(chunks)):
        here = pl.ds(first, seqs)
        copy = remote(numer.at[here, other], recv_d.at[here], sems_d.at[c], other_core)
        copy.start()
        core_copies.append(copy)
    w_copies = []
    for p in range(w_pieces):
        src = wo_hbm.at[pl.ds(pl.multiple_of(w_first + p * w_rows, w_rows), w_rows), :]
        copy = pltpu.make_async_copy(src, wo.at[pl.ds(p * w_rows, w_rows), :], sems_w.at[p])
        copy.start()
        w_copies.append(copy)

    stat_copy.wait()
    top, fac_a, fac_b, total = combine(stats[own, :], stat_d[...], batch)
    stat_send[...] = join_stats(top, total, batch)
    scaled[0] = fac_a
    scaled[1] = fac_b
    chip_stat_copy = remote(stat_send, stat_x, sem_stat.at[1], other_chip)
    chip_stat_copy.start()

    chip_copies = []
    for c, (first, seqs) in enumerate(spans(chunks)):
        core_copies[c].wait()
        for i in range(first, first + seqs):
            b = start + i
            joined = numer[i, own, :] * scaled[0, :, b:b + 1] + recv_d[i] * scaled[1, :, b:b + 1]
            send_x[i] = joined.reshape(send_x.shape[1:])
        here = pl.ds(first, seqs)
        if c < len(chunks) - 1:
            views = [(send_x.at[here], recv_x.at[here])]
        else:
            views = [(send_x.at[here, :, part], recv_x.at[here, :, part]) for part in range(2)]
        for src, dst in views:
            copy = remote(src, dst, sems_x.at[len(chip_copies)], other_chip)
            copy.start()
            chip_copies.append(copy)

    width = 512
    y_copies = []

    def finish(mine, theirs, first, seqs, begin, parts):
        size = half // 2
        for i in range(first, first + seqs):
            b = begin + i
            for t in range(steps):
                for part in parts:
                    at = t * half + part * size
                    here = slice(at, at + size)
                    merged = mine[i, t, part] * scaled[0, here, b:b + 1] + theirs[i, t, part] * scaled[1, here, b:b + 1]
                    att_f32[pl.ds((i - first) * rows + at, size), :] = merged
        for t in range(steps):
            for h in range(parts[0] * size, (parts[-1] + 1) * size):
                values = att_f32[pl.ds(t * half + h, seqs, stride=rows), :]
                attended[t * seqs:(t + 1) * seqs, h * HEAD_DIM:(h + 1) * HEAD_DIM] = values
        if not y_copies:
            for copy in w_copies:
                copy.wait()
        at = begin + first
        depth = slice(parts[0] * size * HEAD_DIM, (parts[-1] + 1) * size * HEAD_DIM)

        @pl.loop(0, hidden // width)
        def _(j):
            cols = pl.ds(pl.multiple_of(j * width, width), width)
            out = jnp.dot(attended[:steps * seqs, depth].astype(BF16), wo[depth, cols], preferred_element_type=F32)
            for t in range(steps):
                if parts[0] == 0:
                    y_own[t, at:at + seqs, cols] = out[t * seqs:(t + 1) * seqs, :]
                else:
                    y_own[t, at:at + seqs, cols] += out[t * seqs:(t + 1) * seqs, :]

        if parts[-1] == 1:
            here = pl.ds(at, seqs)
            copy = remote(y_own.at[:, here, :], y_other.at[:, here, :], sems_y.at[len(y_copies)], other_core)
            copy.start()
            y_copies.append(copy)

    def set_factors(mine, theirs):
        _, fac_a, fac_b, total = combine(mine, theirs, batch)
        scaled[0] = fac_a / total
        scaled[1] = fac_b / total

    set_factors(early_own[start].reshape(rows, 128), early_theirs[start].reshape(rows, 128))
    for first, seqs in spans(early_chunks):
        finish(early_own, early_theirs, first, seqs, 0, (0, 1))
    chip_stat_copy.wait()
    set_factors(stat_send[...], stat_x[...])
    for c, (first, seqs) in enumerate(spans(chunks)):
        for parts in [(0, 1)] if c < len(chunks) - 1 else [(0,), (1,)]:
            chip_copies[c + parts[0]].wait()
            finish(send_x, recv_x, first, seqs, start, parts)
    for copy in y_copies:
        copy.wait()


def merge(numer, stats, early_own, early_theirs, w_o, steps, batch):
    count, rows, _ = numer.shape
    hidden = w_o.shape[1]
    early_chunks = (16, 8)
    chunks = (8, 16, 8, 8)
    largest = max(chunks + early_chunks)
    part = jax.ShapeDtypeStruct((steps, batch, hidden), F32)
    stat = VMEM((rows // 2, 128), F32)
    split = (steps, 2, rows // (4 * steps), HEAD_DIM)
    moved = VMEM((count,) + split, F32)
    return pl.pallas_call(
        functools.partial(merge_kernel, early_chunks, chunks, steps),
        name='merge',
        out_shape=(part, part),
        in_specs=[IN_VMEM] * 4 + [IN_PLACE],
        out_specs=(IN_VMEM, IN_VMEM),
        scratch_shapes=[
            VMEM((w_o.shape[0] // 2, hidden), BF16),
            stat,
            stat,
            stat,
            VMEM((count, rows // 2, HEAD_DIM), F32),
            moved,
            moved,
            VMEM((2, rows // 2, 128), F32),
            VMEM((largest * rows // 2, HEAD_DIM), F32),
            VMEM((steps * largest, w_o.shape[0] // 2), F32),
            DMA((8,)),
            DMA((2, 2)),
            DMA((len(chunks), 2)),
            DMA((len(chunks) + 1, 2)),
            DMA((len(chunks) + len(early_chunks), 2)),
        ],
        compiler_params=pltpu.CompilerParams(collective_id=0, has_side_effects=True, vmem_limit_bytes=40 * MIB),
    )(numer, stats, early_own.reshape((-1,) + split), early_theirs.reshape((-1,) + split), w_o)


def solution(mesh):
    def per_device(x_steps, k_local, v_local, seq_lens, norm_gain, w_q, w_k, w_v, w_o, q_gain, k_gain):
        steps, batch, _ = x_steps.shape
        early = 24
        rope, gains = small_tables(seq_lens, steps, norm_gain, q_gain, k_gain)
        fresh = project(x_steps, rope, gains, w_q, w_k, w_v)
        flat = (batch, -1, HEAD_DIM)
        caches = (k_local.reshape(flat), v_local.reshape(flat))
        k_part, v_part, early_numer, early_stats = attend(seq_lens, *caches, *fresh, steps, 0, early)
        early_own = merge_pair(early_numer, early_stats, batch)
        early_theirs = lax.ppermute(early_own, 'sp', [(i, (i + 2) % 4) for i in range(4)])
        k_out, v_out, numer, stats = attend(seq_lens, *caches, *fresh, steps, early, batch - early, (k_part, v_part))
        own, other = merge(numer, stats, early_own, early_theirs, w_o, steps, batch)
        y_steps = (x_steps.astype(F32) + (own + other)).astype(BF16)
        return y_steps, k_out.reshape(k_local.shape), v_out.reshape(v_local.shape)

    cache_spec = P('dp', 'sp', None, None)
    step_spec = P(None, 'dp', None)
    return jax.shard_map(per_device, mesh=mesh, in_specs=(step_spec, cache_spec, cache_spec, P('dp'), P(), P(), P(), P(), P(), P(), P()), out_specs=(step_spec, cache_spec, cache_spec), check_vma=False)
```

```python
import functools
import math

import jax
import jax.numpy as jnp
from jax import lax
from jax.experimental import pallas as pl
from jax.experimental.pallas import tpu as pltpu
from jax.sharding import PartitionSpec as P

NORM_EPS = 1e-6
ROPE_BASE = 1000000.0
MASKED_MAX = -1e30
HEAD_DIM = 128
F32 = jnp.float32
BF16 = jnp.bfloat16
MIB = 1024 * 1024
VMEM = pltpu.VMEM
DMA = pltpu.SemaphoreType.DMA
IN_VMEM = pl.BlockSpec(memory_space=VMEM)
IN_PLACE = pl.BlockSpec(memory_space=pl.ANY)


def small_tables(seq_lens, steps, norm_gain, q_gain, k_gain):
    half = HEAD_DIM // 2
    positions = (seq_lens[None, :] + jnp.arange(steps, dtype=jnp.int32)[:, None]).reshape(-1)
    inv_freq = jnp.exp(jnp.arange(half, dtype=F32) * (-2.0 * math.log(ROPE_BASE) / HEAD_DIM))
    angles = positions.astype(F32)[:, None] * inv_freq
    cosine = jnp.cos(angles)
    sine = jnp.sin(angles)
    rope = jnp.concatenate([jnp.concatenate([cosine, cosine], axis=-1), jnp.concatenate([-sine, sine], axis=-1)], axis=0)
    gains = jnp.concatenate([norm_gain, q_gain, k_gain]).astype(F32).reshape(-1, HEAD_DIM)
    return rope, gains


def remote(src, dst, sems, peer):
    return pltpu.make_async_remote_copy(src_ref=src, dst_ref=dst, send_sem=sems.at[0], recv_sem=sems.at[1], device_id={'sp': peer}, device_id_type=pl.DeviceIdType.MESH)


def meet(*peers):
    barrier = pltpu.get_barrier_semaphore()
    for peer in peers:
        pl.semaphore_signal(barrier, inc=1, device_id={'sp': peer}, device_id_type=pl.DeviceIdType.MESH)
    pl.semaphore_wait(barrier, len(peers))


def project_kernel(width, heads, kv_heads, x_hbm, rope_ref, gain_ref, wq_hbm, wk_hbm, wv_hbm, q_ref, k_ref, v_ref, x_rows, normed, acc, wbuf, sem_x, sems_w, sems_q, sems_k, sems_v):
    rows, hidden = x_rows.shape
    per_block = width // HEAD_DIM
    core = lax.rem(lax.axis_index('sp'), 2)
    other_core = lax.axis_index('sp') + 1 - 2 * core

    x_copy = pltpu.make_async_copy(x_hbm, x_rows, sem_x)
    x_copy.start()
    blocks = [(wk_hbm, k_ref, sems_k, kv_heads, 0)]
    blocks += [(wq_hbm, q_ref, sems_q, heads, i) for i in range(heads // 2 // per_block)]
    blocks += [(wv_hbm, v_ref, sems_v, kv_heads, 0)]
    w_copies = []
    for n, (w_hbm, _, _, total, i) in enumerate(blocks):
        cols = pl.ds(pl.multiple_of(core * (total // 2 * HEAD_DIM) + i * width, width), width)
        w_copies.append(pltpu.make_async_copy(w_hbm.at[:, cols], wbuf.at[n], sems_w.at[n]))

    w_copies[0].start()
    meet(other_core)
    x_copy.wait()
    w_copies[1].start()

    @pl.loop(0, rows // 16)
    def _(i):
        here = pl.ds(pl.multiple_of(i * 16, 16), 16)
        values = x_rows[here, :].astype(F32)
        inv_rms = lax.rsqrt(jnp.mean(values * values, axis=-1, keepdims=True) + NORM_EPS)
        for n in range(hidden // HEAD_DIM):
            lanes = slice(n * HEAD_DIM, (n + 1) * HEAD_DIM)
            normed[here, lanes] = (x_rows[here, lanes].astype(F32) * inv_rms * gain_ref[n:n + 1, :]).astype(BF16)

    def finish(n):
        w_hbm, out_ref, sems, total, i = blocks[n]
        first = core * (total // 2) + i * per_block
        for j in range(per_block):
            values = acc[n % 2, :, j * HEAD_DIM:(j + 1) * HEAD_DIM].astype(BF16).astype(F32)
            if out_ref is not v_ref:
                row = hidden // HEAD_DIM + (1 if out_ref is k_ref else 0)
                inv_rms = lax.rsqrt(jnp.mean(values * values, axis=-1, keepdims=True) + NORM_EPS)
                scaled = values * inv_rms * gain_ref[row:row + 1, :]
                values = scaled * rope_ref[:rows, :] + pltpu.roll(scaled, HEAD_DIM // 2, 1) * rope_ref[rows:, :]
                values = values.astype(BF16).astype(F32)
            out_ref[:, first + j, :, :] = values.reshape(rows // 8, 8, HEAD_DIM)

    def send(n):
        _, out_ref, sems, total, i = blocks[n]
        there = pl.ds(core * (total // 2) + i * per_block, per_block)
        copy = remote(out_ref.at[:, there], out_ref.at[:, there], sems.at[i], other_core)
        copy.start()
        return copy

    sends = []
    for n in range(len(blocks)):
        w_copies[n].wait()
        if n + 2 < len(blocks):
            w_copies[n + 2].start()
        acc[n % 2] = jnp.dot(normed[...], wbuf[n], preferred_element_type=F32)
        if n > 0:
            finish(n - 1)
            sends.append(send(n - 1))
    finish(len(blocks) - 1)
    sends.append(send(len(blocks) - 1))
    for copy in sends:
        copy.wait()


def project(x_steps, rope, gains, w_q, w_k, w_v):
    steps, batch, hidden = x_steps.shape
    rows = steps * batch
    heads = w_q.shape[1] // HEAD_DIM
    kv_heads = w_k.shape[1] // HEAD_DIM
    width = kv_heads // 2 * HEAD_DIM
    q_blocks = heads // kv_heads
    return pl.pallas_call(
        functools.partial(project_kernel, width, heads, kv_heads),
        name='project',
        out_shape=tuple(jax.ShapeDtypeStruct((rows // 8, n, 8, HEAD_DIM), F32) for n in (heads, kv_heads, kv_heads)),
        in_specs=[pl.BlockSpec(memory_space=pltpu.HBM), IN_VMEM, IN_VMEM] + [IN_PLACE] * 3,
        out_specs=(IN_VMEM,) * 3,
        scratch_shapes=[
            VMEM((rows, hidden), BF16),
            VMEM((rows, hidden), BF16),
            VMEM((2, rows, width), F32),
            VMEM((q_blocks + 2, hidden, width), BF16),
            DMA,
            DMA((q_blocks + 2,)),
            DMA((q_blocks, 2)),
            DMA((1, 2)),
            DMA((1, 2)),
        ],
        compiler_params=pltpu.CompilerParams(collective_id=1, has_side_effects=True, vmem_limit_bytes=40 * MIB),
    )(pltpu.with_memory_space_constraint(x_steps.reshape(rows, hidden), pltpu.HBM), rope, gains, w_q, w_k, w_v)


def attend_kernel(steps, depth, start, lens_ref, k_hbm, v_hbm, q_ref, kn_ref, vn_ref, ko_hbm, vo_hbm, num_ref, stat_ref, k_buf, v_buf, dist, scores_0, scores_1, weights_0, weights_1, sems_in, sems_out):
    held, key_rows, _ = k_buf.shape
    batch = lens_ref.shape[0]
    count = num_ref.shape[0]
    heads, kv_heads = q_ref.shape[0] // (steps * batch), kn_ref.shape[0] // (steps * batch)
    slots = key_rows // kv_heads
    rows = steps * heads
    half = heads // 2
    first_slot = lax.axis_index('sp') * slots
    upper = lax.broadcasted_iota(jnp.int32, (2 * kv_heads, HEAD_DIM), 0) >= kv_heads
    scale = HEAD_DIM ** -0.5 * math.log2(math.e)
    scores_refs, weights_refs = (scores_0, scores_1), (weights_0, weights_1)

    def copies_in(b):
        slot = lax.rem(b, held)
        return (pltpu.make_async_copy(k_hbm.at[start + b], k_buf.at[slot], sems_in.at[slot, 0]),
                pltpu.make_async_copy(v_hbm.at[start + b], v_buf.at[slot], sems_in.at[slot, 1]))

    def copies_out(b):
        slot = lax.rem(b, held)
        return (pltpu.make_async_copy(k_buf.at[slot], ko_hbm.at[start + b], sems_out.at[slot, 0]),
                pltpu.make_async_copy(v_buf.at[slot], vo_hbm.at[start + b], sems_out.at[slot, 1]))

    for b in range(depth):
        for copy in copies_in(b):
            copy.start()

    lane = lax.broadcasted_iota(jnp.int32, (rows, 128), 1)
    stat_ref[...] = jnp.where(lane < batch, MASKED_MAX, 0.0)
    row = lax.broadcasted_iota(jnp.int32, (rows, key_rows), 0)
    col = lax.broadcasted_iota(jnp.int32, (rows, key_rows), 1)
    row_half, in_half = row // (steps * half), lax.rem(row, steps * half)
    row_kv = (row_half * half + lax.rem(in_half, half)) // (heads // kv_heads)
    dist[...] = jnp.where(row_kv == lax.rem(col, kv_heads), col // kv_heads - in_half // half, 1 << 24)

    def rel_of(b):
        return lens_ref[start + jnp.clip(b, 0, count - 1)] - first_slot

    def receive(b):
        slot = lax.rem(b, held)
        for copy in copies_in(b):
            copy.wait()
        rel = rel_of(b)
        for t in range(steps):
            at = rel + t

            @pl.when((at >= 0) & (at < slots))
            def _():
                base = pl.multiple_of((at >> 1) * (2 * kv_heads), 2 * kv_heads)
                mine = upper == ((at & 1) == 1)
                r = t * batch + start + b
                new_rows = pl.ds((r >> 3) * (8 * kv_heads) + (r & 7), kv_heads, stride=8)
                for buf, new in ((k_buf, kn_ref), (v_buf, vn_ref)):
                    fresh = new[new_rows, :]
                    fresh = jnp.concatenate([fresh, fresh], axis=0)
                    old = buf[slot, pl.ds(base, 2 * kv_heads), :].astype(F32)
                    buf[slot, pl.ds(base, 2 * kv_heads), :] = jnp.where(mine, fresh, old).astype(BF16)

    def score(j, parity):
        b = jnp.clip(j, 0, count - 1)
        pieces = []
        for h in range(2):
            for t in range(steps):
                r = t * batch + start + b
                at = (r >> 3) * (8 * heads) + (r & 7) + h * (8 * half)
                pieces.append(q_ref[pl.ds(at, half, stride=8), :].astype(BF16))
        query = jnp.concatenate(pieces, axis=0)
        scores_refs[parity][...] = lax.dot_general(query, k_buf[lax.rem(b, held)], (((1,), (1,)), ((), ())), preferred_element_type=F32)

    def soften(j, parity):
        rel = rel_of(j)
        known = (j >= 0) & (j < count)
        max_lane = jnp.where(known, start + j, 1024)
        sum_lane = jnp.where(known, start + j + batch, 1024)
        size = 16
        block_lane = lax.broadcasted_iota(jnp.int32, (size, 128), 1)
        for first in range(0, rows, size):
            here = slice(first, first + size)
            scores = jnp.where(dist[here, :] <= rel, scores_refs[parity][here, :], -jnp.inf)
            row_max = jnp.maximum(jnp.max(scores, axis=1, keepdims=True), MASKED_MAX)
            weights = jnp.exp2((scores - row_max) * scale)
            row_sum = jnp.sum(weights, axis=1, keepdims=True)
            weights_refs[parity][here, :] = weights.astype(BF16)
            stats = jnp.where(block_lane == max_lane, row_max, stat_ref[here, :])
            stat_ref[here, :] = jnp.where(block_lane == sum_lane, row_sum, stats)

    def mix(j, parity):
        b = jnp.clip(j, 0, count - 1)
        mixed = jnp.dot(weights_refs[parity][...], v_buf[lax.rem(b, held)], preferred_element_type=F32)
        num_ref[b] = jnp.where(rel_of(j) + steps - 1 >= 0, mixed, 0.0)

    def pair(k, carry):
        first = 2 * k

        @pl.when(first < count)
        def _():
            receive(first)
            receive(first + 1)

        longest = functools.reduce(jnp.maximum, [rel_of(first + n) for n in range(-2, 2)])
        visible = longest + steps - 1 >= 0

        @pl.when(visible)
        def _():
            for parity in range(2):
                score(first + parity, parity)
                soften(first + parity - 1, 1 - parity)
                mix(first + parity - 2, parity)

        @pl.when(jnp.logical_not(visible))
        def _():
            for parity in range(2):
                num_ref[jnp.clip(first + parity - 2, 0, count - 1)] = jnp.zeros((rows, HEAD_DIM), F32)

        @pl.when(first >= 2)
        def _():
            for n in range(2):
                for copy in copies_out(first - 2 + n):
                    copy.start()

        for n in range(2):
            ahead = first + depth + n

            @pl.when(ahead < count)
            def _():
                @pl.when(ahead >= held)
                def _():
                    for copy in copies_out(ahead - held):
                        copy.wait()

                for copy in copies_in(ahead):
                    copy.start()

        return carry

    lax.fori_loop(0, count // 2 + 1, pair, 0)
    for b in range(max(count - held, 0), count):
        for copy in copies_out(b):
            copy.wait()


def attend(seq_lens, k_cache, v_cache, queries, k_new, v_new, steps, start, count, partial=()):
    batch, key_rows, head_dim = k_cache.shape
    heads = queries.shape[1]
    rows = steps * heads
    depth, held = 8, 32
    cache = jax.ShapeDtypeStruct(k_cache.shape, BF16)
    flops = 4 * count * rows * key_rows * head_dim
    kernel = functools.partial(attend_kernel, steps, depth, start)

    def continued(*refs):
        kernel(*refs[:6], *refs[8:])

    return pl.pallas_call(
        continued if partial else kernel,
        name='attend',
        in_specs=[pl.BlockSpec(memory_space=pltpu.SMEM), IN_PLACE, IN_PLACE, IN_VMEM, IN_VMEM, IN_VMEM] + [IN_PLACE] * len(partial),
        out_specs=(IN_PLACE, IN_PLACE, IN_VMEM, IN_VMEM),
        out_shape=(cache, cache, jax.ShapeDtypeStruct((count, rows, head_dim), F32), jax.ShapeDtypeStruct((rows, 128), F32)),
        input_output_aliases={6: 0, 7: 1} if partial else {},
        scratch_shapes=[
            VMEM((held, key_rows, head_dim), BF16),
            VMEM((held, key_rows, head_dim), BF16),
            VMEM((rows, key_rows), jnp.int32),
            VMEM((rows, key_rows), F32),
            VMEM((rows, key_rows), F32),
            VMEM((rows, key_rows), BF16),
            VMEM((rows, key_rows), BF16),
            DMA((held, 2)),
            DMA((held, 2)),
        ],
        cost_estimate=pl.CostEstimate(flops=flops, bytes_accessed=4 * count * key_rows * head_dim * 2, transcendentals=0),
        compiler_params=pltpu.CompilerParams(vmem_limit_bytes=32 * MIB),
    )(seq_lens, k_cache, v_cache, queries.reshape(-1, head_dim), k_new.reshape(-1, head_dim), v_new.reshape(-1, head_dim), *partial)


def combine(mine, theirs, batch):
    scale = HEAD_DIM ** -0.5
    top = jnp.maximum(mine, theirs)
    fac_a, fac_b = jnp.exp((mine - top) * scale), jnp.exp((theirs - top) * scale)
    total = pltpu.roll(mine, 128 - batch, 1) * fac_a + pltpu.roll(theirs, 128 - batch, 1) * fac_b
    return top, fac_a, fac_b, total


def join_stats(top, total, batch):
    lane = lax.broadcasted_iota(jnp.int32, top.shape, 1)
    return jnp.where(lane < batch, top, pltpu.roll(total, batch, 1))


def places():
    me = lax.axis_index('sp')
    core = lax.rem(me, 2)
    return core, me + 1 - 2 * core, lax.rem(me + 2, 4)


def spans(chunks):
    return [(sum(chunks[:c]), seqs) for c, seqs in enumerate(chunks)]


def pair_kernel(chunks, batch, numer, stats, out, stat_d, recv_d, scaled, sem_stat, sems_d):
    rows = numer.shape[1] // 2
    core, other_core, _ = places()
    own = pl.ds(pl.multiple_of(core * rows, rows), rows)
    other = pl.ds(pl.multiple_of((1 - core) * rows, rows), rows)
    meet(other_core)
    stat_copy = remote(stats.at[other], stat_d, sem_stat, other_core)
    stat_copy.start()
    copies = []
    for c, (first, seqs) in enumerate(spans(chunks)):
        here = pl.ds(first, seqs)
        copy = remote(numer.at[here, other], recv_d.at[here], sems_d.at[c], other_core)
        copy.start()
        copies.append(copy)
    stat_copy.wait()
    top, fac_a, fac_b, total = combine(stats[own, :], stat_d[...], batch)
    out[numer.shape[0]] = join_stats(top, total, batch)
    scaled[0] = fac_a
    scaled[1] = fac_b
    for copy, (first, seqs) in zip(copies, spans(chunks)):
        copy.wait()
        for b in range(first, first + seqs):
            out[b] = numer[b, own, :] * scaled[0, :, b:b + 1] + recv_d[b] * scaled[1, :, b:b + 1]


def merge_pair(numer, stats, batch):
    count, rows, _ = numer.shape
    chunks = (8,) * (count // 8)
    return pl.pallas_call(
        functools.partial(pair_kernel, chunks, batch),
        name='merge_pair',
        out_shape=jax.ShapeDtypeStruct((count + 1, rows // 2, HEAD_DIM), F32),
        in_specs=[IN_VMEM, IN_VMEM],
        out_specs=IN_VMEM,
        scratch_shapes=[
            VMEM((rows // 2, 128), F32),
            VMEM((count, rows // 2, HEAD_DIM), F32),
            VMEM((2, rows // 2, 128), F32),
            DMA((2,)),
            DMA((len(chunks), 2)),
        ],
        compiler_params=pltpu.CompilerParams(collective_id=2, has_side_effects=True, vmem_limit_bytes=16 * MIB),
    )(numer, stats)


def merge_kernel(early_chunks, chunks, steps, numer, stats, early_own, early_theirs, wo_hbm, y_own, y_other, wo, stat_d, stat_send, stat_x, recv_d, send_x, recv_x, scaled, att_f32, attended, sems_w, sem_stat, sems_d, sems_x, sems_y):
    _, batch, hidden = y_own.shape
    rows = numer.shape[1] // 2
    half = rows // steps
    start = batch - numer.shape[0]
    core, other_core, other_chip = places()
    own = pl.ds(pl.multiple_of(core * rows, rows), rows)
    other = pl.ds(pl.multiple_of((1 - core) * rows, rows), rows)

    w_pieces = sems_w.shape[0]
    w_rows = half * HEAD_DIM // w_pieces
    w_first = core * (half * HEAD_DIM)
    meet(other_core, other_chip)

    stat_copy = remote(stats.at[other], stat_d, sem_stat.at[0], other_core)
    stat_copy.start()
    core_copies = []
    for c, (first, seqs) in enumerate(spans(chunks)):
        here = pl.ds(first, seqs)
        copy = remote(numer.at[here, other], recv_d.at[here], sems_d.at[c], other_core)
        copy.start()
        core_copies.append(copy)
    w_copies = []
    for p in range(w_pieces):
        src = wo_hbm.at[pl.ds(pl.multiple_of(w_first + p * w_rows, w_rows), w_rows), :]
        copy = pltpu.make_async_copy(src, wo.at[pl.ds(p * w_rows, w_rows), :], sems_w.at[p])
        copy.start()
        w_copies.append(copy)

    stat_copy.wait()
    top, fac_a, fac_b, total = combine(stats[own, :], stat_d[...], batch)
    stat_send[...] = join_stats(top, total, batch)
    scaled[0] = fac_a
    scaled[1] = fac_b
    chip_stat_copy = remote(stat_send, stat_x, sem_stat.at[1], other_chip)
    chip_stat_copy.start()

    chip_copies = []
    for c, (first, seqs) in enumerate(spans(chunks)):
        core_copies[c].wait()
        for i in range(first, first + seqs):
            b = start + i
            joined = numer[i, own, :] * scaled[0, :, b:b + 1] + recv_d[i] * scaled[1, :, b:b + 1]
            send_x[i] = joined.reshape(send_x.shape[1:])
        here = pl.ds(first, seqs)
        if c < len(chunks) - 1:
            views = [(send_x.at[here], recv_x.at[here])]
        else:
            views = [(send_x.at[here, :, part], recv_x.at[here, :, part]) for part in range(2)]
        for src, dst in views:
            copy = remote(src, dst, sems_x.at[len(chip_copies)], other_chip)
            copy.start()
            chip_copies.append(copy)

    width = 512
    y_copies = []

    def finish(mine, theirs, first, seqs, begin, parts):
        size = half // 2
        for i in range(first, first + seqs):
            b = begin + i
            for t in range(steps):
                for part in parts:
                    at = t * half + part * size
                    here = slice(at, at + size)
                    merged = mine[i, t, part] * scaled[0, here, b:b + 1] + theirs[i, t, part] * scaled[1, here, b:b + 1]
                    att_f32[pl.ds((i - first) * rows + at, size), :] = merged
        for t in range(steps):
            for h in range(parts[0] * size, (parts[-1] + 1) * size):
                values = att_f32[pl.ds(t * half + h, seqs, stride=rows), :]
                attended[t * seqs:(t + 1) * seqs, h * HEAD_DIM:(h + 1) * HEAD_DIM] = values
        if not y_copies:
            for copy in w_copies:
                copy.wait()
        at = begin + first
        depth = slice(parts[0] * size * HEAD_DIM, (parts[-1] + 1) * size * HEAD_DIM)

        here = pl.ds(at, seqs)
        span = hidden // 2
        for side in range(2):

            @pl.loop(side * span // width, (side + 1) * span // width)
            def _(j):
                cols = pl.ds(pl.multiple_of(j * width, width), width)
                out = jnp.dot(attended[:steps * seqs, depth].astype(BF16), wo[depth, cols], preferred_element_type=F32)
                for t in range(steps):
                    if parts[0] == 0:
                        y_own[t, at:at + seqs, cols] = out[t * seqs:(t + 1) * seqs, :]
                    else:
                        y_own[t, at:at + seqs, cols] += out[t * seqs:(t + 1) * seqs, :]

            if parts[-1] == 1:
                lanes = pl.ds(side * span, span)
                copy = remote(y_own.at[:, here, lanes], y_other.at[:, here, lanes], sems_y.at[len(y_copies)], other_core)
                copy.start()
                y_copies.append(copy)

    def set_factors(mine, theirs):
        _, fac_a, fac_b, total = combine(mine, theirs, batch)
        scaled[0] = fac_a / total
        scaled[1] = fac_b / total

    set_factors(early_own[start].reshape(rows, 128), early_theirs[start].reshape(rows, 128))
    for first, seqs in spans(early_chunks):
        finish(early_own, early_theirs, first, seqs, 0, (0, 1))
    chip_stat_copy.wait()
    set_factors(stat_send[...], stat_x[...])
    for c, (first, seqs) in enumerate(spans(chunks)):
        for parts in [(0, 1)] if c < len(chunks) - 1 else [(0,), (1,)]:
            chip_copies[c + parts[0]].wait()
            finish(send_x, recv_x, first, seqs, start, parts)
    for copy in y_copies:
        copy.wait()


def merge(numer, stats, early_own, early_theirs, w_o, steps, batch):
    count, rows, _ = numer.shape
    hidden = w_o.shape[1]
    early_chunks = (16, 8)
    chunks = (8, 16, 16)
    largest = max(chunks + early_chunks)
    part = jax.ShapeDtypeStruct((steps, batch, hidden), F32)
    stat = VMEM((rows // 2, 128), F32)
    split = (steps, 2, rows // (4 * steps), HEAD_DIM)
    moved = VMEM((count,) + split, F32)
    return pl.pallas_call(
        functools.partial(merge_kernel, early_chunks, chunks, steps),
        name='merge',
        out_shape=(part, part),
        in_specs=[IN_VMEM] * 4 + [IN_PLACE],
        out_specs=(IN_VMEM, IN_VMEM),
        scratch_shapes=[
            VMEM((w_o.shape[0] // 2, hidden), BF16),
            stat,
            stat,
            stat,
            VMEM((count, rows // 2, HEAD_DIM), F32),
            moved,
            moved,
            VMEM((2, rows // 2, 128), F32),
            VMEM((largest * rows // 2, HEAD_DIM), F32),
            VMEM((steps * largest, w_o.shape[0] // 2), F32),
            DMA((8,)),
            DMA((2, 2)),
            DMA((len(chunks), 2)),
            DMA((len(chunks) + 1, 2)),
            DMA((2 * (len(chunks) + len(early_chunks)), 2)),
        ],
        compiler_params=pltpu.CompilerParams(collective_id=0, has_side_effects=True, vmem_limit_bytes=40 * MIB),
    )(numer, stats, early_own.reshape((-1,) + split), early_theirs.reshape((-1,) + split), w_o)


def solution(mesh):
    def per_device(x_steps, k_local, v_local, seq_lens, norm_gain, w_q, w_k, w_v, w_o, q_gain, k_gain):
        steps, batch, _ = x_steps.shape
        early = 24
        rope, gains = small_tables(seq_lens, steps, norm_gain, q_gain, k_gain)
        fresh = project(x_steps, rope, gains, w_q, w_k, w_v)
        flat = (batch, -1, HEAD_DIM)
        caches = (k_local.reshape(flat), v_local.reshape(flat))
        k_part, v_part, early_numer, early_stats = attend(seq_lens, *caches, *fresh, steps, 0, early)
        early_own = merge_pair(early_numer, early_stats, batch)
        early_theirs = lax.ppermute(early_own, 'sp', [(i, (i + 2) % 4) for i in range(4)])
        k_out, v_out, numer, stats = attend(seq_lens, *caches, *fresh, steps, early, batch - early, (k_part, v_part))
        own, other = merge(numer, stats, early_own, early_theirs, w_o, steps, batch)
        y_steps = (x_steps.astype(F32) + (own + other)).astype(BF16)
        return y_steps, k_out.reshape(k_local.shape), v_out.reshape(v_local.shape)

    cache_spec = P('dp', 'sp', None, None)
    step_spec = P(None, 'dp', None)
    return jax.shard_map(per_device, mesh=mesh, in_specs=(step_spec, cache_spec, cache_spec, P('dp'), P(), P(), P(), P(), P(), P(), P()), out_specs=(step_spec, cache_spec, cache_spec), check_vma=False)
```

```python
import functools
import math

import jax
import jax.numpy as jnp
from jax import lax
from jax.experimental import pallas as pl
from jax.experimental.pallas import tpu as pltpu
from jax.sharding import PartitionSpec as P

NORM_EPS = 1e-6
ROPE_BASE = 1000000.0
MASKED_MAX = -1e30
HEAD_DIM = 128
F32 = jnp.float32
BF16 = jnp.bfloat16
MIB = 1024 * 1024
VMEM = pltpu.VMEM
DMA = pltpu.SemaphoreType.DMA
IN_VMEM = pl.BlockSpec(memory_space=VMEM)
IN_PLACE = pl.BlockSpec(memory_space=pl.ANY)


def small_tables(seq_lens, steps, norm_gain, q_gain, k_gain):
    half = HEAD_DIM // 2
    positions = (seq_lens[None, :] + jnp.arange(steps, dtype=jnp.int32)[:, None]).reshape(-1)
    inv_freq = jnp.exp(jnp.arange(half, dtype=F32) * (-2.0 * math.log(ROPE_BASE) / HEAD_DIM))
    angles = positions.astype(F32)[:, None] * inv_freq
    cosine = jnp.cos(angles)
    sine = jnp.sin(angles)
    rope = jnp.concatenate([jnp.concatenate([cosine, cosine], axis=-1), jnp.concatenate([-sine, sine], axis=-1)], axis=0)
    gains = jnp.concatenate([norm_gain, q_gain, k_gain]).astype(F32).reshape(-1, HEAD_DIM)
    return rope, gains


def remote(src, dst, sems, peer):
    return pltpu.make_async_remote_copy(src_ref=src, dst_ref=dst, send_sem=sems.at[0], recv_sem=sems.at[1], device_id={'sp': peer}, device_id_type=pl.DeviceIdType.MESH)


def meet(*peers):
    barrier = pltpu.get_barrier_semaphore()
    for peer in peers:
        pl.semaphore_signal(barrier, inc=1, device_id={'sp': peer}, device_id_type=pl.DeviceIdType.MESH)
    pl.semaphore_wait(barrier, len(peers))


def project_kernel(width, heads, kv_heads, x_hbm, rope_ref, gain_ref, wq_hbm, wk_hbm, wv_hbm, q_ref, k_ref, v_ref, x_rows, normed, acc, wbuf, sem_x, sems_w, sems_q, sems_k, sems_v):
    rows, hidden = x_rows.shape
    per_block = width // HEAD_DIM
    core = lax.rem(lax.axis_index('sp'), 2)
    other_core = lax.axis_index('sp') + 1 - 2 * core

    x_copy = pltpu.make_async_copy(x_hbm, x_rows, sem_x)
    x_copy.start()
    blocks = [(wk_hbm, k_ref, sems_k, kv_heads, 0)]
    blocks += [(wq_hbm, q_ref, sems_q, heads, i) for i in range(heads // 2 // per_block)]
    blocks += [(wv_hbm, v_ref, sems_v, kv_heads, 0)]
    w_copies = []
    for n, (w_hbm, _, _, total, i) in enumerate(blocks):
        cols = pl.ds(pl.multiple_of(core * (total // 2 * HEAD_DIM) + i * width, width), width)
        w_copies.append(pltpu.make_async_copy(w_hbm.at[:, cols], wbuf.at[n], sems_w.at[n]))

    w_copies[0].start()
    meet(other_core)
    x_copy.wait()
    w_copies[1].start()

    @pl.loop(0, rows // 16, unroll=4)
    def _(i):
        here = pl.ds(pl.multiple_of(i * 16, 16), 16)
        values = x_rows[here, :].astype(F32)
        inv_rms = lax.rsqrt(jnp.mean(values * values, axis=-1, keepdims=True) + NORM_EPS)
        for n in range(hidden // HEAD_DIM):
            lanes = slice(n * HEAD_DIM, (n + 1) * HEAD_DIM)
            normed[here, lanes] = (x_rows[here, lanes].astype(F32) * inv_rms * gain_ref[n:n + 1, :]).astype(BF16)

    def finish(n):
        w_hbm, out_ref, sems, total, i = blocks[n]
        first = core * (total // 2) + i * per_block
        for j in range(per_block):
            values = acc[n % 2, :, j * HEAD_DIM:(j + 1) * HEAD_DIM].astype(BF16).astype(F32)
            if out_ref is not v_ref:
                row = hidden // HEAD_DIM + (1 if out_ref is k_ref else 0)
                inv_rms = lax.rsqrt(jnp.mean(values * values, axis=-1, keepdims=True) + NORM_EPS)
                scaled = values * inv_rms * gain_ref[row:row + 1, :]
                values = scaled * rope_ref[:rows, :] + pltpu.roll(scaled, HEAD_DIM // 2, 1) * rope_ref[rows:, :]
                values = values.astype(BF16).astype(F32)
            out_ref[:, first + j, :, :] = values.reshape(rows // 8, 8, HEAD_DIM)

    def send(n):
        _, out_ref, sems, total, i = blocks[n]
        there = pl.ds(core * (total // 2) + i * per_block, per_block)
        copy = remote(out_ref.at[:, there], out_ref.at[:, there], sems.at[i], other_core)
        copy.start()
        return copy

    sends = []
    for n in range(len(blocks)):
        w_copies[n].wait()
        if n + 2 < len(blocks):
            w_copies[n + 2].start()
        acc[n % 2] = jnp.dot(normed[...], wbuf[n], preferred_element_type=F32)
        if n > 0:
            finish(n - 1)
            sends.append(send(n - 1))
    finish(len(blocks) - 1)
    sends.append(send(len(blocks) - 1))
    for copy in sends:
        copy.wait()


def project(x_steps, rope, gains, w_q, w_k, w_v):
    steps, batch, hidden = x_steps.shape
    rows = steps * batch
    heads = w_q.shape[1] // HEAD_DIM
    kv_heads = w_k.shape[1] // HEAD_DIM
    width = kv_heads // 2 * HEAD_DIM
    q_blocks = heads // kv_heads
    return pl.pallas_call(
        functools.partial(project_kernel, width, heads, kv_heads),
        name='project',
        out_shape=tuple(jax.ShapeDtypeStruct((rows // 8, n, 8, HEAD_DIM), F32) for n in (heads, kv_heads, kv_heads)),
        in_specs=[pl.BlockSpec(memory_space=pltpu.HBM), IN_VMEM, IN_VMEM] + [IN_PLACE] * 3,
        out_specs=(IN_VMEM,) * 3,
        scratch_shapes=[
            VMEM((rows, hidden), BF16),
            VMEM((rows, hidden), BF16),
            VMEM((2, rows, width), F32),
            VMEM((q_blocks + 2, hidden, width), BF16),
            DMA,
            DMA((q_blocks + 2,)),
            DMA((q_blocks, 2)),
            DMA((1, 2)),
            DMA((1, 2)),
        ],
        compiler_params=pltpu.CompilerParams(collective_id=1, has_side_effects=True, vmem_limit_bytes=40 * MIB),
    )(pltpu.with_memory_space_constraint(x_steps.reshape(rows, hidden), pltpu.HBM), rope, gains, w_q, w_k, w_v)


def attend_kernel(steps, depth, start, lens_ref, k_hbm, v_hbm, q_ref, kn_ref, vn_ref, ko_hbm, vo_hbm, num_ref, stat_ref, k_buf, v_buf, dist, scores_0, scores_1, weights_0, weights_1, sems_in, sems_out):
    held, key_rows, _ = k_buf.shape
    batch = lens_ref.shape[0]
    count = num_ref.shape[0]
    heads, kv_heads = q_ref.shape[0] // (steps * batch), kn_ref.shape[0] // (steps * batch)
    slots = key_rows // kv_heads
    rows = steps * heads
    half = heads // 2
    first_slot = lax.axis_index('sp') * slots
    upper = lax.broadcasted_iota(jnp.int32, (2 * kv_heads, HEAD_DIM), 0) >= kv_heads
    scale = HEAD_DIM ** -0.5 * math.log2(math.e)
    scores_refs, weights_refs = (scores_0, scores_1), (weights_0, weights_1)

    def copies_in(b):
        slot = lax.rem(b, held)
        return (pltpu.make_async_copy(k_hbm.at[start + b], k_buf.at[slot], sems_in.at[slot, 0]),
                pltpu.make_async_copy(v_hbm.at[start + b], v_buf.at[slot], sems_in.at[slot, 1]))

    def copies_out(b):
        slot = lax.rem(b, held)
        return (pltpu.make_async_copy(k_buf.at[slot], ko_hbm.at[start + b], sems_out.at[slot, 0]),
                pltpu.make_async_copy(v_buf.at[slot], vo_hbm.at[start + b], sems_out.at[slot, 1]))

    for b in range(depth // 2):
        for copy in copies_in(b):
            copy.start()

    lane = lax.broadcasted_iota(jnp.int32, (rows, 128), 1)
    stat_ref[...] = jnp.where(lane < batch, MASKED_MAX, 0.0)
    row = lax.broadcasted_iota(jnp.int32, (rows, key_rows), 0)
    col = lax.broadcasted_iota(jnp.int32, (rows, key_rows), 1)
    row_half, in_half = row // (steps * half), lax.rem(row, steps * half)
    row_kv = (row_half * half + lax.rem(in_half, half)) // (heads // kv_heads)
    dist[...] = jnp.where(row_kv == lax.rem(col, kv_heads), col // kv_heads - in_half // half, 1 << 24)

    def rel_of(b):
        return lens_ref[start + jnp.clip(b, 0, count - 1)] - first_slot

    def receive(b):
        slot = lax.rem(b, held)
        for copy in copies_in(b):
            copy.wait()
        rel = rel_of(b)
        for t in range(steps):
            at = rel + t

            @pl.when((at >= 0) & (at < slots))
            def _():
                base = pl.multiple_of((at >> 1) * (2 * kv_heads), 2 * kv_heads)
                mine = upper == ((at & 1) == 1)
                r = t * batch + start + b
                new_rows = pl.ds((r >> 3) * (8 * kv_heads) + (r & 7), kv_heads, stride=8)
                for buf, new in ((k_buf, kn_ref), (v_buf, vn_ref)):
                    fresh = new[new_rows, :]
                    fresh = jnp.concatenate([fresh, fresh], axis=0)
                    old = buf[slot, pl.ds(base, 2 * kv_heads), :].astype(F32)
                    buf[slot, pl.ds(base, 2 * kv_heads), :] = jnp.where(mine, fresh, old).astype(BF16)

    def score(j, parity):
        b = jnp.clip(j, 0, count - 1)
        pieces = []
        for h in range(2):
            for t in range(steps):
                r = t * batch + start + b
                at = (r >> 3) * (8 * heads) + (r & 7) + h * (8 * half)
                pieces.append(q_ref[pl.ds(at, half, stride=8), :].astype(BF16))
        query = jnp.concatenate(pieces, axis=0)
        scores_refs[parity][...] = lax.dot_general(query, k_buf[lax.rem(b, held)], (((1,), (1,)), ((), ())), preferred_element_type=F32)

    def soften(j, parity):
        rel = rel_of(j)
        known = (j >= 0) & (j < count)
        max_lane = jnp.where(known, start + j, 1024)
        sum_lane = jnp.where(known, start + j + batch, 1024)
        size = 16
        block_lane = lax.broadcasted_iota(jnp.int32, (size, 128), 1)
        for first in range(0, rows, size):
            here = slice(first, first + size)
            scores = jnp.where(dist[here, :] <= rel, scores_refs[parity][here, :], -jnp.inf)
            row_max = jnp.maximum(jnp.max(scores, axis=1, keepdims=True), MASKED_MAX)
            weights = jnp.exp2((scores - row_max) * scale)
            row_sum = jnp.sum(weights, axis=1, keepdims=True)
            weights_refs[parity][here, :] = weights.astype(BF16)
            stats = jnp.where(block_lane == max_lane, row_max, stat_ref[here, :])
            stat_ref[here, :] = jnp.where(block_lane == sum_lane, row_sum, stats)

    def mix(j, parity):
        b = jnp.clip(j, 0, count - 1)
        mixed = jnp.dot(weights_refs[parity][...], v_buf[lax.rem(b, held)], preferred_element_type=F32)
        num_ref[b] = jnp.where(rel_of(j) + steps - 1 >= 0, mixed, 0.0)

    def pair(k, carry):
        first = 2 * k

        @pl.when(first < count)
        def _():
            receive(first)
            receive(first + 1)

        @pl.when(first == 0)
        def _():
            for b in range(depth // 2, depth):
                for copy in copies_in(b):
                    copy.start()

        longest = functools.reduce(jnp.maximum, [rel_of(first + n) for n in range(-2, 2)])
        visible = longest + steps - 1 >= 0

        @pl.when(visible)
        def _():
            for parity in range(2):
                score(first + parity, parity)
                soften(first + parity - 1, 1 - parity)
                mix(first + parity - 2, parity)

        @pl.when(jnp.logical_not(visible))
        def _():
            for parity in range(2):
                num_ref[jnp.clip(first + parity - 2, 0, count - 1)] = jnp.zeros((rows, HEAD_DIM), F32)

        @pl.when(first < count)
        def _():
            for n in range(2):
                for copy in copies_out(first + n):
                    copy.start()

        for n in range(2):
            ahead = first + depth + n

            @pl.when(ahead < count)
            def _():
                @pl.when(ahead >= held)
                def _():
                    for copy in copies_out(ahead - held):
                        copy.wait()

                for copy in copies_in(ahead):
                    copy.start()

        return carry

    lax.fori_loop(0, count // 2 + 1, pair, 0)
    for b in range(max(count - held, 0), count):
        for copy in copies_out(b):
            copy.wait()


def attend(seq_lens, k_cache, v_cache, queries, k_new, v_new, steps, start, count, partial=()):
    batch, key_rows, head_dim = k_cache.shape
    heads = queries.shape[1]
    rows = steps * heads
    depth, held = 16, 32
    cache = jax.ShapeDtypeStruct(k_cache.shape, BF16)
    flops = 4 * count * rows * key_rows * head_dim
    kernel = functools.partial(attend_kernel, steps, depth, start)

    def continued(*refs):
        kernel(*refs[:6], *refs[8:])

    return pl.pallas_call(
        continued if partial else kernel,
        name='attend',
        in_specs=[pl.BlockSpec(memory_space=pltpu.SMEM), IN_PLACE, IN_PLACE, IN_VMEM, IN_VMEM, IN_VMEM] + [IN_PLACE] * len(partial),
        out_specs=(IN_PLACE, IN_PLACE, IN_VMEM, IN_VMEM),
        out_shape=(cache, cache, jax.ShapeDtypeStruct((count, rows, head_dim), F32), jax.ShapeDtypeStruct((rows, 128), F32)),
        input_output_aliases={6: 0, 7: 1} if partial else {},
        scratch_shapes=[
            VMEM((held, key_rows, head_dim), BF16),
            VMEM((held, key_rows, head_dim), BF16),
            VMEM((rows, key_rows), jnp.int32),
            VMEM((rows, key_rows), F32),
            VMEM((rows, key_rows), F32),
            VMEM((rows, key_rows), BF16),
            VMEM((rows, key_rows), BF16),
            DMA((held, 2)),
            DMA((held, 2)),
        ],
        cost_estimate=pl.CostEstimate(flops=flops, bytes_accessed=4 * count * key_rows * head_dim * 2, transcendentals=0),
        compiler_params=pltpu.CompilerParams(vmem_limit_bytes=32 * MIB),
    )(seq_lens, k_cache, v_cache, queries.reshape(-1, head_dim), k_new.reshape(-1, head_dim), v_new.reshape(-1, head_dim), *partial)


def combine(mine, theirs, batch):
    scale = HEAD_DIM ** -0.5
    top = jnp.maximum(mine, theirs)
    fac_a, fac_b = jnp.exp((mine - top) * scale), jnp.exp((theirs - top) * scale)
    total = pltpu.roll(mine, 128 - batch, 1) * fac_a + pltpu.roll(theirs, 128 - batch, 1) * fac_b
    return top, fac_a, fac_b, total


def join_stats(top, total, batch):
    lane = lax.broadcasted_iota(jnp.int32, top.shape, 1)
    return jnp.where(lane < batch, top, pltpu.roll(total, batch, 1))


def places():
    me = lax.axis_index('sp')
    core = lax.rem(me, 2)
    return core, me + 1 - 2 * core, lax.rem(me + 2, 4)


def spans(chunks):
    return [(sum(chunks[:c]), seqs) for c, seqs in enumerate(chunks)]


def pair_kernel(chunks, batch, numer, stats, out, stat_d, recv_d, scaled, sem_stat, sems_d):
    rows = numer.shape[1] // 2
    core, other_core, _ = places()
    own = pl.ds(pl.multiple_of(core * rows, rows), rows)
    other = pl.ds(pl.multiple_of((1 - core) * rows, rows), rows)
    meet(other_core)
    stat_copy = remote(stats.at[other], stat_d, sem_stat, other_core)
    stat_copy.start()
    copies = []
    for c, (first, seqs) in enumerate(spans(chunks)):
        here = pl.ds(first, seqs)
        copy = remote(numer.at[here, other], recv_d.at[here], sems_d.at[c], other_core)
        copy.start()
        copies.append(copy)
    stat_copy.wait()
    top, fac_a, fac_b, total = combine(stats[own, :], stat_d[...], batch)
    out[numer.shape[0]] = join_stats(top, total, batch)
    scaled[0] = fac_a
    scaled[1] = fac_b
    for copy, (first, seqs) in zip(copies, spans(chunks)):
        copy.wait()
        for b in range(first, first + seqs):
            out[b] = numer[b, own, :] * scaled[0, :, b:b + 1] + recv_d[b] * scaled[1, :, b:b + 1]


def merge_pair(numer, stats, batch):
    count, rows, _ = numer.shape
    chunks = (8,) * (count // 8)
    return pl.pallas_call(
        functools.partial(pair_kernel, chunks, batch),
        name='merge_pair',
        out_shape=jax.ShapeDtypeStruct((count + 1, rows // 2, HEAD_DIM), F32),
        in_specs=[IN_VMEM, IN_VMEM],
        out_specs=IN_VMEM,
        scratch_shapes=[
            VMEM((rows // 2, 128), F32),
            VMEM((count, rows // 2, HEAD_DIM), F32),
            VMEM((2, rows // 2, 128), F32),
            DMA((2,)),
            DMA((len(chunks), 2)),
        ],
        compiler_params=pltpu.CompilerParams(collective_id=2, has_side_effects=True, vmem_limit_bytes=16 * MIB),
    )(numer, stats)


def merge_kernel(early_chunks, chunks, steps, numer, stats, early_own, early_theirs, wo_hbm, y_own, y_other, wo, stat_d, stat_send, stat_x, recv_d, send_x, recv_x, scaled, att_f32, attended, sems_w, sem_stat, sems_d, sems_x, sems_y):
    _, batch, hidden = y_own.shape
    rows = numer.shape[1] // 2
    half = rows // steps
    start = batch - numer.shape[0]
    core, other_core, other_chip = places()
    own = pl.ds(pl.multiple_of(core * rows, rows), rows)
    other = pl.ds(pl.multiple_of((1 - core) * rows, rows), rows)

    w_pieces = sems_w.shape[0]
    w_rows = half * HEAD_DIM // w_pieces
    w_first = core * (half * HEAD_DIM)
    meet(other_core, other_chip)

    stat_copy = remote(stats.at[other], stat_d, sem_stat.at[0], other_core)
    stat_copy.start()
    core_copies = []
    for c, (first, seqs) in enumerate(spans(chunks)):
        here = pl.ds(first, seqs)
        copy = remote(numer.at[here, other], recv_d.at[here], sems_d.at[c], other_core)
        copy.start()
        core_copies.append(copy)
    w_copies = []
    for p in range(w_pieces):
        src = wo_hbm.at[pl.ds(pl.multiple_of(w_first + p * w_rows, w_rows), w_rows), :]
        copy = pltpu.make_async_copy(src, wo.at[pl.ds(p * w_rows, w_rows), :], sems_w.at[p])
        copy.start()
        w_copies.append(copy)

    stat_copy.wait()
    top, fac_a, fac_b, total = combine(stats[own, :], stat_d[...], batch)
    stat_send[...] = join_stats(top, total, batch)
    scaled[0] = fac_a
    scaled[1] = fac_b
    chip_stat_copy = remote(stat_send, stat_x, sem_stat.at[1], other_chip)
    chip_stat_copy.start()

    chip_copies = []
    for c, (first, seqs) in enumerate(spans(chunks)):
        core_copies[c].wait()
        for i in range(first, first + seqs):
            b = start + i
            joined = numer[i, own, :] * scaled[0, :, b:b + 1] + recv_d[i] * scaled[1, :, b:b + 1]
            send_x[i] = joined.reshape(send_x.shape[1:])
        here = pl.ds(first, seqs)
        if c < len(chunks) - 1:
            views = [(send_x.at[here], recv_x.at[here])]
        else:
            views = [(send_x.at[here, :, part], recv_x.at[here, :, part]) for part in range(2)]
        for src, dst in views:
            copy = remote(src, dst, sems_x.at[len(chip_copies)], other_chip)
            copy.start()
            chip_copies.append(copy)

    width = 512
    y_copies = []

    def finish(mine, theirs, first, seqs, begin, parts):
        size = half // 2
        for i in range(first, first + seqs):
            b = begin + i
            for t in range(steps):
                for part in parts:
                    at = t * half + part * size
                    here = slice(at, at + size)
                    merged = mine[i, t, part] * scaled[0, here, b:b + 1] + theirs[i, t, part] * scaled[1, here, b:b + 1]
                    att_f32[pl.ds((i - first) * rows + at, size), :] = merged
        for t in range(steps):
            for h in range(parts[0] * size, (parts[-1] + 1) * size):
                values = att_f32[pl.ds(t * half + h, seqs, stride=rows), :]
                attended[t * seqs:(t + 1) * seqs, h * HEAD_DIM:(h + 1) * HEAD_DIM] = values
        if not y_copies:
            for copy in w_copies:
                copy.wait()
        at = begin + first
        depth = slice(parts[0] * size * HEAD_DIM, (parts[-1] + 1) * size * HEAD_DIM)

        here = pl.ds(at, seqs)
        span = hidden // 2
        for side in range(2):

            @pl.loop(side * span // width, (side + 1) * span // width)
            def _(j):
                cols = pl.ds(pl.multiple_of(j * width, width), width)
                out = jnp.dot(attended[:steps * seqs, depth].astype(BF16), wo[depth, cols], preferred_element_type=F32)
                for t in range(steps):
                    if parts[0] == 0:
                        y_own[t, at:at + seqs, cols] = out[t * seqs:(t + 1) * seqs, :]
                    else:
                        y_own[t, at:at + seqs, cols] += out[t * seqs:(t + 1) * seqs, :]

            if parts[-1] == 1:
                lanes = pl.ds(side * span, span)
                copy = remote(y_own.at[:, here, lanes], y_other.at[:, here, lanes], sems_y.at[len(y_copies)], other_core)
                copy.start()
                y_copies.append(copy)

    def set_factors(mine, theirs):
        _, fac_a, fac_b, total = combine(mine, theirs, batch)
        scaled[0] = fac_a / total
        scaled[1] = fac_b / total

    set_factors(early_own[start].reshape(rows, 128), early_theirs[start].reshape(rows, 128))
    for first, seqs in spans(early_chunks):
        finish(early_own, early_theirs, first, seqs, 0, (0, 1))
    chip_stat_copy.wait()
    set_factors(stat_send[...], stat_x[...])
    for c, (first, seqs) in enumerate(spans(chunks)):
        for parts in [(0, 1)] if c < len(chunks) - 1 else [(0,), (1,)]:
            chip_copies[c + parts[0]].wait()
            finish(send_x, recv_x, first, seqs, start, parts)
    for copy in y_copies:
        copy.wait()


def merge(numer, stats, early_own, early_theirs, w_o, steps, batch):
    count, rows, _ = numer.shape
    hidden = w_o.shape[1]
    early_chunks = (16, 8)
    chunks = (8, 16, 16)
    largest = max(chunks + early_chunks)
    part = jax.ShapeDtypeStruct((steps, batch, hidden), F32)
    stat = VMEM((rows // 2, 128), F32)
    split = (steps, 2, rows // (4 * steps), HEAD_DIM)
    moved = VMEM((count,) + split, F32)
    return pl.pallas_call(
        functools.partial(merge_kernel, early_chunks, chunks, steps),
        name='merge',
        out_shape=(part, part),
        in_specs=[IN_VMEM] * 4 + [IN_PLACE],
        out_specs=(IN_VMEM, IN_VMEM),
        scratch_shapes=[
            VMEM((w_o.shape[0] // 2, hidden), BF16),
            stat,
            stat,
            stat,
            VMEM((count, rows // 2, HEAD_DIM), F32),
            moved,
            moved,
            VMEM((2, rows // 2, 128), F32),
            VMEM((largest * rows // 2, HEAD_DIM), F32),
            VMEM((steps * largest, w_o.shape[0] // 2), F32),
            DMA((8,)),
            DMA((2, 2)),
            DMA((len(chunks), 2)),
            DMA((len(chunks) + 1, 2)),
            DMA((2 * (len(chunks) + len(early_chunks)), 2)),
        ],
        compiler_params=pltpu.CompilerParams(collective_id=0, has_side_effects=True, vmem_limit_bytes=40 * MIB),
    )(numer, stats, early_own.reshape((-1,) + split), early_theirs.reshape((-1,) + split), w_o)


def solution(mesh):
    def per_device(x_steps, k_local, v_local, seq_lens, norm_gain, w_q, w_k, w_v, w_o, q_gain, k_gain):
        steps, batch, _ = x_steps.shape
        early = 24
        rope, gains = small_tables(seq_lens, steps, norm_gain, q_gain, k_gain)
        fresh = project(x_steps, rope, gains, w_q, w_k, w_v)
        flat = (batch, -1, HEAD_DIM)
        caches = (k_local.reshape(flat), v_local.reshape(flat))
        k_part, v_part, early_numer, early_stats = attend(seq_lens, *caches, *fresh, steps, 0, early)
        early_own = merge_pair(early_numer, early_stats, batch)
        early_theirs = lax.ppermute(early_own, 'sp', [(i, (i + 2) % 4) for i in range(4)])
        k_out, v_out, numer, stats = attend(seq_lens, *caches, *fresh, steps, early, batch - early, (k_part, v_part))
        own, other = merge(numer, stats, early_own, early_theirs, w_o, steps, batch)
        y_steps = (x_steps.astype(F32) + (own + other)).astype(BF16)
        return y_steps, k_out.reshape(k_local.shape), v_out.reshape(v_local.shape)

    cache_spec = P('dp', 'sp', None, None)
    step_spec = P(None, 'dp', None)
    return jax.shard_map(per_device, mesh=mesh, in_specs=(step_spec, cache_spec, cache_spec, P('dp'), P(), P(), P(), P(), P(), P(), P()), out_specs=(step_spec, cache_spec, cache_spec), check_vma=False)
```

```python
import functools
import math

import jax
import jax.numpy as jnp
from jax import lax
from jax.experimental import pallas as pl
from jax.experimental.pallas import tpu as pltpu
from jax.sharding import PartitionSpec as P

NORM_EPS = 1e-6
ROPE_BASE = 1000000.0
MASKED_MAX = -1e30
HEAD_DIM = 128
F32 = jnp.float32
BF16 = jnp.bfloat16
MIB = 1024 * 1024
VMEM = pltpu.VMEM
DMA = pltpu.SemaphoreType.DMA
IN_VMEM = pl.BlockSpec(memory_space=VMEM)
IN_PLACE = pl.BlockSpec(memory_space=pl.ANY)


def rope_table(seq_lens, steps):
    half = HEAD_DIM // 2
    positions = (seq_lens[None, :] + jnp.arange(steps, dtype=jnp.int32)[:, None]).reshape(-1)
    inv_freq = jnp.exp(jnp.arange(half, dtype=F32) * (-2.0 * math.log(ROPE_BASE) / HEAD_DIM))
    angles = positions.astype(F32)[:, None] * inv_freq
    cosine = jnp.cos(angles)
    sine = jnp.sin(angles)
    return jnp.concatenate([jnp.concatenate([cosine, cosine], axis=-1), jnp.concatenate([-sine, sine], axis=-1)], axis=0)


def remote(src, dst, sems, peer):
    return pltpu.make_async_remote_copy(src_ref=src, dst_ref=dst, send_sem=sems.at[0], recv_sem=sems.at[1], device_id={'sp': peer}, device_id_type=pl.DeviceIdType.MESH)


def meet(*peers):
    barrier = pltpu.get_barrier_semaphore()
    for peer in peers:
        pl.semaphore_signal(barrier, inc=1, device_id={'sp': peer}, device_id_type=pl.DeviceIdType.MESH)
    pl.semaphore_wait(barrier, len(peers))


def project_kernel(width, heads, kv_heads, x_hbm, norm_hbm, q_gain_hbm, k_gain_hbm, rope_ref, wq_hbm, wk_hbm, wv_hbm, q_ref, k_ref, v_ref, x_rows, norm_rows, q_gain, k_gain, gain_ref, normed, acc, wbuf, sem_x, sems_gain, sems_w, sems_q, sems_k, sems_v):
    rows, hidden = x_rows.shape
    per_block = width // HEAD_DIM
    core = lax.rem(lax.axis_index('sp'), 2)
    other_core = lax.axis_index('sp') + 1 - 2 * core

    x_copy = pltpu.make_async_copy(x_hbm, x_rows, sem_x)
    x_copy.start()
    gain_copies = []
    for n, (src, dst) in enumerate(((norm_hbm, norm_rows), (q_gain_hbm, q_gain), (k_gain_hbm, k_gain))):
        copy = pltpu.make_async_copy(src, dst, sems_gain.at[n])
        copy.start()
        gain_copies.append(copy)
    blocks = [(wk_hbm, k_ref, sems_k, kv_heads, 0)]
    blocks += [(wq_hbm, q_ref, sems_q, heads, i) for i in range(heads // 2 // per_block)]
    blocks += [(wv_hbm, v_ref, sems_v, kv_heads, 0)]
    w_copies = []
    for n, (w_hbm, _, _, total, i) in enumerate(blocks):
        cols = pl.ds(pl.multiple_of(core * (total // 2 * HEAD_DIM) + i * width, width), width)
        w_copies.append(pltpu.make_async_copy(w_hbm.at[:, cols], wbuf.at[n], sems_w.at[n]))

    w_copies[0].start()
    meet(other_core)
    for copy in gain_copies:
        copy.wait()
    norm_count = hidden // HEAD_DIM
    gain_ref[:norm_count, :] = norm_rows[...].astype(F32)
    gain_ref[norm_count:norm_count + 1, :] = q_gain[...].astype(F32)
    gain_ref[norm_count + 1:norm_count + 2, :] = k_gain[...].astype(F32)
    x_copy.wait()
    w_copies[1].start()

    @pl.loop(0, rows // 16, unroll=4)
    def _(i):
        here = pl.ds(pl.multiple_of(i * 16, 16), 16)
        values = x_rows[here, :].astype(F32)
        inv_rms = lax.rsqrt(jnp.mean(values * values, axis=-1, keepdims=True) + NORM_EPS)
        for n in range(hidden // HEAD_DIM):
            lanes = slice(n * HEAD_DIM, (n + 1) * HEAD_DIM)
            normed[here, lanes] = (x_rows[here, lanes].astype(F32) * inv_rms * gain_ref[n:n + 1, :]).astype(BF16)

    def finish(n):
        w_hbm, out_ref, sems, total, i = blocks[n]
        first = core * (total // 2) + i * per_block
        for j in range(per_block):
            values = acc[n % 2, :, j * HEAD_DIM:(j + 1) * HEAD_DIM].astype(BF16).astype(F32)
            if out_ref is not v_ref:
                row = hidden // HEAD_DIM + (1 if out_ref is k_ref else 0)
                inv_rms = lax.rsqrt(jnp.mean(values * values, axis=-1, keepdims=True) + NORM_EPS)
                scaled = values * inv_rms * gain_ref[row:row + 1, :]
                values = scaled * rope_ref[:rows, :] + pltpu.roll(scaled, HEAD_DIM // 2, 1) * rope_ref[rows:, :]
                values = values.astype(BF16).astype(F32)
            out_ref[:, first + j, :, :] = values.reshape(rows // 8, 8, HEAD_DIM)

    def send(n):
        _, out_ref, sems, total, i = blocks[n]
        there = pl.ds(core * (total // 2) + i * per_block, per_block)
        copy = remote(out_ref.at[:, there], out_ref.at[:, there], sems.at[i], other_core)
        copy.start()
        return copy

    sends = []
    for n in range(len(blocks)):
        w_copies[n].wait()
        if n + 2 < len(blocks):
            w_copies[n + 2].start()
        acc[n % 2] = jnp.dot(normed[...], wbuf[n], preferred_element_type=F32)
        if n > 0:
            finish(n - 1)
            sends.append(send(n - 1))
    finish(len(blocks) - 1)
    sends.append(send(len(blocks) - 1))
    for copy in sends:
        copy.wait()


def project(x_steps, norm_gain, q_gain, k_gain, rope, w_q, w_k, w_v):
    steps, batch, hidden = x_steps.shape
    rows = steps * batch
    heads = w_q.shape[1] // HEAD_DIM
    kv_heads = w_k.shape[1] // HEAD_DIM
    width = kv_heads // 2 * HEAD_DIM
    q_blocks = heads // kv_heads
    pinned = [x_steps.reshape(rows, hidden)] + [gain.reshape(-1, HEAD_DIM) for gain in (norm_gain, q_gain, k_gain)]
    pinned = [pltpu.with_memory_space_constraint(array, pltpu.HBM) for array in pinned]
    return pl.pallas_call(
        functools.partial(project_kernel, width, heads, kv_heads),
        name='project',
        out_shape=tuple(jax.ShapeDtypeStruct((rows // 8, n, 8, HEAD_DIM), F32) for n in (heads, kv_heads, kv_heads)),
        in_specs=[pl.BlockSpec(memory_space=pltpu.HBM)] * 4 + [IN_VMEM] + [IN_PLACE] * 3,
        out_specs=(IN_VMEM,) * 3,
        scratch_shapes=[
            VMEM((rows, hidden), BF16),
            VMEM((hidden // HEAD_DIM, HEAD_DIM), BF16),
            VMEM((1, HEAD_DIM), BF16),
            VMEM((1, HEAD_DIM), BF16),
            VMEM((hidden // HEAD_DIM + 2, HEAD_DIM), F32),
            VMEM((rows, hidden), BF16),
            VMEM((2, rows, width), F32),
            VMEM((q_blocks + 2, hidden, width), BF16),
            DMA,
            DMA((3,)),
            DMA((q_blocks + 2,)),
            DMA((q_blocks, 2)),
            DMA((1, 2)),
            DMA((1, 2)),
        ],
        compiler_params=pltpu.CompilerParams(collective_id=1, has_side_effects=True, vmem_limit_bytes=40 * MIB),
    )(*pinned, rope, w_q, w_k, w_v)


def attend_kernel(steps, depth, start, lens_ref, k_hbm, v_hbm, q_ref, kn_ref, vn_ref, ko_hbm, vo_hbm, num_ref, stat_ref, k_buf, v_buf, dist, scores_0, scores_1, weights_0, weights_1, sems_in, sems_out):
    held, key_rows, _ = k_buf.shape
    batch = lens_ref.shape[0]
    count = num_ref.shape[0]
    heads, kv_heads = q_ref.shape[0] // (steps * batch), kn_ref.shape[0] // (steps * batch)
    slots = key_rows // kv_heads
    rows = steps * heads
    half = heads // 2
    first_slot = lax.axis_index('sp') * slots
    upper = lax.broadcasted_iota(jnp.int32, (2 * kv_heads, HEAD_DIM), 0) >= kv_heads
    scale = HEAD_DIM ** -0.5 * math.log2(math.e)
    scores_refs, weights_refs = (scores_0, scores_1), (weights_0, weights_1)

    def copies_in(b):
        slot = lax.rem(b, held)
        return (pltpu.make_async_copy(k_hbm.at[start + b], k_buf.at[slot], sems_in.at[slot, 0]),
                pltpu.make_async_copy(v_hbm.at[start + b], v_buf.at[slot], sems_in.at[slot, 1]))

    def copies_out(b):
        slot = lax.rem(b, held)
        return (pltpu.make_async_copy(k_buf.at[slot], ko_hbm.at[start + b], sems_out.at[slot, 0]),
                pltpu.make_async_copy(v_buf.at[slot], vo_hbm.at[start + b], sems_out.at[slot, 1]))

    for b in range(2):
        for copy in copies_in(b):
            copy.start()

    lane = lax.broadcasted_iota(jnp.int32, (rows, 128), 1)
    stat_ref[...] = jnp.where(lane < batch, MASKED_MAX, 0.0)
    row = lax.broadcasted_iota(jnp.int32, (rows, key_rows), 0)
    col = lax.broadcasted_iota(jnp.int32, (rows, key_rows), 1)
    row_half, in_half = row // (steps * half), lax.rem(row, steps * half)
    row_kv = (row_half * half + lax.rem(in_half, half)) // (heads // kv_heads)
    dist[...] = jnp.where(row_kv == lax.rem(col, kv_heads), col // kv_heads - in_half // half, 1 << 24)
    for b in range(2, depth // 2):
        for copy in copies_in(b):
            copy.start()

    def rel_of(b):
        return lens_ref[start + jnp.clip(b, 0, count - 1)] - first_slot

    def receive(b):
        slot = lax.rem(b, held)
        for copy in copies_in(b):
            copy.wait()
        rel = rel_of(b)
        for t in range(steps):
            at = rel + t

            @pl.when((at >= 0) & (at < slots))
            def _():
                base = pl.multiple_of((at >> 1) * (2 * kv_heads), 2 * kv_heads)
                mine = upper == ((at & 1) == 1)
                r = t * batch + start + b
                new_rows = pl.ds((r >> 3) * (8 * kv_heads) + (r & 7), kv_heads, stride=8)
                for buf, new in ((k_buf, kn_ref), (v_buf, vn_ref)):
                    fresh = new[new_rows, :]
                    fresh = jnp.concatenate([fresh, fresh], axis=0)
                    old = buf[slot, pl.ds(base, 2 * kv_heads), :].astype(F32)
                    buf[slot, pl.ds(base, 2 * kv_heads), :] = jnp.where(mine, fresh, old).astype(BF16)

    def score(j, parity):
        b = jnp.clip(j, 0, count - 1)
        pieces = []
        for h in range(2):
            for t in range(steps):
                r = t * batch + start + b
                at = (r >> 3) * (8 * heads) + (r & 7) + h * (8 * half)
                pieces.append(q_ref[pl.ds(at, half, stride=8), :].astype(BF16))
        query = jnp.concatenate(pieces, axis=0)
        scores_refs[parity][...] = lax.dot_general(query, k_buf[lax.rem(b, held)], (((1,), (1,)), ((), ())), preferred_element_type=F32)

    def soften(j, parity):
        rel = rel_of(j)
        known = (j >= 0) & (j < count)
        max_lane = jnp.where(known, start + j, 1024)
        sum_lane = jnp.where(known, start + j + batch, 1024)
        size = 16
        block_lane = lax.broadcasted_iota(jnp.int32, (size, 128), 1)
        for first in range(0, rows, size):
            here = slice(first, first + size)
            scores = jnp.where(dist[here, :] <= rel, scores_refs[parity][here, :], -jnp.inf)
            row_max = jnp.maximum(jnp.max(scores, axis=1, keepdims=True), MASKED_MAX)
            weights = jnp.exp2((scores - row_max) * scale)
            row_sum = jnp.sum(weights, axis=1, keepdims=True)
            weights_refs[parity][here, :] = weights.astype(BF16)
            stats = jnp.where(block_lane == max_lane, row_max, stat_ref[here, :])
            stat_ref[here, :] = jnp.where(block_lane == sum_lane, row_sum, stats)

    def mix(j, parity):
        b = jnp.clip(j, 0, count - 1)
        mixed = jnp.dot(weights_refs[parity][...], v_buf[lax.rem(b, held)], preferred_element_type=F32)
        num_ref[b] = jnp.where(rel_of(j) + steps - 1 >= 0, mixed, 0.0)

    def pair(k, carry):
        first = 2 * k

        @pl.when(first < count)
        def _():
            receive(first)
            receive(first + 1)

        @pl.when(first == 0)
        def _():
            for b in range(depth // 2, depth):
                for copy in copies_in(b):
                    copy.start()

        longest = functools.reduce(jnp.maximum, [rel_of(first + n) for n in range(-2, 2)])
        visible = longest + steps - 1 >= 0

        @pl.when(visible)
        def _():
            for parity in range(2):
                score(first + parity, parity)
                soften(first + parity - 1, 1 - parity)
                mix(first + parity - 2, parity)

        @pl.when(jnp.logical_not(visible))
        def _():
            for parity in range(2):
                num_ref[jnp.clip(first + parity - 2, 0, count - 1)] = jnp.zeros((rows, HEAD_DIM), F32)

        @pl.when(first < count)
        def _():
            for n in range(2):
                for copy in copies_out(first + n):
                    copy.start()

        for n in range(2):
            ahead = first + depth + n

            @pl.when(ahead < count)
            def _():
                @pl.when(ahead >= held)
                def _():
                    for copy in copies_out(ahead - held):
                        copy.wait()

                for copy in copies_in(ahead):
                    copy.start()

        return carry

    lax.fori_loop(0, count // 2 + 1, pair, 0)
    for b in range(max(count - held, 0), count):
        for copy in copies_out(b):
            copy.wait()


def attend(seq_lens, k_cache, v_cache, queries, k_new, v_new, steps, start, count, partial=()):
    batch, key_rows, head_dim = k_cache.shape
    heads = queries.shape[1]
    rows = steps * heads
    depth, held = 16, 32
    cache = jax.ShapeDtypeStruct(k_cache.shape, BF16)
    flops = 4 * count * rows * key_rows * head_dim
    kernel = functools.partial(attend_kernel, steps, depth, start)

    def continued(*refs):
        kernel(*refs[:6], *refs[8:])

    return pl.pallas_call(
        continued if partial else kernel,
        name='attend',
        in_specs=[pl.BlockSpec(memory_space=pltpu.SMEM), IN_PLACE, IN_PLACE, IN_VMEM, IN_VMEM, IN_VMEM] + [IN_PLACE] * len(partial),
        out_specs=(IN_PLACE, IN_PLACE, IN_VMEM, IN_VMEM),
        out_shape=(cache, cache, jax.ShapeDtypeStruct((count, rows, head_dim), F32), jax.ShapeDtypeStruct((rows, 128), F32)),
        input_output_aliases={6: 0, 7: 1} if partial else {},
        scratch_shapes=[
            VMEM((held, key_rows, head_dim), BF16),
            VMEM((held, key_rows, head_dim), BF16),
            VMEM((rows, key_rows), jnp.int32),
            VMEM((rows, key_rows), F32),
            VMEM((rows, key_rows), F32),
            VMEM((rows, key_rows), BF16),
            VMEM((rows, key_rows), BF16),
            DMA((held, 2)),
            DMA((held, 2)),
        ],
        cost_estimate=pl.CostEstimate(flops=flops, bytes_accessed=4 * count * key_rows * head_dim * 2, transcendentals=0),
        compiler_params=pltpu.CompilerParams(vmem_limit_bytes=32 * MIB),
    )(seq_lens, k_cache, v_cache, queries.reshape(-1, head_dim), k_new.reshape(-1, head_dim), v_new.reshape(-1, head_dim), *partial)


def combine(mine, theirs, batch):
    scale = HEAD_DIM ** -0.5
    top = jnp.maximum(mine, theirs)
    fac_a, fac_b = jnp.exp((mine - top) * scale), jnp.exp((theirs - top) * scale)
    total = pltpu.roll(mine, 128 - batch, 1) * fac_a + pltpu.roll(theirs, 128 - batch, 1) * fac_b
    return top, fac_a, fac_b, total


def join_stats(top, total, batch):
    lane = lax.broadcasted_iota(jnp.int32, top.shape, 1)
    return jnp.where(lane < batch, top, pltpu.roll(total, batch, 1))


def places():
    me = lax.axis_index('sp')
    core = lax.rem(me, 2)
    return core, me + 1 - 2 * core, lax.rem(me + 2, 4)


def spans(chunks):
    return [(sum(chunks[:c]), seqs) for c, seqs in enumerate(chunks)]


def pair_kernel(chunks, batch, numer, stats, out, stat_d, recv_d, scaled, sem_stat, sems_d):
    rows = numer.shape[1] // 2
    core, other_core, _ = places()
    own = pl.ds(pl.multiple_of(core * rows, rows), rows)
    other = pl.ds(pl.multiple_of((1 - core) * rows, rows), rows)
    meet(other_core)
    stat_copy = remote(stats.at[other], stat_d, sem_stat, other_core)
    stat_copy.start()
    copies = []
    for c, (first, seqs) in enumerate(spans(chunks)):
        here = pl.ds(first, seqs)
        copy = remote(numer.at[here, other], recv_d.at[here], sems_d.at[c], other_core)
        copy.start()
        copies.append(copy)
    stat_copy.wait()
    top, fac_a, fac_b, total = combine(stats[own, :], stat_d[...], batch)
    out[numer.shape[0]] = join_stats(top, total, batch)
    scaled[0] = fac_a
    scaled[1] = fac_b
    for copy, (first, seqs) in zip(copies, spans(chunks)):
        copy.wait()
        for b in range(first, first + seqs):
            out[b] = numer[b, own, :] * scaled[0, :, b:b + 1] + recv_d[b] * scaled[1, :, b:b + 1]


def merge_pair(numer, stats, batch):
    count, rows, _ = numer.shape
    chunks = (8,) * (count // 8)
    return pl.pallas_call(
        functools.partial(pair_kernel, chunks, batch),
        name='merge_pair',
        out_shape=jax.ShapeDtypeStruct((count + 1, rows // 2, HEAD_DIM), F32),
        in_specs=[IN_VMEM, IN_VMEM],
        out_specs=IN_VMEM,
        scratch_shapes=[
            VMEM((rows // 2, 128), F32),
            VMEM((count, rows // 2, HEAD_DIM), F32),
            VMEM((2, rows // 2, 128), F32),
            DMA((2,)),
            DMA((len(chunks), 2)),
        ],
        compiler_params=pltpu.CompilerParams(collective_id=2, has_side_effects=True, vmem_limit_bytes=16 * MIB),
    )(numer, stats)


def merge_kernel(early_chunks, chunks, steps, numer, stats, early_own, early_theirs, wo_hbm, y_own, y_other, wo, stat_d, stat_send, stat_x, recv_d, send_x, recv_x, scaled, att_f32, attended, sems_w, sem_stat, sems_d, sems_x, sems_y):
    _, batch, hidden = y_own.shape
    rows = numer.shape[1] // 2
    half = rows // steps
    start = batch - numer.shape[0]
    core, other_core, other_chip = places()
    own = pl.ds(pl.multiple_of(core * rows, rows), rows)
    other = pl.ds(pl.multiple_of((1 - core) * rows, rows), rows)

    w_pieces = sems_w.shape[0]
    w_rows = half * HEAD_DIM // w_pieces
    w_first = core * (half * HEAD_DIM)
    meet(other_core, other_chip)

    stat_copy = remote(stats.at[other], stat_d, sem_stat.at[0], other_core)
    stat_copy.start()
    core_copies = []
    for c, (first, seqs) in enumerate(spans(chunks)):
        here = pl.ds(first, seqs)
        copy = remote(numer.at[here, other], recv_d.at[here], sems_d.at[c], other_core)
        copy.start()
        core_copies.append(copy)
    w_copies = []
    for p in range(w_pieces):
        src = wo_hbm.at[pl.ds(pl.multiple_of(w_first + p * w_rows, w_rows), w_rows), :]
        copy = pltpu.make_async_copy(src, wo.at[pl.ds(p * w_rows, w_rows), :], sems_w.at[p])
        copy.start()
        w_copies.append(copy)

    stat_copy.wait()
    top, fac_a, fac_b, total = combine(stats[own, :], stat_d[...], batch)
    stat_send[...] = join_stats(top, total, batch)
    scaled[0] = fac_a
    scaled[1] = fac_b
    chip_stat_copy = remote(stat_send, stat_x, sem_stat.at[1], other_chip)
    chip_stat_copy.start()

    chip_copies = []
    for c, (first, seqs) in enumerate(spans(chunks)):
        core_copies[c].wait()
        for i in range(first, first + seqs):
            b = start + i
            joined = numer[i, own, :] * scaled[0, :, b:b + 1] + recv_d[i] * scaled[1, :, b:b + 1]
            send_x[i] = joined.reshape(send_x.shape[1:])
        here = pl.ds(first, seqs)
        if c < len(chunks) - 1:
            views = [(send_x.at[here], recv_x.at[here])]
        else:
            views = [(send_x.at[here, :, part], recv_x.at[here, :, part]) for part in range(2)]
        for src, dst in views:
            copy = remote(src, dst, sems_x.at[len(chip_copies)], other_chip)
            copy.start()
            chip_copies.append(copy)

    width = 512
    y_copies = []

    def finish(mine, theirs, first, seqs, begin, parts):
        size = half // 2
        for i in range(first, first + seqs):
            b = begin + i
            for t in range(steps):
                for part in parts:
                    at = t * half + part * size
                    here = slice(at, at + size)
                    merged = mine[i, t, part] * scaled[0, here, b:b + 1] + theirs[i, t, part] * scaled[1, here, b:b + 1]
                    att_f32[pl.ds((i - first) * rows + at, size), :] = merged
        for t in range(steps):
            for h in range(parts[0] * size, (parts[-1] + 1) * size):
                values = att_f32[pl.ds(t * half + h, seqs, stride=rows), :]
                attended[t * seqs:(t + 1) * seqs, h * HEAD_DIM:(h + 1) * HEAD_DIM] = values
        if not y_copies:
            for copy in w_copies:
                copy.wait()
        at = begin + first
        depth = slice(parts[0] * size * HEAD_DIM, (parts[-1] + 1) * size * HEAD_DIM)

        here = pl.ds(at, seqs)
        span = hidden // 4
        for side in range(4):

            @pl.loop(side * span // width, (side + 1) * span // width)
            def _(j):
                cols = pl.ds(pl.multiple_of(j * width, width), width)
                out = jnp.dot(attended[:steps * seqs, depth].astype(BF16), wo[depth, cols], preferred_element_type=F32)
                for t in range(steps):
                    if parts[0] == 0:
                        y_own[t, at:at + seqs, cols] = out[t * seqs:(t + 1) * seqs, :]
                    else:
                        y_own[t, at:at + seqs, cols] += out[t * seqs:(t + 1) * seqs, :]

            if parts[-1] == 1:
                lanes = pl.ds(side * span, span)
                copy = remote(y_own.at[:, here, lanes], y_other.at[:, here, lanes], sems_y.at[len(y_copies)], other_core)
                copy.start()
                y_copies.append(copy)

    def set_factors(mine, theirs):
        _, fac_a, fac_b, total = combine(mine, theirs, batch)
        scaled[0] = fac_a / total
        scaled[1] = fac_b / total

    set_factors(early_own[start].reshape(rows, 128), early_theirs[start].reshape(rows, 128))
    for first, seqs in spans(early_chunks):
        finish(early_own, early_theirs, first, seqs, 0, (0, 1))
    chip_stat_copy.wait()
    set_factors(stat_send[...], stat_x[...])
    for c, (first, seqs) in enumerate(spans(chunks)):
        for parts in [(0, 1)] if c < len(chunks) - 1 else [(0,), (1,)]:
            chip_copies[c + parts[0]].wait()
            finish(send_x, recv_x, first, seqs, start, parts)
    for copy in y_copies:
        copy.wait()


def merge(numer, stats, early_own, early_theirs, w_o, steps, batch):
    count, rows, _ = numer.shape
    hidden = w_o.shape[1]
    early_chunks = (16, 8)
    chunks = (8, 16, 16)
    largest = max(chunks + early_chunks)
    part = jax.ShapeDtypeStruct((steps, batch, hidden), F32)
    stat = VMEM((rows // 2, 128), F32)
    split = (steps, 2, rows // (4 * steps), HEAD_DIM)
    moved = VMEM((count,) + split, F32)
    return pl.pallas_call(
        functools.partial(merge_kernel, early_chunks, chunks, steps),
        name='merge',
        out_shape=(part, part),
        in_specs=[IN_VMEM] * 4 + [IN_PLACE],
        out_specs=(IN_VMEM, IN_VMEM),
        scratch_shapes=[
            VMEM((w_o.shape[0] // 2, hidden), BF16),
            stat,
            stat,
            stat,
            VMEM((count, rows // 2, HEAD_DIM), F32),
            moved,
            moved,
            VMEM((2, rows // 2, 128), F32),
            VMEM((largest * rows // 2, HEAD_DIM), F32),
            VMEM((steps * largest, w_o.shape[0] // 2), F32),
            DMA((8,)),
            DMA((2, 2)),
            DMA((len(chunks), 2)),
            DMA((len(chunks) + 1, 2)),
            DMA((4 * (len(chunks) + len(early_chunks)), 2)),
        ],
        compiler_params=pltpu.CompilerParams(collective_id=0, has_side_effects=True, vmem_limit_bytes=40 * MIB),
    )(numer, stats, early_own.reshape((-1,) + split), early_theirs.reshape((-1,) + split), w_o)


def solution(mesh):
    def per_device(x_steps, k_local, v_local, seq_lens, norm_gain, w_q, w_k, w_v, w_o, q_gain, k_gain):
        steps, batch, _ = x_steps.shape
        early = 24
        fresh = project(x_steps, norm_gain, q_gain, k_gain, rope_table(seq_lens, steps), w_q, w_k, w_v)
        flat = (batch, -1, HEAD_DIM)
        caches = (k_local.reshape(flat), v_local.reshape(flat))
        k_part, v_part, early_numer, early_stats = attend(seq_lens, *caches, *fresh, steps, 0, early)
        early_own = merge_pair(early_numer, early_stats, batch)
        early_theirs = lax.ppermute(early_own, 'sp', [(i, (i + 2) % 4) for i in range(4)])
        k_out, v_out, numer, stats = attend(seq_lens, *caches, *fresh, steps, early, batch - early, (k_part, v_part))
        own, other = merge(numer, stats, early_own, early_theirs, w_o, steps, batch)
        y_steps = (x_steps.astype(F32) + (own + other)).astype(BF16)
        return y_steps, k_out.reshape(k_local.shape), v_out.reshape(v_local.shape)

    cache_spec = P('dp', 'sp', None, None)
    step_spec = P(None, 'dp', None)
    return jax.shard_map(per_device, mesh=mesh, in_specs=(step_spec, cache_spec, cache_spec, P('dp'), P(), P(), P(), P(), P(), P(), P()), out_specs=(step_spec, cache_spec, cache_spec), check_vma=False)
```

```python
import functools
import math

import jax
import jax.numpy as jnp
from jax import lax
from jax.experimental import pallas as pl
from jax.experimental.pallas import tpu as pltpu
from jax.sharding import PartitionSpec as P

NORM_EPS = 1e-6
ROPE_BASE = 1000000.0
MASKED_MAX = -1e30
HEAD_DIM = 128
F32 = jnp.float32
BF16 = jnp.bfloat16
MIB = 1024 * 1024
VMEM = pltpu.VMEM
DMA = pltpu.SemaphoreType.DMA
IN_VMEM = pl.BlockSpec(memory_space=VMEM)
IN_PLACE = pl.BlockSpec(memory_space=pl.ANY)


def fill_rope_table(lens_ref, rope, steps):
    half = HEAD_DIM // 2
    batch = lens_ref.shape[0]
    shape = (batch, HEAD_DIM)
    row = lax.broadcasted_iota(jnp.int32, shape, 0)
    lane = lax.broadcasted_iota(jnp.int32, shape, 1)
    lengths = jnp.zeros(shape, jnp.int32)
    for b in range(batch):
        lengths = jnp.where(row == b, lens_ref[b], lengths)
    index = jnp.where(lane < half, lane, lane - half).astype(F32)
    inv_freq = jnp.exp(index * (-2.0 * math.log(ROPE_BASE) / HEAD_DIM))
    sign = jnp.where(lane < half, -1.0, 1.0)
    for t in range(steps):
        angles = (lengths + t).astype(F32) * inv_freq
        rope[t * batch:(t + 1) * batch, :] = jnp.cos(angles)
        rope[(steps + t) * batch:(steps + t + 1) * batch, :] = sign * jnp.sin(angles)


def remote(src, dst, sems, peer):
    return pltpu.make_async_remote_copy(src_ref=src, dst_ref=dst, send_sem=sems.at[0], recv_sem=sems.at[1], device_id={'sp': peer}, device_id_type=pl.DeviceIdType.MESH)


def meet(*peers):
    barrier = pltpu.get_barrier_semaphore()
    for peer in peers:
        pl.semaphore_signal(barrier, inc=1, device_id={'sp': peer}, device_id_type=pl.DeviceIdType.MESH)
    pl.semaphore_wait(barrier, len(peers))


def project_kernel(width, heads, kv_heads, steps, lens_hbm, x_hbm, norm_hbm, q_gain_hbm, k_gain_hbm, wq_hbm, wk_hbm, wv_hbm, q_ref, k_ref, v_ref, x_rows, lens_ref, norm_rows, q_gain, k_gain, gain_ref, rope_ref, normed, acc, wbuf, sem_x, sems_gain, sems_w, sems_q, sems_k, sems_v):
    rows, hidden = x_rows.shape
    per_block = width // HEAD_DIM
    core = lax.rem(lax.axis_index('sp'), 2)
    other_core = lax.axis_index('sp') + 1 - 2 * core

    x_copy = pltpu.make_async_copy(x_hbm, x_rows, sem_x)
    x_copy.start()
    gain_copies = []
    for n, (src, dst) in enumerate(((lens_hbm, lens_ref), (norm_hbm, norm_rows), (q_gain_hbm, q_gain), (k_gain_hbm, k_gain))):
        copy = pltpu.make_async_copy(src, dst, sems_gain.at[n])
        copy.start()
        gain_copies.append(copy)
    blocks = [(wk_hbm, k_ref, sems_k, kv_heads, 0)]
    blocks += [(wq_hbm, q_ref, sems_q, heads, i) for i in range(heads // 2 // per_block)]
    blocks += [(wv_hbm, v_ref, sems_v, kv_heads, 0)]
    w_copies = []
    for n, (w_hbm, _, _, total, i) in enumerate(blocks):
        cols = pl.ds(pl.multiple_of(core * (total // 2 * HEAD_DIM) + i * width, width), width)
        w_copies.append(pltpu.make_async_copy(w_hbm.at[:, cols], wbuf.at[n], sems_w.at[n]))

    w_copies[0].start()
    meet(other_core)
    for copy in gain_copies:
        copy.wait()
    norm_count = hidden // HEAD_DIM
    gain_ref[:norm_count, :] = norm_rows[...].astype(F32)
    gain_ref[norm_count:norm_count + 1, :] = q_gain[...].astype(F32)
    gain_ref[norm_count + 1:norm_count + 2, :] = k_gain[...].astype(F32)
    fill_rope_table(lens_ref, rope_ref, steps)
    x_copy.wait()
    w_copies[1].start()

    @pl.loop(0, rows // 16, unroll=4)
    def _(i):
        here = pl.ds(pl.multiple_of(i * 16, 16), 16)
        values = x_rows[here, :].astype(F32)
        inv_rms = lax.rsqrt(jnp.mean(values * values, axis=-1, keepdims=True) + NORM_EPS)
        for n in range(hidden // HEAD_DIM):
            lanes = slice(n * HEAD_DIM, (n + 1) * HEAD_DIM)
            normed[here, lanes] = (x_rows[here, lanes].astype(F32) * inv_rms * gain_ref[n:n + 1, :]).astype(BF16)

    def finish(n):
        w_hbm, out_ref, sems, total, i = blocks[n]
        first = core * (total // 2) + i * per_block
        for j in range(per_block):
            values = acc[n % 2, :, j * HEAD_DIM:(j + 1) * HEAD_DIM].astype(BF16).astype(F32)
            if out_ref is not v_ref:
                row = hidden // HEAD_DIM + (1 if out_ref is k_ref else 0)
                inv_rms = lax.rsqrt(jnp.mean(values * values, axis=-1, keepdims=True) + NORM_EPS)
                scaled = values * inv_rms * gain_ref[row:row + 1, :]
                values = scaled * rope_ref[:rows, :] + pltpu.roll(scaled, HEAD_DIM // 2, 1) * rope_ref[rows:, :]
                values = values.astype(BF16).astype(F32)
            out_ref[:, first + j, :, :] = values.reshape(rows // 8, 8, HEAD_DIM)

    def send(n):
        _, out_ref, sems, total, i = blocks[n]
        there = pl.ds(core * (total // 2) + i * per_block, per_block)
        copy = remote(out_ref.at[:, there], out_ref.at[:, there], sems.at[i], other_core)
        copy.start()
        return copy

    sends = []
    for n in range(len(blocks)):
        w_copies[n].wait()
        if n + 2 < len(blocks):
            w_copies[n + 2].start()
        acc[n % 2] = jnp.dot(normed[...], wbuf[n], preferred_element_type=F32)
        if n > 0:
            finish(n - 1)
            sends.append(send(n - 1))
    finish(len(blocks) - 1)
    sends.append(send(len(blocks) - 1))
    for copy in sends:
        copy.wait()


def project(seq_lens, x_steps, norm_gain, q_gain, k_gain, w_q, w_k, w_v):
    steps, batch, hidden = x_steps.shape
    rows = steps * batch
    heads = w_q.shape[1] // HEAD_DIM
    kv_heads = w_k.shape[1] // HEAD_DIM
    width = kv_heads // 2 * HEAD_DIM
    q_blocks = heads // kv_heads
    pinned = [seq_lens, x_steps.reshape(rows, hidden)] + [gain.reshape(-1, HEAD_DIM) for gain in (norm_gain, q_gain, k_gain)]
    pinned = [pltpu.with_memory_space_constraint(array, pltpu.HBM) for array in pinned]
    return pl.pallas_call(
        functools.partial(project_kernel, width, heads, kv_heads, steps),
        name='project',
        out_shape=tuple(jax.ShapeDtypeStruct((rows // 8, n, 8, HEAD_DIM), F32) for n in (heads, kv_heads, kv_heads)),
        in_specs=[pl.BlockSpec(memory_space=pltpu.HBM)] * 5 + [IN_PLACE] * 3,
        out_specs=(IN_VMEM,) * 3,
        scratch_shapes=[
            VMEM((rows, hidden), BF16),
            pltpu.SMEM(seq_lens.shape, jnp.int32),
            VMEM((hidden // HEAD_DIM, HEAD_DIM), BF16),
            VMEM((1, HEAD_DIM), BF16),
            VMEM((1, HEAD_DIM), BF16),
            VMEM((hidden // HEAD_DIM + 2, HEAD_DIM), F32),
            VMEM((2 * rows, HEAD_DIM), F32),
            VMEM((rows, hidden), BF16),
            VMEM((2, rows, width), F32),
            VMEM((q_blocks + 2, hidden, width), BF16),
            DMA,
            DMA((4,)),
            DMA((q_blocks + 2,)),
            DMA((q_blocks, 2)),
            DMA((1, 2)),
            DMA((1, 2)),
        ],
        compiler_params=pltpu.CompilerParams(collective_id=1, has_side_effects=True, vmem_limit_bytes=40 * MIB),
    )(*pinned, w_q, w_k, w_v)


def attend_kernel(steps, depth, start, lens_ref, k_hbm, v_hbm, q_ref, kn_ref, vn_ref, ko_hbm, vo_hbm, num_ref, stat_ref, k_buf, v_buf, dist, scores_0, scores_1, weights_0, weights_1, sems_in, sems_out):
    held, key_rows, _ = k_buf.shape
    batch = lens_ref.shape[0]
    count = num_ref.shape[0]
    heads, kv_heads = q_ref.shape[0] // (steps * batch), kn_ref.shape[0] // (steps * batch)
    slots = key_rows // kv_heads
    rows = steps * heads
    half = heads // 2
    first_slot = lax.axis_index('sp') * slots
    upper = lax.broadcasted_iota(jnp.int32, (2 * kv_heads, HEAD_DIM), 0) >= kv_heads
    scale = HEAD_DIM ** -0.5 * math.log2(math.e)
    scores_refs, weights_refs = (scores_0, scores_1), (weights_0, weights_1)

    def copies_in(b):
        slot = lax.rem(b, held)
        return (pltpu.make_async_copy(k_hbm.at[start + b], k_buf.at[slot], sems_in.at[slot, 0]),
                pltpu.make_async_copy(v_hbm.at[start + b], v_buf.at[slot], sems_in.at[slot, 1]))

    def copies_out(b):
        slot = lax.rem(b, held)
        return (pltpu.make_async_copy(k_buf.at[slot], ko_hbm.at[start + b], sems_out.at[slot, 0]),
                pltpu.make_async_copy(v_buf.at[slot], vo_hbm.at[start + b], sems_out.at[slot, 1]))

    for b in range(2):
        for copy in copies_in(b):
            copy.start()

    lane = lax.broadcasted_iota(jnp.int32, (rows, 128), 1)
    stat_ref[...] = jnp.where(lane < batch, MASKED_MAX, 0.0)
    row = lax.broadcasted_iota(jnp.int32, (rows, key_rows), 0)
    col = lax.broadcasted_iota(jnp.int32, (rows, key_rows), 1)
    row_half, in_half = row // (steps * half), lax.rem(row, steps * half)
    row_kv = (row_half * half + lax.rem(in_half, half)) // (heads // kv_heads)
    dist[...] = jnp.where(row_kv == lax.rem(col, kv_heads), col // kv_heads - in_half // half, 1 << 24)
    for b in range(2, depth // 2):
        for copy in copies_in(b):
            copy.start()

    def rel_of(b):
        return lens_ref[start + jnp.clip(b, 0, count - 1)] - first_slot

    def receive(b):
        slot = lax.rem(b, held)
        for copy in copies_in(b):
            copy.wait()
        rel = rel_of(b)
        for t in range(steps):
            at = rel + t

            @pl.when((at >= 0) & (at < slots))
            def _():
                base = pl.multiple_of((at >> 1) * (2 * kv_heads), 2 * kv_heads)
                mine = upper == ((at & 1) == 1)
                r = t * batch + start + b
                new_rows = pl.ds((r >> 3) * (8 * kv_heads) + (r & 7), kv_heads, stride=8)
                for buf, new in ((k_buf, kn_ref), (v_buf, vn_ref)):
                    fresh = new[new_rows, :]
                    fresh = jnp.concatenate([fresh, fresh], axis=0)
                    old = buf[slot, pl.ds(base, 2 * kv_heads), :].astype(F32)
                    buf[slot, pl.ds(base, 2 * kv_heads), :] = jnp.where(mine, fresh, old).astype(BF16)

    def score(j, parity):
        b = jnp.clip(j, 0, count - 1)
        pieces = []
        for h in range(2):
            for t in range(steps):
                r = t * batch + start + b
                at = (r >> 3) * (8 * heads) + (r & 7) + h * (8 * half)
                pieces.append(q_ref[pl.ds(at, half, stride=8), :].astype(BF16))
        query = jnp.concatenate(pieces, axis=0)
        scores_refs[parity][...] = lax.dot_general(query, k_buf[lax.rem(b, held)], (((1,), (1,)), ((), ())), preferred_element_type=F32)

    def soften(j, parity):
        rel = rel_of(j)
        known = (j >= 0) & (j < count)
        max_lane = jnp.where(known, start + j, 1024)
        sum_lane = jnp.where(known, start + j + batch, 1024)
        size = 16
        block_lane = lax.broadcasted_iota(jnp.int32, (size, 128), 1)
        for first in range(0, rows, size):
            here = slice(first, first + size)
            scores = jnp.where(dist[here, :] <= rel, scores_refs[parity][here, :], -jnp.inf)
            row_max = jnp.maximum(jnp.max(scores, axis=1, keepdims=True), MASKED_MAX)
            weights = jnp.exp2((scores - row_max) * scale)
            row_sum = jnp.sum(weights, axis=1, keepdims=True)
            weights_refs[parity][here, :] = weights.astype(BF16)
            stats = jnp.where(block_lane == max_lane, row_max, stat_ref[here, :])
            stat_ref[here, :] = jnp.where(block_lane == sum_lane, row_sum, stats)

    def mix(j, parity):
        b = jnp.clip(j, 0, count - 1)
        mixed = jnp.dot(weights_refs[parity][...], v_buf[lax.rem(b, held)], preferred_element_type=F32)
        num_ref[b] = jnp.where(rel_of(j) + steps - 1 >= 0, mixed, 0.0)

    def pair(k, carry):
        first = 2 * k

        @pl.when(first < count)
        def _():
            receive(first)
            receive(first + 1)

        @pl.when(first == 0)
        def _():
            for b in range(depth // 2, depth):
                for copy in copies_in(b):
                    copy.start()

        longest = functools.reduce(jnp.maximum, [rel_of(first + n) for n in range(-2, 2)])
        visible = longest + steps - 1 >= 0

        @pl.when(visible)
        def _():
            for parity in range(2):
                score(first + parity, parity)
                soften(first + parity - 1, 1 - parity)
                mix(first + parity - 2, parity)

        @pl.when(jnp.logical_not(visible))
        def _():
            for parity in range(2):
                num_ref[jnp.clip(first + parity - 2, 0, count - 1)] = jnp.zeros((rows, HEAD_DIM), F32)

        @pl.when(first < count)
        def _():
            for n in range(2):
                for copy in copies_out(first + n):
                    copy.start()

        for n in range(2):
            ahead = first + depth + n

            @pl.when(ahead < count)
            def _():
                @pl.when(ahead >= held)
                def _():
                    for copy in copies_out(ahead - held):
                        copy.wait()

                for copy in copies_in(ahead):
                    copy.start()

        return carry

    lax.fori_loop(0, count // 2 + 1, pair, 0)
    for b in range(max(count - held, 0), count):
        for copy in copies_out(b):
            copy.wait()


def attend(seq_lens, k_cache, v_cache, queries, k_new, v_new, steps, start, count, partial=()):
    batch, key_rows, head_dim = k_cache.shape
    heads = queries.shape[1]
    rows = steps * heads
    depth, held = 16, 32
    cache = jax.ShapeDtypeStruct(k_cache.shape, BF16)
    flops = 4 * count * rows * key_rows * head_dim
    kernel = functools.partial(attend_kernel, steps, depth, start)

    def continued(*refs):
        kernel(*refs[:6], *refs[8:])

    return pl.pallas_call(
        continued if partial else kernel,
        name='attend',
        in_specs=[pl.BlockSpec(memory_space=pltpu.SMEM), IN_PLACE, IN_PLACE, IN_VMEM, IN_VMEM, IN_VMEM] + [IN_PLACE] * len(partial),
        out_specs=(IN_PLACE, IN_PLACE, IN_VMEM, IN_VMEM),
        out_shape=(cache, cache, jax.ShapeDtypeStruct((count, rows, head_dim), F32), jax.ShapeDtypeStruct((rows, 128), F32)),
        input_output_aliases={6: 0, 7: 1} if partial else {},
        scratch_shapes=[
            VMEM((held, key_rows, head_dim), BF16),
            VMEM((held, key_rows, head_dim), BF16),
            VMEM((rows, key_rows), jnp.int32),
            VMEM((rows, key_rows), F32),
            VMEM((rows, key_rows), F32),
            VMEM((rows, key_rows), BF16),
            VMEM((rows, key_rows), BF16),
            DMA((held, 2)),
            DMA((held, 2)),
        ],
        cost_estimate=pl.CostEstimate(flops=flops, bytes_accessed=4 * count * key_rows * head_dim * 2, transcendentals=0),
        compiler_params=pltpu.CompilerParams(vmem_limit_bytes=32 * MIB),
    )(seq_lens, k_cache, v_cache, queries.reshape(-1, head_dim), k_new.reshape(-1, head_dim), v_new.reshape(-1, head_dim), *partial)


def combine(mine, theirs, batch):
    scale = HEAD_DIM ** -0.5
    top = jnp.maximum(mine, theirs)
    fac_a, fac_b = jnp.exp((mine - top) * scale), jnp.exp((theirs - top) * scale)
    total = pltpu.roll(mine, 128 - batch, 1) * fac_a + pltpu.roll(theirs, 128 - batch, 1) * fac_b
    return top, fac_a, fac_b, total


def join_stats(top, total, batch):
    lane = lax.broadcasted_iota(jnp.int32, top.shape, 1)
    return jnp.where(lane < batch, top, pltpu.roll(total, batch, 1))


def places():
    me = lax.axis_index('sp')
    core = lax.rem(me, 2)
    return core, me + 1 - 2 * core, lax.rem(me + 2, 4)


def spans(chunks):
    return [(sum(chunks[:c]), seqs) for c, seqs in enumerate(chunks)]


def pair_kernel(chunks, batch, numer, stats, out, stat_d, recv_d, scaled, sem_stat, sems_d):
    rows = numer.shape[1] // 2
    core, other_core, _ = places()
    own = pl.ds(pl.multiple_of(core * rows, rows), rows)
    other = pl.ds(pl.multiple_of((1 - core) * rows, rows), rows)
    meet(other_core)
    stat_copy = remote(stats.at[other], stat_d, sem_stat, other_core)
    stat_copy.start()
    copies = []
    for c, (first, seqs) in enumerate(spans(chunks)):
        here = pl.ds(first, seqs)
        copy = remote(numer.at[here, other], recv_d.at[here], sems_d.at[c], other_core)
        copy.start()
        copies.append(copy)
    stat_copy.wait()
    top, fac_a, fac_b, total = combine(stats[own, :], stat_d[...], batch)
    out[numer.shape[0]] = join_stats(top, total, batch)
    scaled[0] = fac_a
    scaled[1] = fac_b
    for copy, (first, seqs) in zip(copies, spans(chunks)):
        copy.wait()
        for b in range(first, first + seqs):
            out[b] = numer[b, own, :] * scaled[0, :, b:b + 1] + recv_d[b] * scaled[1, :, b:b + 1]


def merge_pair(numer, stats, batch):
    count, rows, _ = numer.shape
    chunks = (8,) * (count // 8)
    return pl.pallas_call(
        functools.partial(pair_kernel, chunks, batch),
        name='merge_pair',
        out_shape=jax.ShapeDtypeStruct((count + 1, rows // 2, HEAD_DIM), F32),
        in_specs=[IN_VMEM, IN_VMEM],
        out_specs=IN_VMEM,
        scratch_shapes=[
            VMEM((rows // 2, 128), F32),
            VMEM((count, rows // 2, HEAD_DIM), F32),
            VMEM((2, rows // 2, 128), F32),
            DMA((2,)),
            DMA((len(chunks), 2)),
        ],
        compiler_params=pltpu.CompilerParams(collective_id=2, has_side_effects=True, vmem_limit_bytes=16 * MIB),
    )(numer, stats)


def merge_kernel(early_chunks, chunks, steps, numer, stats, early_own, early_theirs, wo_hbm, y_own, y_other, wo, stat_d, stat_send, stat_x, recv_d, send_x, recv_x, scaled, att_f32, attended, sems_w, sem_stat, sems_d, sems_x, sems_y):
    _, batch, hidden = y_own.shape
    rows = numer.shape[1] // 2
    half = rows // steps
    start = batch - numer.shape[0]
    core, other_core, other_chip = places()
    own = pl.ds(pl.multiple_of(core * rows, rows), rows)
    other = pl.ds(pl.multiple_of((1 - core) * rows, rows), rows)

    w_pieces = sems_w.shape[0]
    w_rows = half * HEAD_DIM // w_pieces
    w_first = core * (half * HEAD_DIM)
    meet(other_core, other_chip)

    stat_copy = remote(stats.at[other], stat_d, sem_stat.at[0], other_core)
    stat_copy.start()
    core_copies = []
    for c, (first, seqs) in enumerate(spans(chunks)):
        here = pl.ds(first, seqs)
        copy = remote(numer.at[here, other], recv_d.at[here], sems_d.at[c], other_core)
        copy.start()
        core_copies.append(copy)
    w_copies = []
    for p in range(w_pieces):
        src = wo_hbm.at[pl.ds(pl.multiple_of(w_first + p * w_rows, w_rows), w_rows), :]
        copy = pltpu.make_async_copy(src, wo.at[pl.ds(p * w_rows, w_rows), :], sems_w.at[p])
        copy.start()
        w_copies.append(copy)

    stat_copy.wait()
    top, fac_a, fac_b, total = combine(stats[own, :], stat_d[...], batch)
    stat_send[...] = join_stats(top, total, batch)
    scaled[0] = fac_a
    scaled[1] = fac_b
    chip_stat_copy = remote(stat_send, stat_x, sem_stat.at[1], other_chip)
    chip_stat_copy.start()

    chip_copies = []
    for c, (first, seqs) in enumerate(spans(chunks)):
        core_copies[c].wait()
        for i in range(first, first + seqs):
            b = start + i
            joined = numer[i, own, :] * scaled[0, :, b:b + 1] + recv_d[i] * scaled[1, :, b:b + 1]
            send_x[i] = joined.reshape(send_x.shape[1:])
        here = pl.ds(first, seqs)
        if c < len(chunks) - 1:
            views = [(send_x.at[here], recv_x.at[here])]
        else:
            views = [(send_x.at[here, :, part], recv_x.at[here, :, part]) for part in range(2)]
        for src, dst in views:
            copy = remote(src, dst, sems_x.at[len(chip_copies)], other_chip)
            copy.start()
            chip_copies.append(copy)

    width = 512
    y_copies = []

    def finish(mine, theirs, first, seqs, begin, parts):
        size = half // 2
        for i in range(first, first + seqs):
            b = begin + i
            for t in range(steps):
                for part in parts:
                    at = t * half + part * size
                    here = slice(at, at + size)
                    merged = mine[i, t, part] * scaled[0, here, b:b + 1] + theirs[i, t, part] * scaled[1, here, b:b + 1]
                    att_f32[pl.ds((i - first) * rows + at, size), :] = merged
        for t in range(steps):
            for h in range(parts[0] * size, (parts[-1] + 1) * size):
                values = att_f32[pl.ds(t * half + h, seqs, stride=rows), :]
                attended[t * seqs:(t + 1) * seqs, h * HEAD_DIM:(h + 1) * HEAD_DIM] = values
        if not y_copies:
            for copy in w_copies:
                copy.wait()
        at = begin + first
        depth = slice(parts[0] * size * HEAD_DIM, (parts[-1] + 1) * size * HEAD_DIM)

        here = pl.ds(at, seqs)
        span = hidden // 4
        for side in range(4):

            @pl.loop(side * span // width, (side + 1) * span // width)
            def _(j):
                cols = pl.ds(pl.multiple_of(j * width, width), width)
                out = jnp.dot(attended[:steps * seqs, depth].astype(BF16), wo[depth, cols], preferred_element_type=F32)
                for t in range(steps):
                    if parts[0] == 0:
                        y_own[t, at:at + seqs, cols] = out[t * seqs:(t + 1) * seqs, :]
                    else:
                        y_own[t, at:at + seqs, cols] += out[t * seqs:(t + 1) * seqs, :]

            if parts[-1] == 1:
                lanes = pl.ds(side * span, span)
                copy = remote(y_own.at[:, here, lanes], y_other.at[:, here, lanes], sems_y.at[len(y_copies)], other_core)
                copy.start()
                y_copies.append(copy)

    def set_factors(mine, theirs):
        _, fac_a, fac_b, total = combine(mine, theirs, batch)
        scaled[0] = fac_a / total
        scaled[1] = fac_b / total

    set_factors(early_own[start].reshape(rows, 128), early_theirs[start].reshape(rows, 128))
    for first, seqs in spans(early_chunks):
        finish(early_own, early_theirs, first, seqs, 0, (0, 1))
    chip_stat_copy.wait()
    set_factors(stat_send[...], stat_x[...])
    for c, (first, seqs) in enumerate(spans(chunks)):
        for parts in [(0, 1)] if c < len(chunks) - 1 else [(0,), (1,)]:
            chip_copies[c + parts[0]].wait()
            finish(send_x, recv_x, first, seqs, start, parts)
    for copy in y_copies:
        copy.wait()


def merge(numer, stats, early_own, early_theirs, w_o, steps, batch):
    count, rows, _ = numer.shape
    hidden = w_o.shape[1]
    early_chunks = (16, 8)
    chunks = (8, 16, 16)
    largest = max(chunks + early_chunks)
    part = jax.ShapeDtypeStruct((steps, batch, hidden), F32)
    stat = VMEM((rows // 2, 128), F32)
    split = (steps, 2, rows // (4 * steps), HEAD_DIM)
    moved = VMEM((count,) + split, F32)
    return pl.pallas_call(
        functools.partial(merge_kernel, early_chunks, chunks, steps),
        name='merge',
        out_shape=(part, part),
        in_specs=[IN_VMEM] * 4 + [IN_PLACE],
        out_specs=(IN_VMEM, IN_VMEM),
        scratch_shapes=[
            VMEM((w_o.shape[0] // 2, hidden), BF16),
            stat,
            stat,
            stat,
            VMEM((count, rows // 2, HEAD_DIM), F32),
            moved,
            moved,
            VMEM((2, rows // 2, 128), F32),
            VMEM((largest * rows // 2, HEAD_DIM), F32),
            VMEM((steps * largest, w_o.shape[0] // 2), F32),
            DMA((8,)),
            DMA((2, 2)),
            DMA((len(chunks), 2)),
            DMA((len(chunks) + 1, 2)),
            DMA((4 * (len(chunks) + len(early_chunks)), 2)),
        ],
        compiler_params=pltpu.CompilerParams(collective_id=0, has_side_effects=True, vmem_limit_bytes=40 * MIB),
    )(numer, stats, early_own.reshape((-1,) + split), early_theirs.reshape((-1,) + split), w_o)


def solution(mesh):
    def per_device(x_steps, k_local, v_local, seq_lens, norm_gain, w_q, w_k, w_v, w_o, q_gain, k_gain):
        steps, batch, _ = x_steps.shape
        early = 24
        fresh = project(seq_lens, x_steps, norm_gain, q_gain, k_gain, w_q, w_k, w_v)
        flat = (batch, -1, HEAD_DIM)
        caches = (k_local.reshape(flat), v_local.reshape(flat))
        k_part, v_part, early_numer, early_stats = attend(seq_lens, *caches, *fresh, steps, 0, early)
        early_own = merge_pair(early_numer, early_stats, batch)
        early_theirs = lax.ppermute(early_own, 'sp', [(i, (i + 2) % 4) for i in range(4)])
        k_out, v_out, numer, stats = attend(seq_lens, *caches, *fresh, steps, early, batch - early, (k_part, v_part))
        own, other = merge(numer, stats, early_own, early_theirs, w_o, steps, batch)
        y_steps = (x_steps.astype(F32) + (own + other)).astype(BF16)
        return y_steps, k_out.reshape(k_local.shape), v_out.reshape(v_local.shape)

    cache_spec = P('dp', 'sp', None, None)
    step_spec = P(None, 'dp', None)
    return jax.shard_map(per_device, mesh=mesh, in_specs=(step_spec, cache_spec, cache_spec, P('dp'), P(), P(), P(), P(), P(), P(), P()), out_specs=(step_spec, cache_spec, cache_spec), check_vma=False)
```

```python
import functools
import math

import jax
import jax.numpy as jnp
from jax import lax
from jax.experimental import pallas as pl
from jax.experimental.pallas import tpu as pltpu
from jax.sharding import PartitionSpec as P

NORM_EPS = 1e-6
ROPE_BASE = 1000000.0
MASKED_MAX = -1e30
HEAD_DIM = 128
F32 = jnp.float32
BF16 = jnp.bfloat16
MIB = 1024 * 1024
VMEM = pltpu.VMEM
DMA = pltpu.SemaphoreType.DMA
IN_VMEM = pl.BlockSpec(memory_space=VMEM)
IN_PLACE = pl.BlockSpec(memory_space=pl.ANY)


def fill_rope_table(lens_ref, rope, steps):
    half = HEAD_DIM // 2
    batch = lens_ref.shape[0]
    shape = (batch, HEAD_DIM)
    row = lax.broadcasted_iota(jnp.int32, shape, 0)
    lane = lax.broadcasted_iota(jnp.int32, shape, 1)
    lengths = jnp.zeros(shape, jnp.int32)
    for b in range(batch):
        lengths = jnp.where(row == b, lens_ref[b], lengths)
    index = jnp.where(lane < half, lane, lane - half).astype(F32)
    inv_freq = jnp.exp(index * (-2.0 * math.log(ROPE_BASE) / HEAD_DIM))
    sign = jnp.where(lane < half, -1.0, 1.0)
    for t in range(steps):
        angles = (lengths + t).astype(F32) * inv_freq
        rope[t * batch:(t + 1) * batch, :] = jnp.cos(angles)
        rope[(steps + t) * batch:(steps + t + 1) * batch, :] = sign * jnp.sin(angles)


def remote(src, dst, sems, peer):
    return pltpu.make_async_remote_copy(src_ref=src, dst_ref=dst, send_sem=sems.at[0], recv_sem=sems.at[1], device_id={'sp': peer}, device_id_type=pl.DeviceIdType.MESH)


def meet(*peers):
    barrier = pltpu.get_barrier_semaphore()
    for peer in peers:
        pl.semaphore_signal(barrier, inc=1, device_id={'sp': peer}, device_id_type=pl.DeviceIdType.MESH)
    pl.semaphore_wait(barrier, len(peers))


def project_kernel(width, heads, kv_heads, steps, lens_hbm, x_hbm, norm_hbm, q_gain_hbm, k_gain_hbm, wq_hbm, wk_hbm, wv_hbm, q_ref, k_ref, v_ref, x_rows, lens_ref, norm_rows, q_gain, k_gain, gain_ref, rope_ref, normed, acc, wbuf, sems_x, sems_gain, sems_w, sems_q, sems_k, sems_v):
    rows, hidden = x_rows.shape
    per_block = width // HEAD_DIM
    core = lax.rem(lax.axis_index('sp'), 2)
    other_core = lax.axis_index('sp') + 1 - 2 * core

    pieces = sems_x.shape[0]
    piece = rows // pieces
    x_copies = []
    for n in range(pieces):
        here = pl.ds(n * piece, piece)
        copy = pltpu.make_async_copy(x_hbm.at[here], x_rows.at[here], sems_x.at[n])
        copy.start()
        x_copies.append(copy)
    gain_copies = []
    for n, (src, dst) in enumerate(((lens_hbm, lens_ref), (norm_hbm, norm_rows), (q_gain_hbm, q_gain), (k_gain_hbm, k_gain))):
        copy = pltpu.make_async_copy(src, dst, sems_gain.at[n])
        copy.start()
        gain_copies.append(copy)
    blocks = [(wk_hbm, k_ref, sems_k, kv_heads, 0)]
    blocks += [(wq_hbm, q_ref, sems_q, heads, i) for i in range(heads // 2 // per_block)]
    blocks += [(wv_hbm, v_ref, sems_v, kv_heads, 0)]
    w_copies = []
    for n, (w_hbm, _, _, total, i) in enumerate(blocks):
        cols = pl.ds(pl.multiple_of(core * (total // 2 * HEAD_DIM) + i * width, width), width)
        w_copies.append(pltpu.make_async_copy(w_hbm.at[:, cols], wbuf.at[n], sems_w.at[n]))

    w_copies[0].start()
    meet(other_core)
    for copy in gain_copies:
        copy.wait()
    norm_count = hidden // HEAD_DIM
    gain_ref[:norm_count, :] = norm_rows[...].astype(F32)
    gain_ref[norm_count:norm_count + 1, :] = q_gain[...].astype(F32)
    gain_ref[norm_count + 1:norm_count + 2, :] = k_gain[...].astype(F32)
    fill_rope_table(lens_ref, rope_ref, steps)
    def norm_piece(first):
        @pl.loop(0, piece // 16, unroll=4)
        def _(i):
            here = pl.ds(pl.multiple_of(first + i * 16, 16), 16)
            values = x_rows[here, :].astype(F32)
            inv_rms = lax.rsqrt(jnp.mean(values * values, axis=-1, keepdims=True) + NORM_EPS)
            for n in range(hidden // HEAD_DIM):
                lanes = slice(n * HEAD_DIM, (n + 1) * HEAD_DIM)
                normed[here, lanes] = (x_rows[here, lanes].astype(F32) * inv_rms * gain_ref[n:n + 1, :]).astype(BF16)

    for n in range(pieces):
        x_copies[n].wait()
        if n == 0:
            w_copies[1].start()
        norm_piece(n * piece)

    def finish(n):
        w_hbm, out_ref, sems, total, i = blocks[n]
        first = core * (total // 2) + i * per_block
        for j in range(per_block):
            values = acc[n % 2, :, j * HEAD_DIM:(j + 1) * HEAD_DIM].astype(BF16).astype(F32)
            if out_ref is not v_ref:
                row = hidden // HEAD_DIM + (1 if out_ref is k_ref else 0)
                inv_rms = lax.rsqrt(jnp.mean(values * values, axis=-1, keepdims=True) + NORM_EPS)
                scaled = values * inv_rms * gain_ref[row:row + 1, :]
                values = scaled * rope_ref[:rows, :] + pltpu.roll(scaled, HEAD_DIM // 2, 1) * rope_ref[rows:, :]
                values = values.astype(BF16).astype(F32)
            out_ref[:, first + j, :, :] = values.reshape(rows // 8, 8, HEAD_DIM)

    def send(n):
        _, out_ref, sems, total, i = blocks[n]
        there = pl.ds(core * (total // 2) + i * per_block, per_block)
        copy = remote(out_ref.at[:, there], out_ref.at[:, there], sems.at[i], other_core)
        copy.start()
        return copy

    sends = []
    for n in range(len(blocks)):
        w_copies[n].wait()
        if n + 2 < len(blocks):
            w_copies[n + 2].start()
        acc[n % 2] = jnp.dot(normed[...], wbuf[n], preferred_element_type=F32)
        if n > 0:
            finish(n - 1)
            sends.append(send(n - 1))
    finish(len(blocks) - 1)
    sends.append(send(len(blocks) - 1))
    for copy in sends:
        copy.wait()


def project(seq_lens, x_steps, norm_gain, q_gain, k_gain, w_q, w_k, w_v):
    steps, batch, hidden = x_steps.shape
    rows = steps * batch
    heads = w_q.shape[1] // HEAD_DIM
    kv_heads = w_k.shape[1] // HEAD_DIM
    width = kv_heads // 2 * HEAD_DIM
    q_blocks = heads // kv_heads
    pinned = [seq_lens, x_steps.reshape(rows, hidden)] + [gain.reshape(-1, HEAD_DIM) for gain in (norm_gain, q_gain, k_gain)]
    pinned = [pltpu.with_memory_space_constraint(array, pltpu.HBM) for array in pinned]
    return pl.pallas_call(
        functools.partial(project_kernel, width, heads, kv_heads, steps),
        name='project',
        out_shape=tuple(jax.ShapeDtypeStruct((rows // 8, n, 8, HEAD_DIM), F32) for n in (heads, kv_heads, kv_heads)),
        in_specs=[pl.BlockSpec(memory_space=pltpu.HBM)] * 5 + [IN_PLACE] * 3,
        out_specs=(IN_VMEM,) * 3,
        scratch_shapes=[
            VMEM((rows, hidden), BF16),
            pltpu.SMEM(seq_lens.shape, jnp.int32),
            VMEM((hidden // HEAD_DIM, HEAD_DIM), BF16),
            VMEM((1, HEAD_DIM), BF16),
            VMEM((1, HEAD_DIM), BF16),
            VMEM((hidden // HEAD_DIM + 2, HEAD_DIM), F32),
            VMEM((2 * rows, HEAD_DIM), F32),
            VMEM((rows, hidden), BF16),
            VMEM((2, rows, width), F32),
            VMEM((q_blocks + 2, hidden, width), BF16),
            DMA((4,)),
            DMA((4,)),
            DMA((q_blocks + 2,)),
            DMA((q_blocks, 2)),
            DMA((1, 2)),
            DMA((1, 2)),
        ],
        compiler_params=pltpu.CompilerParams(collective_id=1, has_side_effects=True, vmem_limit_bytes=40 * MIB),
    )(*pinned, w_q, w_k, w_v)


def attend_kernel(steps, depth, start, lens_ref, k_hbm, v_hbm, q_ref, kn_ref, vn_ref, ko_hbm, vo_hbm, num_ref, stat_ref, k_buf, v_buf, dist, scores_0, scores_1, weights_0, weights_1, sems_in, sems_out):
    held, key_rows, _ = k_buf.shape
    batch = lens_ref.shape[0]
    count = num_ref.shape[0]
    heads, kv_heads = q_ref.shape[0] // (steps * batch), kn_ref.shape[0] // (steps * batch)
    slots = key_rows // kv_heads
    rows = steps * heads
    half = heads // 2
    first_slot = lax.axis_index('sp') * slots
    upper = lax.broadcasted_iota(jnp.int32, (2 * kv_heads, HEAD_DIM), 0) >= kv_heads
    scale = HEAD_DIM ** -0.5 * math.log2(math.e)
    scores_refs, weights_refs = (scores_0, scores_1), (weights_0, weights_1)

    def copies_in(b):
        slot = lax.rem(b, held)
        return (pltpu.make_async_copy(k_hbm.at[start + b], k_buf.at[slot], sems_in.at[slot, 0]),
                pltpu.make_async_copy(v_hbm.at[start + b], v_buf.at[slot], sems_in.at[slot, 1]))

    def copies_out(b):
        slot = lax.rem(b, held)
        return (pltpu.make_async_copy(k_buf.at[slot], ko_hbm.at[start + b], sems_out.at[slot, 0]),
                pltpu.make_async_copy(v_buf.at[slot], vo_hbm.at[start + b], sems_out.at[slot, 1]))

    for b in range(2):
        for copy in copies_in(b):
            copy.start()

    lane = lax.broadcasted_iota(jnp.int32, (rows, 128), 1)
    stat_ref[...] = jnp.where(lane < batch, MASKED_MAX, 0.0)
    row = lax.broadcasted_iota(jnp.int32, (rows, key_rows), 0)
    col = lax.broadcasted_iota(jnp.int32, (rows, key_rows), 1)
    row_half, in_half = row // (steps * half), lax.rem(row, steps * half)
    row_kv = (row_half * half + lax.rem(in_half, half)) // (heads // kv_heads)
    dist[...] = jnp.where(row_kv == lax.rem(col, kv_heads), col // kv_heads - in_half // half, 1 << 24)
    for b in range(2, depth // 2):
        for copy in copies_in(b):
            copy.start()

    def rel_of(b):
        return lens_ref[start + jnp.clip(b, 0, count - 1)] - first_slot

    def receive(b):
        slot = lax.rem(b, held)
        for copy in copies_in(b):
            copy.wait()
        rel = rel_of(b)
        for t in range(steps):
            at = rel + t

            @pl.when((at >= 0) & (at < slots))
            def _():
                base = pl.multiple_of((at >> 1) * (2 * kv_heads), 2 * kv_heads)
                mine = upper == ((at & 1) == 1)
                r = t * batch + start + b
                new_rows = pl.ds((r >> 3) * (8 * kv_heads) + (r & 7), kv_heads, stride=8)
                for buf, new in ((k_buf, kn_ref), (v_buf, vn_ref)):
                    fresh = new[new_rows, :]
                    fresh = jnp.concatenate([fresh, fresh], axis=0)
                    old = buf[slot, pl.ds(base, 2 * kv_heads), :].astype(F32)
                    buf[slot, pl.ds(base, 2 * kv_heads), :] = jnp.where(mine, fresh, old).astype(BF16)

    def score(j, parity):
        b = jnp.clip(j, 0, count - 1)
        pieces = []
        for h in range(2):
            for t in range(steps):
                r = t * batch + start + b
                at = (r >> 3) * (8 * heads) + (r & 7) + h * (8 * half)
                pieces.append(q_ref[pl.ds(at, half, stride=8), :].astype(BF16))
        query = jnp.concatenate(pieces, axis=0)
        scores_refs[parity][...] = lax.dot_general(query, k_buf[lax.rem(b, held)], (((1,), (1,)), ((), ())), preferred_element_type=F32)

    def soften(j, parity):
        rel = rel_of(j)
        known = (j >= 0) & (j < count)
        max_lane = jnp.where(known, start + j, 1024)
        sum_lane = jnp.where(known, start + j + batch, 1024)
        size = 16
        block_lane = lax.broadcasted_iota(jnp.int32, (size, 128), 1)
        for first in range(0, rows, size):
            here = slice(first, first + size)
            scores = jnp.where(dist[here, :] <= rel, scores_refs[parity][here, :], -jnp.inf)
            row_max = jnp.maximum(jnp.max(scores, axis=1, keepdims=True), MASKED_MAX)
            weights = jnp.exp2((scores - row_max) * scale)
            row_sum = jnp.sum(weights, axis=1, keepdims=True)
            weights_refs[parity][here, :] = weights.astype(BF16)
            stats = jnp.where(block_lane == max_lane, row_max, stat_ref[here, :])
            stat_ref[here, :] = jnp.where(block_lane == sum_lane, row_sum, stats)

    def mix(j, parity):
        b = jnp.clip(j, 0, count - 1)
        mixed = jnp.dot(weights_refs[parity][...], v_buf[lax.rem(b, held)], preferred_element_type=F32)
        num_ref[b] = jnp.where(rel_of(j) + steps - 1 >= 0, mixed, 0.0)

    def pair(k, carry):
        first = 2 * k

        @pl.when(first < count)
        def _():
            receive(first)
            receive(first + 1)

        @pl.when(first == 0)
        def _():
            for b in range(depth // 2, depth):
                for copy in copies_in(b):
                    copy.start()

        longest = functools.reduce(jnp.maximum, [rel_of(first + n) for n in range(-2, 2)])
        visible = longest + steps - 1 >= 0

        @pl.when(visible)
        def _():
            for parity in range(2):
                score(first + parity, parity)
                soften(first + parity - 1, 1 - parity)
                mix(first + parity - 2, parity)

        @pl.when(jnp.logical_not(visible))
        def _():
            for parity in range(2):
                num_ref[jnp.clip(first + parity - 2, 0, count - 1)] = jnp.zeros((rows, HEAD_DIM), F32)

        @pl.when(first < count)
        def _():
            for n in range(2):
                for copy in copies_out(first + n):
                    copy.start()

        for n in range(2):
            ahead = first + depth + n

            @pl.when(ahead < count)
            def _():
                @pl.when(ahead >= held)
                def _():
                    for copy in copies_out(ahead - held):
                        copy.wait()

                for copy in copies_in(ahead):
                    copy.start()

        return carry

    lax.fori_loop(0, count // 2 + 1, pair, 0)
    for b in range(max(count - held, 0), count):
        for copy in copies_out(b):
            copy.wait()


def attend(seq_lens, k_cache, v_cache, queries, k_new, v_new, steps, start, count, partial=()):
    batch, key_rows, head_dim = k_cache.shape
    heads = queries.shape[1]
    rows = steps * heads
    depth, held = 16, 32
    cache = jax.ShapeDtypeStruct(k_cache.shape, BF16)
    flops = 4 * count * rows * key_rows * head_dim
    kernel = functools.partial(attend_kernel, steps, depth, start)

    def continued(*refs):
        kernel(*refs[:6], *refs[8:])

    return pl.pallas_call(
        continued if partial else kernel,
        name='attend',
        in_specs=[pl.BlockSpec(memory_space=pltpu.SMEM), IN_PLACE, IN_PLACE, IN_VMEM, IN_VMEM, IN_VMEM] + [IN_PLACE] * len(partial),
        out_specs=(IN_PLACE, IN_PLACE, IN_VMEM, IN_VMEM),
        out_shape=(cache, cache, jax.ShapeDtypeStruct((count, rows, head_dim), F32), jax.ShapeDtypeStruct((rows, 128), F32)),
        input_output_aliases={6: 0, 7: 1} if partial else {},
        scratch_shapes=[
            VMEM((held, key_rows, head_dim), BF16),
            VMEM((held, key_rows, head_dim), BF16),
            VMEM((rows, key_rows), jnp.int32),
            VMEM((rows, key_rows), F32),
            VMEM((rows, key_rows), F32),
            VMEM((rows, key_rows), BF16),
            VMEM((rows, key_rows), BF16),
            DMA((held, 2)),
            DMA((held, 2)),
        ],
        cost_estimate=pl.CostEstimate(flops=flops, bytes_accessed=4 * count * key_rows * head_dim * 2, transcendentals=0),
        compiler_params=pltpu.CompilerParams(vmem_limit_bytes=32 * MIB),
    )(seq_lens, k_cache, v_cache, queries.reshape(-1, head_dim), k_new.reshape(-1, head_dim), v_new.reshape(-1, head_dim), *partial)


def combine(mine, theirs, batch):
    scale = HEAD_DIM ** -0.5
    top = jnp.maximum(mine, theirs)
    fac_a, fac_b = jnp.exp((mine - top) * scale), jnp.exp((theirs - top) * scale)
    total = pltpu.roll(mine, 128 - batch, 1) * fac_a + pltpu.roll(theirs, 128 - batch, 1) * fac_b
    return top, fac_a, fac_b, total


def join_stats(top, total, batch):
    lane = lax.broadcasted_iota(jnp.int32, top.shape, 1)
    return jnp.where(lane < batch, top, pltpu.roll(total, batch, 1))


def places():
    me = lax.axis_index('sp')
    core = lax.rem(me, 2)
    return core, me + 1 - 2 * core, lax.rem(me + 2, 4)


def spans(chunks):
    return [(sum(chunks[:c]), seqs) for c, seqs in enumerate(chunks)]


def pair_kernel(chunks, batch, numer, stats, out, stat_d, recv_d, scaled, sem_stat, sems_d):
    rows = numer.shape[1] // 2
    core, other_core, _ = places()
    own = pl.ds(pl.multiple_of(core * rows, rows), rows)
    other = pl.ds(pl.multiple_of((1 - core) * rows, rows), rows)
    meet(other_core)
    stat_copy = remote(stats.at[other], stat_d, sem_stat, other_core)
    stat_copy.start()
    copies = []
    for c, (first, seqs) in enumerate(spans(chunks)):
        here = pl.ds(first, seqs)
        copy = remote(numer.at[here, other], recv_d.at[here], sems_d.at[c], other_core)
        copy.start()
        copies.append(copy)
    stat_copy.wait()
    top, fac_a, fac_b, total = combine(stats[own, :], stat_d[...], batch)
    out[numer.shape[0]] = join_stats(top, total, batch)
    scaled[0] = fac_a
    scaled[1] = fac_b
    for copy, (first, seqs) in zip(copies, spans(chunks)):
        copy.wait()
        for b in range(first, first + seqs):
            out[b] = numer[b, own, :] * scaled[0, :, b:b + 1] + recv_d[b] * scaled[1, :, b:b + 1]


def merge_pair(numer, stats, batch):
    count, rows, _ = numer.shape
    chunks = (8,) * (count // 8)
    return pl.pallas_call(
        functools.partial(pair_kernel, chunks, batch),
        name='merge_pair',
        out_shape=jax.ShapeDtypeStruct((count + 1, rows // 2, HEAD_DIM), F32),
        in_specs=[IN_VMEM, IN_VMEM],
        out_specs=IN_VMEM,
        scratch_shapes=[
            VMEM((rows // 2, 128), F32),
            VMEM((count, rows // 2, HEAD_DIM), F32),
            VMEM((2, rows // 2, 128), F32),
            DMA((2,)),
            DMA((len(chunks), 2)),
        ],
        compiler_params=pltpu.CompilerParams(collective_id=2, has_side_effects=True, vmem_limit_bytes=16 * MIB),
    )(numer, stats)


def merge_kernel(early_chunks, chunks, steps, numer, stats, early_own, early_theirs, wo_hbm, y_own, y_other, wo, stat_d, stat_send, stat_x, recv_d, send_x, recv_x, scaled, att_f32, attended, sems_w, sem_stat, sems_d, sems_x, sems_y):
    _, batch, hidden = y_own.shape
    rows = numer.shape[1] // 2
    half = rows // steps
    start = batch - numer.shape[0]
    core, other_core, other_chip = places()
    own = pl.ds(pl.multiple_of(core * rows, rows), rows)
    other = pl.ds(pl.multiple_of((1 - core) * rows, rows), rows)

    w_pieces = sems_w.shape[0]
    w_rows = half * HEAD_DIM // w_pieces
    w_first = core * (half * HEAD_DIM)
    meet(other_core, other_chip)

    stat_copy = remote(stats.at[other], stat_d, sem_stat.at[0], other_core)
    stat_copy.start()
    core_copies = []
    for c, (first, seqs) in enumerate(spans(chunks)):
        here = pl.ds(first, seqs)
        copy = remote(numer.at[here, other], recv_d.at[here], sems_d.at[c], other_core)
        copy.start()
        core_copies.append(copy)
    w_copies = []
    for p in range(w_pieces):
        src = wo_hbm.at[pl.ds(pl.multiple_of(w_first + p * w_rows, w_rows), w_rows), :]
        copy = pltpu.make_async_copy(src, wo.at[pl.ds(p * w_rows, w_rows), :], sems_w.at[p])
        copy.start()
        w_copies.append(copy)

    stat_copy.wait()
    top, fac_a, fac_b, total = combine(stats[own, :], stat_d[...], batch)
    stat_send[...] = join_stats(top, total, batch)
    scaled[0] = fac_a
    scaled[1] = fac_b
    chip_stat_copy = remote(stat_send, stat_x, sem_stat.at[1], other_chip)
    chip_stat_copy.start()

    chip_copies = []
    for c, (first, seqs) in enumerate(spans(chunks)):
        core_copies[c].wait()
        for i in range(first, first + seqs):
            b = start + i
            joined = numer[i, own, :] * scaled[0, :, b:b + 1] + recv_d[i] * scaled[1, :, b:b + 1]
            send_x[i] = joined.reshape(send_x.shape[1:])
        here = pl.ds(first, seqs)
        if c < len(chunks) - 1:
            views = [(send_x.at[here], recv_x.at[here])]
        else:
            views = [(send_x.at[here, :, part], recv_x.at[here, :, part]) for part in range(2)]
        for src, dst in views:
            copy = remote(src, dst, sems_x.at[len(chip_copies)], other_chip)
            copy.start()
            chip_copies.append(copy)

    width = 512
    y_copies = []

    def finish(mine, theirs, first, seqs, begin, parts):
        size = half // 2
        for i in range(first, first + seqs):
            b = begin + i
            for t in range(steps):
                for part in parts:
                    at = t * half + part * size
                    here = slice(at, at + size)
                    merged = mine[i, t, part] * scaled[0, here, b:b + 1] + theirs[i, t, part] * scaled[1, here, b:b + 1]
                    att_f32[pl.ds((i - first) * rows + at, size), :] = merged
        for t in range(steps):
            for h in range(parts[0] * size, (parts[-1] + 1) * size):
                values = att_f32[pl.ds(t * half + h, seqs, stride=rows), :]
                attended[t * seqs:(t + 1) * seqs, h * HEAD_DIM:(h + 1) * HEAD_DIM] = values
        if not y_copies:
            for copy in w_copies:
                copy.wait()
        at = begin + first
        depth = slice(parts[0] * size * HEAD_DIM, (parts[-1] + 1) * size * HEAD_DIM)

        here = pl.ds(at, seqs)
        span = hidden // 4
        for side in range(4):

            @pl.loop(side * span // width, (side + 1) * span // width)
            def _(j):
                cols = pl.ds(pl.multiple_of(j * width, width), width)
                out = jnp.dot(attended[:steps * seqs, depth].astype(BF16), wo[depth, cols], preferred_element_type=F32)
                for t in range(steps):
                    if parts[0] == 0:
                        y_own[t, at:at + seqs, cols] = out[t * seqs:(t + 1) * seqs, :]
                    else:
                        y_own[t, at:at + seqs, cols] += out[t * seqs:(t + 1) * seqs, :]

            if parts[-1] == 1:
                lanes = pl.ds(side * span, span)
                copy = remote(y_own.at[:, here, lanes], y_other.at[:, here, lanes], sems_y.at[len(y_copies)], other_core)
                copy.start()
                y_copies.append(copy)

    def set_factors(mine, theirs):
        _, fac_a, fac_b, total = combine(mine, theirs, batch)
        scaled[0] = fac_a / total
        scaled[1] = fac_b / total

    set_factors(early_own[start].reshape(rows, 128), early_theirs[start].reshape(rows, 128))
    for first, seqs in spans(early_chunks):
        finish(early_own, early_theirs, first, seqs, 0, (0, 1))
    chip_stat_copy.wait()
    set_factors(stat_send[...], stat_x[...])
    for c, (first, seqs) in enumerate(spans(chunks)):
        for parts in [(0, 1)] if c < len(chunks) - 1 else [(0,), (1,)]:
            chip_copies[c + parts[0]].wait()
            finish(send_x, recv_x, first, seqs, start, parts)
    for copy in y_copies:
        copy.wait()


def merge(numer, stats, early_own, early_theirs, w_o, steps, batch):
    count, rows, _ = numer.shape
    hidden = w_o.shape[1]
    early_chunks = (16, 8)
    chunks = (8, 16, 16)
    largest = max(chunks + early_chunks)
    part = jax.ShapeDtypeStruct((steps, batch, hidden), F32)
    stat = VMEM((rows // 2, 128), F32)
    split = (steps, 2, rows // (4 * steps), HEAD_DIM)
    moved = VMEM((count,) + split, F32)
    return pl.pallas_call(
        functools.partial(merge_kernel, early_chunks, chunks, steps),
        name='merge',
        out_shape=(part, part),
        in_specs=[IN_VMEM] * 4 + [IN_PLACE],
        out_specs=(IN_VMEM, IN_VMEM),
        scratch_shapes=[
            VMEM((w_o.shape[0] // 2, hidden), BF16),
            stat,
            stat,
            stat,
            VMEM((count, rows // 2, HEAD_DIM), F32),
            moved,
            moved,
            VMEM((2, rows // 2, 128), F32),
            VMEM((largest * rows // 2, HEAD_DIM), F32),
            VMEM((steps * largest, w_o.shape[0] // 2), F32),
            DMA((8,)),
            DMA((2, 2)),
            DMA((len(chunks), 2)),
            DMA((len(chunks) + 1, 2)),
            DMA((4 * (len(chunks) + len(early_chunks)), 2)),
        ],
        compiler_params=pltpu.CompilerParams(collective_id=0, has_side_effects=True, vmem_limit_bytes=40 * MIB),
    )(numer, stats, early_own.reshape((-1,) + split), early_theirs.reshape((-1,) + split), w_o)


def solution(mesh):
    def per_device(x_steps, k_local, v_local, seq_lens, norm_gain, w_q, w_k, w_v, w_o, q_gain, k_gain):
        steps, batch, _ = x_steps.shape
        early = 24
        fresh = project(seq_lens, x_steps, norm_gain, q_gain, k_gain, w_q, w_k, w_v)
        flat = (batch, -1, HEAD_DIM)
        caches = (k_local.reshape(flat), v_local.reshape(flat))
        k_part, v_part, early_numer, early_stats = attend(seq_lens, *caches, *fresh, steps, 0, early)
        early_own = merge_pair(early_numer, early_stats, batch)
        early_theirs = lax.ppermute(early_own, 'sp', [(i, (i + 2) % 4) for i in range(4)])
        k_out, v_out, numer, stats = attend(seq_lens, *caches, *fresh, steps, early, batch - early, (k_part, v_part))
        own, other = merge(numer, stats, early_own, early_theirs, w_o, steps, batch)
        y_steps = (x_steps.astype(F32) + (own + other)).astype(BF16)
        return y_steps, k_out.reshape(k_local.shape), v_out.reshape(v_local.shape)

    cache_spec = P('dp', 'sp', None, None)
    step_spec = P(None, 'dp', None)
    return jax.shard_map(per_device, mesh=mesh, in_specs=(step_spec, cache_spec, cache_spec, P('dp'), P(), P(), P(), P(), P(), P(), P()), out_specs=(step_spec, cache_spec, cache_spec), check_vma=False)
```

```python
import functools
import math

import jax
import jax.numpy as jnp
from jax import lax
from jax.experimental import pallas as pl
from jax.experimental.pallas import tpu as pltpu
from jax.sharding import PartitionSpec as P

NORM_EPS = 1e-6
ROPE_BASE = 1000000.0
MASKED_MAX = -1e30
HEAD_DIM = 128
F32 = jnp.float32
BF16 = jnp.bfloat16
MIB = 1024 * 1024
VMEM = pltpu.VMEM
DMA = pltpu.SemaphoreType.DMA
IN_VMEM = pl.BlockSpec(memory_space=VMEM)
IN_PLACE = pl.BlockSpec(memory_space=pl.ANY)


def fill_rope_table(lens_ref, rope, steps):
    half = HEAD_DIM // 2
    batch = lens_ref.shape[0]
    shape = (batch, HEAD_DIM)
    row = lax.broadcasted_iota(jnp.int32, shape, 0)
    lane = lax.broadcasted_iota(jnp.int32, shape, 1)
    lengths = jnp.zeros(shape, jnp.int32)
    for b in range(batch):
        lengths = jnp.where(row == b, lens_ref[b], lengths)
    index = jnp.where(lane < half, lane, lane - half).astype(F32)
    inv_freq = jnp.exp(index * (-2.0 * math.log(ROPE_BASE) / HEAD_DIM))
    sign = jnp.where(lane < half, -1.0, 1.0)
    for t in range(steps):
        angles = (lengths + t).astype(F32) * inv_freq
        rope[t * batch:(t + 1) * batch, :] = jnp.cos(angles)
        rope[(steps + t) * batch:(steps + t + 1) * batch, :] = sign * jnp.sin(angles)


def remote(src, dst, sems, peer):
    return pltpu.make_async_remote_copy(src_ref=src, dst_ref=dst, send_sem=sems.at[0], recv_sem=sems.at[1], device_id={'sp': peer}, device_id_type=pl.DeviceIdType.MESH)


def meet(*peers):
    barrier = pltpu.get_barrier_semaphore()
    for peer in peers:
        pl.semaphore_signal(barrier, inc=1, device_id={'sp': peer}, device_id_type=pl.DeviceIdType.MESH)
    pl.semaphore_wait(barrier, len(peers))


def project_kernel(width, heads, kv_heads, steps, lens_hbm, x_hbm, norm_hbm, q_gain_hbm, k_gain_hbm, wq_hbm, wk_hbm, wv_hbm, q_ref, k_ref, v_ref, x_rows, lens_ref, norm_rows, q_gain, k_gain, gain_ref, rope_ref, normed, acc, wbuf, sems_x, sems_gain, sems_w, sems_q, sems_k, sems_v):
    rows, hidden = x_rows.shape
    per_block = width // HEAD_DIM
    core = lax.rem(lax.axis_index('sp'), 2)
    other_core = lax.axis_index('sp') + 1 - 2 * core

    pieces = sems_x.shape[0]
    piece = rows // pieces
    x_copies = []
    for n in range(pieces):
        here = pl.ds(n * piece, piece)
        copy = pltpu.make_async_copy(x_hbm.at[here], x_rows.at[here], sems_x.at[n])
        copy.start()
        x_copies.append(copy)
    gain_copies = []
    for n, (src, dst) in enumerate(((lens_hbm, lens_ref), (norm_hbm, norm_rows), (q_gain_hbm, q_gain), (k_gain_hbm, k_gain))):
        copy = pltpu.make_async_copy(src, dst, sems_gain.at[n])
        copy.start()
        gain_copies.append(copy)
    blocks = [(wk_hbm, k_ref, sems_k, kv_heads, 0)]
    blocks += [(wq_hbm, q_ref, sems_q, heads, i) for i in range(heads // 2 // per_block)]
    blocks += [(wv_hbm, v_ref, sems_v, kv_heads, 0)]
    w_copies = []
    for n, (w_hbm, _, _, total, i) in enumerate(blocks):
        cols = pl.ds(pl.multiple_of(core * (total // 2 * HEAD_DIM) + i * width, width), width)
        w_copies.append(pltpu.make_async_copy(w_hbm.at[:, cols], wbuf.at[n], sems_w.at[n]))

    w_copies[0].start()
    meet(other_core)
    for copy in gain_copies:
        copy.wait()
    norm_count = hidden // HEAD_DIM
    gain_ref[:norm_count, :] = norm_rows[...].astype(F32)
    gain_ref[norm_count:norm_count + 1, :] = q_gain[...].astype(F32)
    gain_ref[norm_count + 1:norm_count + 2, :] = k_gain[...].astype(F32)
    fill_rope_table(lens_ref, rope_ref, steps)
    def norm_piece(first):
        @pl.loop(0, piece // 16, unroll=4)
        def _(i):
            here = pl.ds(pl.multiple_of(first + i * 16, 16), 16)
            values = x_rows[here, :].astype(F32)
            inv_rms = lax.rsqrt(jnp.mean(values * values, axis=-1, keepdims=True) + NORM_EPS)
            for n in range(hidden // HEAD_DIM):
                lanes = slice(n * HEAD_DIM, (n + 1) * HEAD_DIM)
                normed[here, lanes] = (x_rows[here, lanes].astype(F32) * inv_rms * gain_ref[n:n + 1, :]).astype(BF16)

    for n in range(pieces):
        x_copies[n].wait()
        if n == 0:
            w_copies[1].start()
        norm_piece(n * piece)
    w_copies[2].start()

    def finish(n):
        w_hbm, out_ref, sems, total, i = blocks[n]
        first = core * (total // 2) + i * per_block
        for j in range(per_block):
            values = acc[n % 2, :, j * HEAD_DIM:(j + 1) * HEAD_DIM].astype(BF16).astype(F32)
            if out_ref is not v_ref:
                row = hidden // HEAD_DIM + (1 if out_ref is k_ref else 0)
                inv_rms = lax.rsqrt(jnp.mean(values * values, axis=-1, keepdims=True) + NORM_EPS)
                scaled = values * inv_rms * gain_ref[row:row + 1, :]
                values = scaled * rope_ref[:rows, :] + pltpu.roll(scaled, HEAD_DIM // 2, 1) * rope_ref[rows:, :]
                values = values.astype(BF16).astype(F32)
            out_ref[:, first + j, :, :] = values.reshape(rows // 8, 8, HEAD_DIM)

    def send(n):
        _, out_ref, sems, total, i = blocks[n]
        there = pl.ds(core * (total // 2) + i * per_block, per_block)
        copy = remote(out_ref.at[:, there], out_ref.at[:, there], sems.at[i], other_core)
        copy.start()
        return copy

    sends = []
    for n in range(len(blocks)):
        w_copies[n].wait()
        if n + 3 < len(blocks):
            w_copies[n + 3].start()
        acc[n % 2] = jnp.dot(normed[...], wbuf[n], preferred_element_type=F32)
        if n > 0:
            finish(n - 1)
            sends.append(send(n - 1))
    finish(len(blocks) - 1)
    sends.append(send(len(blocks) - 1))
    for copy in sends:
        copy.wait()


def project(seq_lens, x_steps, norm_gain, q_gain, k_gain, w_q, w_k, w_v):
    steps, batch, hidden = x_steps.shape
    rows = steps * batch
    heads = w_q.shape[1] // HEAD_DIM
    kv_heads = w_k.shape[1] // HEAD_DIM
    width = kv_heads // 2 * HEAD_DIM
    q_blocks = heads // kv_heads
    pinned = [seq_lens, x_steps.reshape(rows, hidden)] + [gain.reshape(-1, HEAD_DIM) for gain in (norm_gain, q_gain, k_gain)]
    pinned = [pltpu.with_memory_space_constraint(array, pltpu.HBM) for array in pinned]
    return pl.pallas_call(
        functools.partial(project_kernel, width, heads, kv_heads, steps),
        name='project',
        out_shape=tuple(jax.ShapeDtypeStruct((rows // 8, n, 8, HEAD_DIM), F32) for n in (heads, kv_heads, kv_heads)),
        in_specs=[pl.BlockSpec(memory_space=pltpu.HBM)] * 5 + [IN_PLACE] * 3,
        out_specs=(IN_VMEM,) * 3,
        scratch_shapes=[
            VMEM((rows, hidden), BF16),
            pltpu.SMEM(seq_lens.shape, jnp.int32),
            VMEM((hidden // HEAD_DIM, HEAD_DIM), BF16),
            VMEM((1, HEAD_DIM), BF16),
            VMEM((1, HEAD_DIM), BF16),
            VMEM((hidden // HEAD_DIM + 2, HEAD_DIM), F32),
            VMEM((2 * rows, HEAD_DIM), F32),
            VMEM((rows, hidden), BF16),
            VMEM((2, rows, width), F32),
            VMEM((q_blocks + 2, hidden, width), BF16),
            DMA((4,)),
            DMA((4,)),
            DMA((q_blocks + 2,)),
            DMA((q_blocks, 2)),
            DMA((1, 2)),
            DMA((1, 2)),
        ],
        compiler_params=pltpu.CompilerParams(collective_id=1, has_side_effects=True, vmem_limit_bytes=40 * MIB),
    )(*pinned, w_q, w_k, w_v)


def attend_kernel(steps, depth, start, lens_ref, k_hbm, v_hbm, q_ref, kn_ref, vn_ref, ko_hbm, vo_hbm, num_ref, stat_ref, k_buf, v_buf, dist, scores_0, scores_1, weights_0, weights_1, sems_in, sems_out):
    held, key_rows, _ = k_buf.shape
    batch = lens_ref.shape[0]
    count = num_ref.shape[0]
    heads, kv_heads = q_ref.shape[0] // (steps * batch), kn_ref.shape[0] // (steps * batch)
    slots = key_rows // kv_heads
    rows = steps * heads
    half = heads // 2
    first_slot = lax.axis_index('sp') * slots
    upper = lax.broadcasted_iota(jnp.int32, (2 * kv_heads, HEAD_DIM), 0) >= kv_heads
    scale = HEAD_DIM ** -0.5 * math.log2(math.e)
    scores_refs, weights_refs = (scores_0, scores_1), (weights_0, weights_1)

    def copies_in(b):
        slot = lax.rem(b, held)
        return (pltpu.make_async_copy(k_hbm.at[start + b], k_buf.at[slot], sems_in.at[slot, 0]),
                pltpu.make_async_copy(v_hbm.at[start + b], v_buf.at[slot], sems_in.at[slot, 1]))

    def copies_out(b):
        slot = lax.rem(b, held)
        return (pltpu.make_async_copy(k_buf.at[slot], ko_hbm.at[start + b], sems_out.at[slot, 0]),
                pltpu.make_async_copy(v_buf.at[slot], vo_hbm.at[start + b], sems_out.at[slot, 1]))

    for b in range(2):
        for copy in copies_in(b):
            copy.start()

    lane = lax.broadcasted_iota(jnp.int32, (rows, 128), 1)
    stat_ref[...] = jnp.where(lane < batch, MASKED_MAX, 0.0)
    row = lax.broadcasted_iota(jnp.int32, (rows, key_rows), 0)
    col = lax.broadcasted_iota(jnp.int32, (rows, key_rows), 1)
    row_half, in_half = row // (steps * half), lax.rem(row, steps * half)
    row_kv = (row_half * half + lax.rem(in_half, half)) // (heads // kv_heads)
    dist[...] = jnp.where(row_kv == lax.rem(col, kv_heads), col // kv_heads - in_half // half, 1 << 24)
    for b in range(2, depth // 2):
        for copy in copies_in(b):
            copy.start()

    def rel_of(b):
        return lens_ref[start + jnp.clip(b, 0, count - 1)] - first_slot

    def receive(b):
        slot = lax.rem(b, held)
        for copy in copies_in(b):
            copy.wait()
        rel = rel_of(b)
        for t in range(steps):
            at = rel + t

            @pl.when((at >= 0) & (at < slots))
            def _():
                base = pl.multiple_of((at >> 1) * (2 * kv_heads), 2 * kv_heads)
                mine = upper == ((at & 1) == 1)
                r = t * batch + start + b
                new_rows = pl.ds((r >> 3) * (8 * kv_heads) + (r & 7), kv_heads, stride=8)
                for buf, new in ((k_buf, kn_ref), (v_buf, vn_ref)):
                    fresh = new[new_rows, :]
                    fresh = jnp.concatenate([fresh, fresh], axis=0)
                    old = buf[slot, pl.ds(base, 2 * kv_heads), :].astype(F32)
                    buf[slot, pl.ds(base, 2 * kv_heads), :] = jnp.where(mine, fresh, old).astype(BF16)

    def score(j, parity):
        b = jnp.clip(j, 0, count - 1)
        pieces = []
        for h in range(2):
            for t in range(steps):
                r = t * batch + start + b
                at = (r >> 3) * (8 * heads) + (r & 7) + h * (8 * half)
                pieces.append(q_ref[pl.ds(at, half, stride=8), :].astype(BF16))
        query = jnp.concatenate(pieces, axis=0)
        scores_refs[parity][...] = lax.dot_general(query, k_buf[lax.rem(b, held)], (((1,), (1,)), ((), ())), preferred_element_type=F32)

    def soften(j, parity):
        rel = rel_of(j)
        known = (j >= 0) & (j < count)
        max_lane = jnp.where(known, start + j, 1024)
        sum_lane = jnp.where(known, start + j + batch, 1024)
        size = 16
        block_lane = lax.broadcasted_iota(jnp.int32, (size, 128), 1)
        for first in range(0, rows, size):
            here = slice(first, first + size)
            scores = jnp.where(dist[here, :] <= rel, scores_refs[parity][here, :], -jnp.inf)
            row_max = jnp.maximum(jnp.max(scores, axis=1, keepdims=True), MASKED_MAX)
            weights = jnp.exp2((scores - row_max) * scale)
            row_sum = jnp.sum(weights, axis=1, keepdims=True)
            weights_refs[parity][here, :] = weights.astype(BF16)
            stats = jnp.where(block_lane == max_lane, row_max, stat_ref[here, :])
            stat_ref[here, :] = jnp.where(block_lane == sum_lane, row_sum, stats)

    def mix(j, parity):
        b = jnp.clip(j, 0, count - 1)
        mixed = jnp.dot(weights_refs[parity][...], v_buf[lax.rem(b, held)], preferred_element_type=F32)
        num_ref[b] = jnp.where(rel_of(j) + steps - 1 >= 0, mixed, 0.0)

    def pair(k, carry):
        first = 2 * k

        @pl.when(first < count)
        def _():
            receive(first)
            receive(first + 1)

        @pl.when(first == 0)
        def _():
            for b in range(depth // 2, depth):
                for copy in copies_in(b):
                    copy.start()

        longest = functools.reduce(jnp.maximum, [rel_of(first + n) for n in range(-2, 2)])
        visible = longest + steps - 1 >= 0

        @pl.when(visible)
        def _():
            for parity in range(2):
                score(first + parity, parity)
                soften(first + parity - 1, 1 - parity)
                mix(first + parity - 2, parity)

        @pl.when(jnp.logical_not(visible))
        def _():
            for parity in range(2):
                num_ref[jnp.clip(first + parity - 2, 0, count - 1)] = jnp.zeros((rows, HEAD_DIM), F32)

        @pl.when(first < count)
        def _():
            for n in range(2):
                for copy in copies_out(first + n):
                    copy.start()

        for n in range(2):
            ahead = first + depth + n

            @pl.when(ahead < count)
            def _():
                @pl.when(ahead >= held)
                def _():
                    for copy in copies_out(ahead - held):
                        copy.wait()

                for copy in copies_in(ahead):
                    copy.start()

        return carry

    lax.fori_loop(0, count // 2 + 1, pair, 0)
    for b in range(max(count - held, 0), count):
        for copy in copies_out(b):
            copy.wait()


def attend(seq_lens, k_cache, v_cache, queries, k_new, v_new, steps, start, count, partial=()):
    batch, key_rows, head_dim = k_cache.shape
    heads = queries.shape[1]
    rows = steps * heads
    depth, held = 16, 32
    cache = jax.ShapeDtypeStruct(k_cache.shape, BF16)
    flops = 4 * count * rows * key_rows * head_dim
    kernel = functools.partial(attend_kernel, steps, depth, start)

    def continued(*refs):
        kernel(*refs[:6], *refs[8:])

    return pl.pallas_call(
        continued if partial else kernel,
        name='attend',
        in_specs=[pl.BlockSpec(memory_space=pltpu.SMEM), IN_PLACE, IN_PLACE, IN_VMEM, IN_VMEM, IN_VMEM] + [IN_PLACE] * len(partial),
        out_specs=(IN_PLACE, IN_PLACE, IN_VMEM, IN_VMEM),
        out_shape=(cache, cache, jax.ShapeDtypeStruct((count, rows, head_dim), F32), jax.ShapeDtypeStruct((rows, 128), F32)),
        input_output_aliases={6: 0, 7: 1} if partial else {},
        scratch_shapes=[
            VMEM((held, key_rows, head_dim), BF16),
            VMEM((held, key_rows, head_dim), BF16),
            VMEM((rows, key_rows), jnp.int32),
            VMEM((rows, key_rows), F32),
            VMEM((rows, key_rows), F32),
            VMEM((rows, key_rows), BF16),
            VMEM((rows, key_rows), BF16),
            DMA((held, 2)),
            DMA((held, 2)),
        ],
        cost_estimate=pl.CostEstimate(flops=flops, bytes_accessed=4 * count * key_rows * head_dim * 2, transcendentals=0),
        compiler_params=pltpu.CompilerParams(vmem_limit_bytes=32 * MIB),
    )(seq_lens, k_cache, v_cache, queries.reshape(-1, head_dim), k_new.reshape(-1, head_dim), v_new.reshape(-1, head_dim), *partial)


def combine(mine, theirs, batch):
    scale = HEAD_DIM ** -0.5
    top = jnp.maximum(mine, theirs)
    fac_a, fac_b = jnp.exp((mine - top) * scale), jnp.exp((theirs - top) * scale)
    total = pltpu.roll(mine, 128 - batch, 1) * fac_a + pltpu.roll(theirs, 128 - batch, 1) * fac_b
    return top, fac_a, fac_b, total


def join_stats(top, total, batch):
    lane = lax.broadcasted_iota(jnp.int32, top.shape, 1)
    return jnp.where(lane < batch, top, pltpu.roll(total, batch, 1))


def places():
    me = lax.axis_index('sp')
    core = lax.rem(me, 2)
    return core, me + 1 - 2 * core, lax.rem(me + 2, 4)


def spans(chunks):
    return [(sum(chunks[:c]), seqs) for c, seqs in enumerate(chunks)]


def pair_kernel(chunks, batch, numer, stats, out, stat_d, recv_d, scaled, sem_stat, sems_d):
    rows = numer.shape[1] // 2
    core, other_core, _ = places()
    own = pl.ds(pl.multiple_of(core * rows, rows), rows)
    other = pl.ds(pl.multiple_of((1 - core) * rows, rows), rows)
    meet(other_core)
    stat_copy = remote(stats.at[other], stat_d, sem_stat, other_core)
    stat_copy.start()
    copies = []
    for c, (first, seqs) in enumerate(spans(chunks)):
        here = pl.ds(first, seqs)
        copy = remote(numer.at[here, other], recv_d.at[here], sems_d.at[c], other_core)
        copy.start()
        copies.append(copy)
    stat_copy.wait()
    top, fac_a, fac_b, total = combine(stats[own, :], stat_d[...], batch)
    out[numer.shape[0]] = join_stats(top, total, batch)
    scaled[0] = fac_a
    scaled[1] = fac_b
    for copy, (first, seqs) in zip(copies, spans(chunks)):
        copy.wait()
        for b in range(first, first + seqs):
            out[b] = numer[b, own, :] * scaled[0, :, b:b + 1] + recv_d[b] * scaled[1, :, b:b + 1]


def merge_pair(numer, stats, batch):
    count, rows, _ = numer.shape
    chunks = (8,) * (count // 8)
    return pl.pallas_call(
        functools.partial(pair_kernel, chunks, batch),
        name='merge_pair',
        out_shape=jax.ShapeDtypeStruct((count + 1, rows // 2, HEAD_DIM), F32),
        in_specs=[IN_VMEM, IN_VMEM],
        out_specs=IN_VMEM,
        scratch_shapes=[
            VMEM((rows // 2, 128), F32),
            VMEM((count, rows // 2, HEAD_DIM), F32),
            VMEM((2, rows // 2, 128), F32),
            DMA((2,)),
            DMA((len(chunks), 2)),
        ],
        compiler_params=pltpu.CompilerParams(collective_id=2, has_side_effects=True, vmem_limit_bytes=16 * MIB),
    )(numer, stats)


def merge_kernel(early_chunks, chunks, steps, numer, stats, early_own, early_theirs, wo_hbm, y_own, y_other, wo, stat_d, stat_send, stat_x, recv_d, send_x, recv_x, scaled, att_f32, attended, sems_w, sem_stat, sems_d, sems_x, sems_y):
    _, batch, hidden = y_own.shape
    rows = numer.shape[1] // 2
    half = rows // steps
    start = batch - numer.shape[0]
    core, other_core, other_chip = places()
    own = pl.ds(pl.multiple_of(core * rows, rows), rows)
    other = pl.ds(pl.multiple_of((1 - core) * rows, rows), rows)

    w_pieces = sems_w.shape[0]
    w_rows = half * HEAD_DIM // w_pieces
    w_first = core * (half * HEAD_DIM)
    meet(other_core, other_chip)

    stat_copy = remote(stats.at[other], stat_d, sem_stat.at[0], other_core)
    stat_copy.start()
    core_copies = []
    for c, (first, seqs) in enumerate(spans(chunks)):
        here = pl.ds(first, seqs)
        copy = remote(numer.at[here, other], recv_d.at[here], sems_d.at[c], other_core)
        copy.start()
        core_copies.append(copy)
    w_copies = []
    for p in range(w_pieces):
        src = wo_hbm.at[pl.ds(pl.multiple_of(w_first + p * w_rows, w_rows), w_rows), :]
        copy = pltpu.make_async_copy(src, wo.at[pl.ds(p * w_rows, w_rows), :], sems_w.at[p])
        copy.start()
        w_copies.append(copy)

    stat_copy.wait()
    top, fac_a, fac_b, total = combine(stats[own, :], stat_d[...], batch)
    stat_send[...] = join_stats(top, total, batch)
    scaled[0] = fac_a
    scaled[1] = fac_b
    chip_stat_copy = remote(stat_send, stat_x, sem_stat.at[1], other_chip)
    chip_stat_copy.start()

    chip_copies = []
    for c, (first, seqs) in enumerate(spans(chunks)):
        core_copies[c].wait()
        for i in range(first, first + seqs):
            b = start + i
            joined = numer[i, own, :] * scaled[0, :, b:b + 1] + recv_d[i] * scaled[1, :, b:b + 1]
            send_x[i] = joined.reshape(send_x.shape[1:])
        here = pl.ds(first, seqs)
        if c < len(chunks) - 1:
            views = [(send_x.at[here], recv_x.at[here])]
        else:
            views = [(send_x.at[here, :, part], recv_x.at[here, :, part]) for part in range(2)]
        for src, dst in views:
            copy = remote(src, dst, sems_x.at[len(chip_copies)], other_chip)
            copy.start()
            chip_copies.append(copy)

    width = 512
    y_copies = []

    def finish(mine, theirs, first, seqs, begin, parts):
        size = half // 2
        for i in range(first, first + seqs):
            b = begin + i
            for t in range(steps):
                for part in parts:
                    at = t * half + part * size
                    here = slice(at, at + size)
                    merged = mine[i, t, part] * scaled[0, here, b:b + 1] + theirs[i, t, part] * scaled[1, here, b:b + 1]
                    att_f32[pl.ds((i - first) * rows + at, size), :] = merged
        for t in range(steps):
            for h in range(parts[0] * size, (parts[-1] + 1) * size):
                values = att_f32[pl.ds(t * half + h, seqs, stride=rows), :]
                attended[t * seqs:(t + 1) * seqs, h * HEAD_DIM:(h + 1) * HEAD_DIM] = values
        if not y_copies:
            for copy in w_copies:
                copy.wait()
        at = begin + first
        depth = slice(parts[0] * size * HEAD_DIM, (parts[-1] + 1) * size * HEAD_DIM)

        here = pl.ds(at, seqs)
        span = hidden // 4
        for side in range(4):

            @pl.loop(side * span // width, (side + 1) * span // width)
            def _(j):
                cols = pl.ds(pl.multiple_of(j * width, width), width)
                out = jnp.dot(attended[:steps * seqs, depth].astype(BF16), wo[depth, cols], preferred_element_type=F32)
                for t in range(steps):
                    if parts[0] == 0:
                        y_own[t, at:at + seqs, cols] = out[t * seqs:(t + 1) * seqs, :]
                    else:
                        y_own[t, at:at + seqs, cols] += out[t * seqs:(t + 1) * seqs, :]

            if parts[-1] == 1:
                lanes = pl.ds(side * span, span)
                copy = remote(y_own.at[:, here, lanes], y_other.at[:, here, lanes], sems_y.at[len(y_copies)], other_core)
                copy.start()
                y_copies.append(copy)

    def set_factors(mine, theirs):
        _, fac_a, fac_b, total = combine(mine, theirs, batch)
        scaled[0] = fac_a / total
        scaled[1] = fac_b / total

    set_factors(early_own[start].reshape(rows, 128), early_theirs[start].reshape(rows, 128))
    for first, seqs in spans(early_chunks):
        finish(early_own, early_theirs, first, seqs, 0, (0, 1))
    chip_stat_copy.wait()
    set_factors(stat_send[...], stat_x[...])
    for c, (first, seqs) in enumerate(spans(chunks)):
        for parts in [(0, 1)] if c < len(chunks) - 1 else [(0,), (1,)]:
            chip_copies[c + parts[0]].wait()
            finish(send_x, recv_x, first, seqs, start, parts)
    for copy in y_copies:
        copy.wait()


def merge(numer, stats, early_own, early_theirs, w_o, steps, batch):
    count, rows, _ = numer.shape
    hidden = w_o.shape[1]
    early_chunks = (16, 8)
    chunks = (8, 16, 16)
    largest = max(chunks + early_chunks)
    part = jax.ShapeDtypeStruct((steps, batch, hidden), F32)
    stat = VMEM((rows // 2, 128), F32)
    split = (steps, 2, rows // (4 * steps), HEAD_DIM)
    moved = VMEM((count,) + split, F32)
    return pl.pallas_call(
        functools.partial(merge_kernel, early_chunks, chunks, steps),
        name='merge',
        out_shape=(part, part),
        in_specs=[IN_VMEM] * 4 + [IN_PLACE],
        out_specs=(IN_VMEM, IN_VMEM),
        scratch_shapes=[
            VMEM((w_o.shape[0] // 2, hidden), BF16),
            stat,
            stat,
            stat,
            VMEM((count, rows // 2, HEAD_DIM), F32),
            moved,
            moved,
            VMEM((2, rows // 2, 128), F32),
            VMEM((largest * rows // 2, HEAD_DIM), F32),
            VMEM((steps * largest, w_o.shape[0] // 2), F32),
            DMA((8,)),
            DMA((2, 2)),
            DMA((len(chunks), 2)),
            DMA((len(chunks) + 1, 2)),
            DMA((4 * (len(chunks) + len(early_chunks)), 2)),
        ],
        compiler_params=pltpu.CompilerParams(collective_id=0, has_side_effects=True, vmem_limit_bytes=40 * MIB),
    )(numer, stats, early_own.reshape((-1,) + split), early_theirs.reshape((-1,) + split), w_o)


def solution(mesh):
    def per_device(x_steps, k_local, v_local, seq_lens, norm_gain, w_q, w_k, w_v, w_o, q_gain, k_gain):
        steps, batch, _ = x_steps.shape
        early = 24
        fresh = project(seq_lens, x_steps, norm_gain, q_gain, k_gain, w_q, w_k, w_v)
        flat = (batch, -1, HEAD_DIM)
        caches = (k_local.reshape(flat), v_local.reshape(flat))
        k_part, v_part, early_numer, early_stats = attend(seq_lens, *caches, *fresh, steps, 0, early)
        early_own = merge_pair(early_numer, early_stats, batch)
        early_theirs = lax.ppermute(early_own, 'sp', [(i, (i + 2) % 4) for i in range(4)])
        k_out, v_out, numer, stats = attend(seq_lens, *caches, *fresh, steps, early, batch - early, (k_part, v_part))
        own, other = merge(numer, stats, early_own, early_theirs, w_o, steps, batch)
        y_steps = (x_steps.astype(F32) + (own + other)).astype(BF16)
        return y_steps, k_out.reshape(k_local.shape), v_out.reshape(v_local.shape)

    cache_spec = P('dp', 'sp', None, None)
    step_spec = P(None, 'dp', None)
    return jax.shard_map(per_device, mesh=mesh, in_specs=(step_spec, cache_spec, cache_spec, P('dp'), P(), P(), P(), P(), P(), P(), P()), out_specs=(step_spec, cache_spec, cache_spec), check_vma=False)
```
